16 devices in a mesh: dp: 2 (over z), fsdp: 8 (over y, x, core).
Axes of the slice: x: 2, y: 2, z: 2, core: 2. Of those that a mesh axis runs over, the one named last changes fastest.
Arguments:
- hidden: bfloat16 [16, 64, 1536], P(('dp', 'fsdp')), parts along dimension 0
- attn_norm: bfloat16 [2, 1536], P(None, 'fsdp')
- w_q: bfloat16 [2, 1536, 12, 128], P(None, 'fsdp')
- w_k: bfloat16 [2, 1536, 2, 128], P(None, 'fsdp')
- w_v: bfloat16 [2, 1536, 2, 128], P(None, 'fsdp')
- w_o: bfloat16 [2, 1536, 1536], P(None, 'fsdp')
- mlp_norm: bfloat16 [2, 1536], P(None, 'fsdp')
- w_gate: bfloat16 [2, 1536, 8960], P(None, 'fsdp')
- w_up: bfloat16 [2, 1536, 8960], P(None, 'fsdp')
- w_down: bfloat16 [2, 8960, 1536], P(None, 'fsdp')
Outputs:
- output: bfloat16 [16, 64, 1536], P(('dp', 'fsdp')), parts along dimension 0
There are 2 independent parts. The reference program is written for one: setup_inputs(seed, part) draws one part's arguments, and reference() takes and returns one part's arrays. A program takes and returns all parts, laid end to end along the dimension named above; an argument that names none is the same for every part.
All inputs are finite; a program needn't handle non-finite values.
Results may differ from the reference program's by a relative error of at most 0.02.
Values are sent between devices in bfloat16 or wider.
A program may use at most 1 GiB of HBM per device.

```python
import jax
import jax.numpy as jnp
from jax import lax

MODEL_DIM = 1536
HEADS = 12
KV_HEADS = 2
HEAD_DIM = 128
FFN_DIM = 8960
SEQ_LEN = 64
BATCH_DEV = 1
FSDP_SIZE = 8
LAYERS = 2

GROUP_SEQS = FSDP_SIZE * BATCH_DEV
ROPE_THETA = 500000.0
NORM_EPS = 1e-5


def setup_inputs(seed: int = 0, part: int = 0) -> dict:
    weight_keys = jax.random.split(jax.random.key(seed), 9)
    seq_key = jax.random.fold_in(jax.random.key(seed + 1), part)
    qo_width = HEADS * HEAD_DIM

    def gain_vector(rng_key):
        return (1.0 + 0.25 * jax.random.normal(rng_key, (LAYERS, MODEL_DIM), jnp.float32)).astype(jnp.bfloat16)

    def weight(rng_key, shape, fan_in, gain):
        scale = gain * fan_in ** -0.5
        return (scale * jax.random.normal(rng_key, shape, jnp.float32)).astype(jnp.bfloat16)

    hidden = (0.5 * jax.random.normal(seq_key, (GROUP_SEQS, SEQ_LEN, MODEL_DIM), jnp.float32)).astype(jnp.bfloat16)
    return {
        "hidden": hidden,
        "attn_norm": gain_vector(weight_keys[0]),
        "w_q": weight(weight_keys[1], (LAYERS, MODEL_DIM, HEADS, HEAD_DIM), MODEL_DIM, 1.5),
        "w_k": weight(weight_keys[2], (LAYERS, MODEL_DIM, KV_HEADS, HEAD_DIM), MODEL_DIM, 1.5),
        "w_v": weight(weight_keys[3], (LAYERS, MODEL_DIM, KV_HEADS, HEAD_DIM), MODEL_DIM, 1.0),
        "w_o": weight(weight_keys[4], (LAYERS, qo_width, MODEL_DIM), qo_width, 1.5),
        "mlp_norm": gain_vector(weight_keys[5]),
        "w_gate": weight(weight_keys[6], (LAYERS, MODEL_DIM, FFN_DIM), MODEL_DIM, 1.0),
        "w_up": weight(weight_keys[7], (LAYERS, MODEL_DIM, FFN_DIM), MODEL_DIM, 1.0),
        "w_down": weight(weight_keys[8], (LAYERS, FFN_DIM, MODEL_DIM), FFN_DIM, 1.0),
    }


def rms_norm(hidden, gain):
    wide_hidden = hidden.astype(jnp.float32)
    inv_rms = lax.rsqrt(jnp.mean(wide_hidden * wide_hidden, axis=-1, keepdims=True) + NORM_EPS)
    return (wide_hidden * inv_rms * gain.astype(jnp.float32)).astype(jnp.bfloat16)


def rope_tables(seq_len, head_dim):
    half = head_dim // 2
    inv_freq = jnp.power(ROPE_THETA, -(jnp.arange(half, dtype=jnp.float32) * 2.0 / head_dim))
    angles = jnp.arange(seq_len, dtype=jnp.float32)[:, None] * inv_freq[None, :]
    return jnp.cos(angles)[:, None, :], jnp.sin(angles)[:, None, :]


def apply_rope(proj, cos_table, sin_table):
    half = proj.shape[-1] // 2
    first = proj[..., :half]
    second = proj[..., half:]
    rotated = jnp.concatenate([first * cos_table - second * sin_table, second * cos_table + first * sin_table], axis=-1)
    return rotated.astype(jnp.bfloat16)


def decoder_layer(seq_hidden, weights, cos_table, sin_table):
    attn_gain, w_q, w_k, w_v, w_o, mlp_gain, w_gate, w_up, w_down = weights
    group = HEADS // KV_HEADS
    normed = rms_norm(seq_hidden, attn_gain)
    q_proj = jnp.dot(normed, w_q.reshape(MODEL_DIM, HEADS * HEAD_DIM), preferred_element_type=jnp.float32)
    k_proj = jnp.dot(normed, w_k.reshape(MODEL_DIM, KV_HEADS * HEAD_DIM), preferred_element_type=jnp.float32)
    v_proj = jnp.dot(normed, w_v.reshape(MODEL_DIM, KV_HEADS * HEAD_DIM), preferred_element_type=jnp.float32)
    queries = apply_rope(q_proj.reshape(SEQ_LEN, HEADS, HEAD_DIM), cos_table, sin_table)
    keys_rot = apply_rope(k_proj.reshape(SEQ_LEN, KV_HEADS, HEAD_DIM), cos_table, sin_table)
    values = v_proj.astype(jnp.bfloat16).reshape(SEQ_LEN, KV_HEADS, HEAD_DIM)
    q_grouped = queries.reshape(SEQ_LEN, KV_HEADS, group, HEAD_DIM)
    scores = jnp.einsum("qkgd,skd->kgqs", q_grouped.astype(jnp.float32), keys_rot.astype(jnp.float32)) * HEAD_DIM ** -0.5
    causal = jnp.arange(SEQ_LEN)[:, None] >= jnp.arange(SEQ_LEN)[None, :]
    probs = jax.nn.softmax(jnp.where(causal, scores, -jnp.inf), axis=-1).astype(jnp.bfloat16)
    attended = jnp.einsum("kgqs,skd->qkgd", probs.astype(jnp.float32), values.astype(jnp.float32)).astype(jnp.bfloat16)
    attended = attended.reshape(SEQ_LEN, HEADS * HEAD_DIM)
    after_attn = (seq_hidden.astype(jnp.float32) + jnp.dot(attended, w_o, preferred_element_type=jnp.float32)).astype(jnp.bfloat16)
    mlp_in = rms_norm(after_attn, mlp_gain)
    gate_proj = jnp.dot(mlp_in, w_gate, preferred_element_type=jnp.float32).astype(jnp.bfloat16)
    up_proj = jnp.dot(mlp_in, w_up, preferred_element_type=jnp.float32).astype(jnp.bfloat16)
    gated = (jax.nn.silu(gate_proj.astype(jnp.float32)) * up_proj.astype(jnp.float32)).astype(jnp.bfloat16)
    return (after_attn.astype(jnp.float32) + jnp.dot(gated, w_down, preferred_element_type=jnp.float32)).astype(jnp.bfloat16)


def reference(hidden, attn_norm, w_q, w_k, w_v, w_o, mlp_norm, w_gate, w_up, w_down):
    cos_table, sin_table = rope_tables(SEQ_LEN, HEAD_DIM)
    stacked = (attn_norm, w_q, w_k, w_v, w_o, mlp_norm, w_gate, w_up, w_down)

    def one_sequence(seq_hidden):
        def layer_step(carry, weights):
            return decoder_layer(carry, weights, cos_table, sin_table), None

        final, unused = lax.scan(layer_step, seq_hidden, stacked)
        return final

    return lax.map(one_sequence, hidden)
```

```python
import jax
import jax.numpy as jnp
from jax import lax
from jax.sharding import PartitionSpec as P

ROPE_THETA = 500000.0
NORM_EPS = 1e-5


def rms_norm(hidden, gain):
    wide_hidden = hidden.astype(jnp.float32)
    inv_rms = lax.rsqrt(jnp.mean(wide_hidden * wide_hidden, axis=-1, keepdims=True) + NORM_EPS)
    return (wide_hidden * inv_rms * gain.astype(jnp.float32)).astype(jnp.bfloat16)


def rope_tables(seq_len, head_dim):
    half = head_dim // 2
    inv_freq = jnp.power(ROPE_THETA, -(jnp.arange(half, dtype=jnp.float32) * 2.0 / head_dim))
    angles = jnp.arange(seq_len, dtype=jnp.float32)[:, None] * inv_freq[None, :]
    return jnp.cos(angles)[:, None, :], jnp.sin(angles)[:, None, :]


def apply_rope(proj, cos_table, sin_table):
    half = proj.shape[-1] // 2
    first = proj[..., :half]
    second = proj[..., half:]
    rotated = jnp.concatenate([first * cos_table - second * sin_table, second * cos_table + first * sin_table], axis=-1)
    return rotated.astype(jnp.bfloat16)


def decoder_layer(hidden, attn_gain, w_q, w_k, w_v, w_o, mlp_gain, w_gate, w_up, w_down):
    batch, seq_len, width = hidden.shape
    heads, head_dim = w_q.shape[1], w_q.shape[2]
    kv_heads = w_k.shape[1]
    group = heads // kv_heads
    cos_table, sin_table = rope_tables(seq_len, head_dim)
    normed = rms_norm(hidden, attn_gain)
    queries = apply_rope(jnp.einsum("bsd,dhe->bshe", normed, w_q, preferred_element_type=jnp.float32), cos_table, sin_table)
    keys_rot = apply_rope(jnp.einsum("bsd,dhe->bshe", normed, w_k, preferred_element_type=jnp.float32), cos_table, sin_table)
    values = jnp.einsum("bsd,dhe->bshe", normed, w_v, preferred_element_type=jnp.float32).astype(jnp.bfloat16)
    q_grouped = queries.reshape(batch, seq_len, kv_heads, group, head_dim)
    scores = jnp.einsum("bqkgd,bskd->bkgqs", q_grouped, keys_rot, preferred_element_type=jnp.float32) * head_dim ** -0.5
    row_pos = lax.broadcasted_iota(jnp.int32, (seq_len, seq_len), 0)
    col_pos = lax.broadcasted_iota(jnp.int32, (seq_len, seq_len), 1)
    probs = jax.nn.softmax(jnp.where(row_pos >= col_pos, scores, -jnp.inf), axis=-1).astype(jnp.bfloat16)
    attended = jnp.einsum("bkgqs,bskd->bqkgd", probs, values, preferred_element_type=jnp.float32).astype(jnp.bfloat16)
    attended = attended.reshape(batch, seq_len, heads * head_dim)
    after_attn = (hidden.astype(jnp.float32) + jnp.einsum("bsf,fd->bsd", attended, w_o, preferred_element_type=jnp.float32)).astype(jnp.bfloat16)
    mlp_in = lax.all_gather(rms_norm(after_attn, mlp_gain).reshape(batch * seq_len, width), "fsdp", axis=0, tiled=True)
    gate_proj = jnp.dot(mlp_in, w_gate, preferred_element_type=jnp.float32).astype(jnp.bfloat16)
    up_proj = jnp.dot(mlp_in, w_up, preferred_element_type=jnp.float32).astype(jnp.bfloat16)
    gated = (jax.nn.silu(gate_proj.astype(jnp.float32)) * up_proj.astype(jnp.float32)).astype(jnp.bfloat16)
    partial = jnp.dot(gated, w_down, preferred_element_type=jnp.float32)
    down = lax.psum_scatter(partial, "fsdp", scatter_dimension=0, tiled=True).reshape(batch, seq_len, width)
    return (after_attn.astype(jnp.float32) + down).astype(jnp.bfloat16)


def solution(mesh):
    batch_spec = P(("dp", "fsdp"), None, None)
    gain_spec = P(None, "fsdp")
    proj_spec = P(None, "fsdp", None, None)
    mat_spec = P(None, "fsdp", None)
    size = mesh.shape["fsdp"]

    def columns(shard):
        rows, cols = shard.shape
        blocks = shard.reshape(rows, size, cols // size).transpose(1, 0, 2)
        return lax.all_to_all(blocks, "fsdp", 0, 0, tiled=True).reshape(rows * size, cols // size)

    def local_forward(hidden, attn_norm, w_q, w_k, w_v, w_o, mlp_norm, w_gate, w_up, w_down):
        for layer in range(w_q.shape[0]):
            whole = [lax.all_gather(shard[layer], "fsdp", axis=0, tiled=True) for shard in (attn_norm, w_q, w_k, w_v, w_o, mlp_norm)]
            hidden = decoder_layer(hidden, *whole, columns(w_gate[layer]), columns(w_up[layer]), w_down[layer])
        return hidden

    return jax.shard_map(local_forward, mesh=mesh, in_specs=(batch_spec, gain_spec, proj_spec, proj_spec, proj_spec, mat_spec, gain_spec, mat_spec, mat_spec, mat_spec), out_specs=batch_spec, check_vma=False)
```

```python
import functools

import jax
import jax.numpy as jnp
from jax import lax
from jax.experimental import pallas as pl
from jax.experimental.pallas import tpu as pltpu
from jax.sharding import PartitionSpec as P

MESH = pl.DeviceIdType.MESH
ROPE_THETA = 500000.0
NORM_EPS = 1e-5
LAYERS = 2
SEQ = 64
DIM = 1536
HEADS = 12
KV_HEADS = 2
HEAD_DIM = 128
GROUP = HEADS // KV_HEADS
QKV = (HEADS + 2 * KV_HEADS) * HEAD_DIM
ATTN = QKV + DIM
FFN = 8960
ROWS = DIM // 8
FFN_ROWS = FFN // 8
WINDOW = 1280
HALF = ROWS // 2
DIRECT = 112
RELAY = ROWS - DIRECT
BF = jnp.bfloat16
F32 = jnp.float32
CHIPS = (2, 4, 6)
GU_ORDER = (2, 4, 6, 3, 5, 7, 1)
GU_RELAYED = (2, 4, 6, 3, 5, 7)


def aligned(value, size):
    return pl.multiple_of(value, size)


def kernel(x_ref, gain_ref, cos_ref, sin_ref, wa_ref, wg_ref, wu_ref, wd_ref, y_ref,
           gains, gain_rows, wa, wgu, wd, res, mid, q_buf, k_buf, v_buf, o_buf, u_buf, z_buf, part, r1, r2a, r2b, r3a, r3b,
           gain_s, gain_r, ad_s, ad_r, az_s, az_r, ac_s, ac_r, gd_s, gd_r, gz_s, gz_r, ag_s, ag_r, rs_s, rs_r, own_a, own_gu, own_wd):
    z = lax.axis_index("dp")
    me = lax.axis_index("fsdp")
    c = me % 2
    x = (me // 2) % 2
    y = me // 4

    def peer(k):
        cc = 1 - c if k % 2 else c
        xx = 1 - x if (k // 2) % 2 else x
        yy = 1 - y if k // 4 else y
        return 4 * yy + 2 * xx + cc

    def block(k):
        cc = 1 - c if k % 2 else c
        xx = 1 - x if (k // 2) % 2 else x
        yy = 1 - y if k // 4 else y
        return 4 * cc + 2 * yy + xx

    def window(j):
        return aligned(128 * ((35 * j) // 4 - j // 7), 128)

    def plane(k):
        return (z, peer(k))

    across = (1 - z, me)
    started = []

    def remote(src, dst, send, recv, device):
        return pltpu.make_async_remote_copy(src_ref=src, dst_ref=dst, send_sem=send, recv_sem=recv, device_id=device, device_id_type=MESH)

    def go(copy):
        copy.start()
        started.append(copy)

    barrier = pltpu.get_barrier_semaphore()
    for k in range(1, 8):
        pl.semaphore_signal(barrier, inc=1, device_id=plane(k), device_id_type=MESH)
    pl.semaphore_signal(barrier, inc=1, device_id=across, device_id_type=MESH)
    pl.semaphore_wait(barrier, 8)

    def gain_copy(k):
        return remote(gain_ref, gains.at[me], gain_s.at[k - 1], gain_r.at[k - 1], plane(k))

    def gain_arrival(k):
        dst = gains.at[peer(k)]
        return remote(dst, dst, gain_s.at[k - 1], gain_r.at[k - 1], plane(k))

    def attn_rows(l, k, half):
        return wa.at[l, pl.ds(aligned(ROWS * peer(k) + HALF * half, 32), HALF), :]

    def attn_direct(l, n):
        src = wa_ref.at[l, pl.ds(aligned(HALF * z, 32), HALF), :]
        return remote(src, attn_rows(l, 0, z), ad_s.at[l, n], ad_r.at[l, n], plane(CHIPS[n]))

    def attn_arrival(l, n):
        dst = attn_rows(l, CHIPS[n], z)
        return remote(dst, dst, ad_s.at[l, n], ad_r.at[l, n], plane(CHIPS[n]))

    def attn_across(l, n):
        rows = attn_rows(l, CHIPS[n], z)
        return remote(rows, rows, az_s.at[l, n], az_r.at[l, n], across)

    def attn_across_arrival(l, n):
        dst = attn_rows(l, CHIPS[n], 1 - z)
        return remote(dst, dst, az_s.at[l, n], az_r.at[l, n], across)

    def attn_core(l, n, half, slot):
        rows = attn_rows(l, CHIPS[n], half)
        return remote(rows, rows, ac_s.at[l, slot], ac_r.at[l, slot], plane(1))

    def attn_core_arrival(l, n, half, slot):
        dst = attn_rows(l, CHIPS[n] + 1, half)
        return remote(dst, dst, ac_s.at[l, slot], ac_r.at[l, slot], plane(1))

    def shard_rows(l, k):
        return wa.at[l, pl.ds(aligned(ROWS * peer(k), 64), ROWS), :]

    def attn_shard(l):
        return remote(wa_ref.at[l], shard_rows(l, 0), ac_s.at[l, 6], ac_r.at[l, 6], plane(1))

    def attn_shard_arrival(l):
        dst = shard_rows(l, 1)
        return remote(dst, dst, ac_s.at[l, 6], ac_r.at[l, 6], plane(1))

    def attn_own(l):
        return pltpu.make_async_copy(wa_ref.at[l], shard_rows(l, 0), own_a.at[l])

    def send_attn(l):
        for n in range(3):
            go(attn_direct(l, n))
        go(attn_shard(l))
        attn_own(l).start()

    def relay_attn(l, n):
        attn_arrival(l, n).wait_recv()
        go(attn_across(l, n))
        go(attn_core(l, n, z, n))

    def relay_attn_across(l, n):
        attn_across_arrival(l, n).wait_recv()
        go(attn_core(l, n, 1 - z, 3 + n))

    def await_attn(l):
        attn_own(l).wait()
        attn_shard_arrival(l).wait_recv()
        for n in range(3):
            attn_core_arrival(l, n, z, n).wait_recv()
        for n in range(3):
            attn_core_arrival(l, n, 1 - z, 3 + n).wait_recv()

    halves = (wg_ref, wu_ref)

    def gu_rows(l, g, k, start, count):
        return wgu.at[l, g, pl.ds(aligned(ROWS * peer(k) + start, 16), count), :]

    def gu_direct(l, g, k):
        start, count = (0, ROWS) if k == 1 else (aligned(RELAY * z, 16), DIRECT)
        src = halves[g].at[l, pl.ds(start, count), pl.ds(window(peer(k)), WINDOW)]
        return remote(src, gu_rows(l, g, 0, start, count), gd_s.at[l, g, k - 1], gd_r.at[l, g, k - 1], plane(k))

    def gu_arrival(l, g, k):
        start, count = (0, ROWS) if k == 1 else (RELAY * z, DIRECT)
        dst = gu_rows(l, g, k, start, count)
        return remote(dst, dst, gd_s.at[l, g, k - 1], gd_r.at[l, g, k - 1], plane(k))

    def gu_across(l, g, k):
        rows = gu_rows(l, g, k, DIRECT * z, RELAY)
        return remote(rows, rows, gz_s.at[l, g, k - 2], gz_r.at[l, g, k - 2], across)

    def gu_across_arrival(l, g, k):
        dst = gu_rows(l, g, k, DIRECT * (1 - z), RELAY)
        return remote(dst, dst, gz_s.at[l, g, k - 2], gz_r.at[l, g, k - 2], across)

    def gu_own(l, g):
        return pltpu.make_async_copy(halves[g].at[l, :, pl.ds(window(me), WINDOW)], gu_rows(l, g, 0, 0, ROWS), own_gu.at[l, g])

    def send_gu(l):
        for k in GU_ORDER:
            for g in range(2):
                go(gu_direct(l, g, k))
        for g in range(2):
            gu_own(l, g).start()

    def relay_gu(l, k):
        for g in range(2):
            gu_arrival(l, g, k).wait_recv()
            go(gu_across(l, g, k))

    def await_gu(l):
        for g in range(2):
            gu_arrival(l, g, 1).wait_recv()
            gu_own(l, g).wait()
        for k in GU_RELAYED:
            for g in range(2):
                gu_across_arrival(l, g, k).wait_recv()

    skip = FFN_ROWS * me - window(me)

    def wd_copy(l):
        return pltpu.make_async_copy(wd_ref.at[l], wd.at[pl.ds(aligned(skip, 32), FFN_ROWS), :], own_wd)

    def normed(ref, row):
        wide = ref[...].astype(F32)
        inv_rms = lax.rsqrt(jnp.mean(wide * wide, axis=-1, keepdims=True) + NORM_EPS)
        return (wide * inv_rms * gain_rows[row : row + 1, :]).astype(BF)

    def project(l):
        u = normed(res, l)
        cos, sin = cos_ref[...], sin_ref[...]

        def rotate(v):
            return (v * cos + pltpu.roll(v, HEAD_DIM // 2, 1) * sin).astype(BF)

        def two_heads(n):
            return jnp.dot(u, wa[l, :, pl.ds(aligned(256 * n, 256), 256)], preferred_element_type=F32)

        def q_heads(n, carry):
            pair = two_heads(n)
            for t in range(2):
                q_buf[pl.ds(aligned((2 * n + t) * SEQ, SEQ), SEQ), :] = rotate(pair[:, 128 * t : 128 * (t + 1)])
            return carry

        lax.fori_loop(0, HEADS // 2, q_heads, 0)
        keys, values = two_heads(HEADS // 2), two_heads(HEADS // 2 + 1)
        for t in range(2):
            k_buf[t] = rotate(keys[:, 128 * t : 128 * (t + 1)])
            v_buf[t] = values[:, 128 * t : 128 * (t + 1)].astype(BF)

    def attend(l):
        row = lax.broadcasted_iota(jnp.int32, (GROUP * SEQ, SEQ), 0) % SEQ
        col = lax.broadcasted_iota(jnp.int32, (GROUP * SEQ, SEQ), 1)
        for g in range(KV_HEADS):
            q = q_buf[g * GROUP * SEQ : (g + 1) * GROUP * SEQ, :]
            scores = lax.dot_general(q, k_buf[g], (((1,), (1,)), ((), ())), preferred_element_type=F32) * HEAD_DIM ** -0.5
            scores = jnp.where(row >= col, scores, -jnp.inf)
            e = jnp.exp(scores - jnp.max(scores, axis=-1, keepdims=True))
            probs = (e / jnp.sum(e, axis=-1, keepdims=True)).astype(BF)
            o = jnp.dot(probs, v_buf[g], preferred_element_type=F32).astype(BF)
            for j in range(GROUP):
                h = g * GROUP + j
                o_buf[:, h * HEAD_DIM : (h + 1) * HEAD_DIM] = o[j * SEQ : (j + 1) * SEQ]

        def out_cols(n, carry):
            cols = pl.ds(aligned(256 * n, 256), 256)
            add = jnp.dot(o_buf[...], wa[l, :, pl.ds(aligned(QKV + 256 * n, 256), 256)], preferred_element_type=F32)
            mid[:, cols] = (res[:, cols].astype(F32) + add).astype(BF)
            return carry

        lax.fori_loop(0, DIM // 256, out_cols, 0)

    def seq_rows(l, k):
        return u_buf.at[l, pl.ds(aligned(SEQ * block(k), SEQ), SEQ), :]

    def ag_copy(l, k):
        return remote(seq_rows(l, 0), seq_rows(l, 0), ag_s.at[l, k - 1], ag_r.at[l, k - 1], plane(k))

    def ag_relay(l, k):
        return remote(seq_rows(l, k), seq_rows(l, k), ag_s.at[l, k], ag_r.at[l, k], plane(1))

    def ag_arrival(l, k):
        dst = seq_rows(l, k)
        return remote(dst, dst, ag_s.at[l, k - 1], ag_r.at[l, k - 1], plane(k))

    def gate_up(l, b):
        rows = pl.ds(aligned(256 * b, 256), 256)

        def cols(n, carry):
            at = pl.ds(aligned(256 * n, 256), 256)
            u = u_buf[l, rows, :]
            gate = jnp.dot(u, wgu[l, 0, :, at], preferred_element_type=F32).astype(BF).astype(F32)
            up = jnp.dot(u, wgu[l, 1, :, at], preferred_element_type=F32).astype(BF).astype(F32)
            gated = (jax.nn.silu(gate) * up).astype(BF)
            place = 256 * n + lax.broadcasted_iota(jnp.int32, (256, 256), 1)
            mine = (place >= skip) & (place < skip + FFN_ROWS)
            z_buf[rows, at] = jnp.where(mine, gated, jnp.zeros_like(gated))
            return carry

        lax.fori_loop(0, WINDOW // 256, cols, 0)

    def down(b):
        rows = pl.ds(aligned(256 * b, 256), 256)

        def cols(n, carry):
            at = pl.ds(aligned(256 * n, 256), 256)
            part[b, :, at] = jnp.dot(z_buf[rows, :], wd[:, at], preferred_element_type=F32)
            return carry

        lax.fori_loop(0, DIM // 256, cols, 0)

    A, B = slice(0, DIM // 2), slice(DIM // 2, DIM)

    def chip_rows(yy, xx):
        return pl.ds(aligned(SEQ * (2 * yy + xx), SEQ), SEQ)

    def rs_core(l):
        return remote(part.at[1 - c], r1.at[l], rs_s.at[l, 0], rs_r.at[l, 0], plane(1))

    def rs_a(l, yy):
        return remote(part.at[c, chip_rows(yy, 1 - x), A], r2a.at[l, yy], rs_s.at[l, 1 + yy], rs_r.at[l, 1 + yy], plane(2))

    def rs_b(l, xx):
        return remote(part.at[c, chip_rows(1 - y, xx), B], r2b.at[l, xx], rs_s.at[l, 3 + xx], rs_r.at[l, 3 + xx], plane(4))

    def rs_a_last(l):
        return remote(part.at[c, chip_rows(1 - y, x), A], r3a.at[l], rs_s.at[l, 5], rs_r.at[l, 5], plane(4))

    def rs_b_last(l):
        return remote(part.at[c, chip_rows(y, 1 - x), B], r3b.at[l], rs_s.at[l, 6], rs_r.at[l, 6], plane(2))

    for k in range(1, 8):
        go(gain_copy(k))
    send_attn(0)
    send_gu(0)
    gains[me] = gain_ref[...]
    res[...] = x_ref[...]

    def clear(n, carry):
        wd[pl.ds(aligned(128 * n, 128), 128), :] = jnp.zeros((128, DIM), BF)
        return carry

    lax.fori_loop(0, WINDOW // 128, clear, 0)
    for k in range(1, 8):
        gain_arrival(k).wait_recv()
    for p in range(4):
        gain_rows[:, 384 * p : 384 * (p + 1)] = gains[2 * p] + gains[2 * p + 1]
    for n in range(3):
        relay_attn(0, n)

    for l in range(LAYERS):
        wd_copy(l).start()
        for n in range(3):
            relay_attn_across(l, n)
        await_attn(l)
        for k in GU_RELAYED[:1]:
            relay_gu(l, k)
        project(l)
        for k in GU_RELAYED[1:2]:
            relay_gu(l, k)
        attend(l)
        u_buf[l, pl.ds(aligned(SEQ * block(0), SEQ), SEQ), :] = normed(mid, 2 + l)
        for k in (2, 4, 6, 1):
            go(ag_copy(l, k))
        if l + 1 < LAYERS:
            send_attn(l + 1)
        for k in GU_RELAYED[2:]:
            relay_gu(l, k)
        for k in CHIPS:
            ag_arrival(l, k).wait_recv()
            go(ag_relay(l, k))
        await_gu(l)
        gate_up(l, c)
        for k in (1, 3, 5, 7):
            ag_arrival(l, k).wait_recv()
        gate_up(l, 1 - c)
        wd_copy(l).wait()
        down(1 - c)
        to_core = rs_core(l)
        to_core.start()
        down(c)
        to_core.wait_recv()
        part[c] = part[c] + r1[l]
        sends = [to_core]
        for t in range(2):
            for copy in (rs_a(l, t), rs_b(l, t)):
                copy.start()
                sends.append(copy)
        if l + 1 < LAYERS:
            for n in range(3):
                relay_attn(l + 1, n)
        for t in range(2):
            rs_a(l, t).wait_recv()
            rs_b(l, t).wait_recv()
            part[c, chip_rows(t, x), A] = part[c, chip_rows(t, x), A] + r2a[l, t]
            part[c, chip_rows(y, t), B] = part[c, chip_rows(y, t), B] + r2b[l, t]
        for copy in (rs_a_last(l), rs_b_last(l)):
            copy.start()
            sends.append(copy)
        if l + 1 < LAYERS:
            send_gu(l + 1)
        rs_a_last(l).wait_recv()
        rs_b_last(l).wait_recv()
        out = y_ref if l + 1 == LAYERS else res
        out[:, A] = (mid[:, A].astype(F32) + (part[c, chip_rows(y, x), A] + r3a[l])).astype(BF)
        out[:, B] = (mid[:, B].astype(F32) + (part[c, chip_rows(y, x), B] + r3b[l])).astype(BF)
        for copy in sends:
            copy.wait_send()
    for copy in started:
        copy.wait_send()


def solution(mesh):
    vmem = pl.BlockSpec(memory_space=pltpu.VMEM)
    hbm = pl.BlockSpec(memory_space=pl.ANY)
    dma = pltpu.SemaphoreType.DMA

    def local_forward(hidden, attn_norm, w_q, w_k, w_v, w_o, mlp_norm, w_gate, w_up, w_down):
        me = lax.axis_index("fsdp")
        gain = jnp.concatenate([attn_norm, mlp_norm, jnp.zeros((4, ROWS), BF)], axis=0).astype(F32)
        gain = jnp.where(me % 2 == 0, jnp.pad(gain, ((0, 0), (0, ROWS))), jnp.pad(gain, ((0, 0), (ROWS, 0))))
        inv_freq = jnp.power(ROPE_THETA, -(jnp.arange(HEAD_DIM // 2, dtype=F32) * 2.0 / HEAD_DIM))
        angles = jnp.arange(SEQ, dtype=F32)[:, None] * inv_freq[None, :]
        cos = jnp.concatenate([jnp.cos(angles), jnp.cos(angles)], axis=1)
        sin = jnp.concatenate([-jnp.sin(angles), jnp.sin(angles)], axis=1)
        flat = [w.reshape(LAYERS, ROWS, -1) for w in (w_q, w_k, w_v, w_o)]
        attn = jnp.concatenate(flat, axis=2)
        y = pl.pallas_call(
            kernel,
            out_shape=jax.ShapeDtypeStruct((SEQ, DIM), BF),
            in_specs=[vmem] * 4 + [hbm] * 4,
            out_specs=vmem,
            scratch_shapes=[
                pltpu.VMEM((8, 8, 2 * ROWS), F32),
                pltpu.VMEM((8, DIM), F32),
                pltpu.VMEM((LAYERS, DIM, ATTN), BF),
                pltpu.VMEM((LAYERS, 2, DIM, WINDOW), BF),
                pltpu.VMEM((WINDOW, DIM), BF),
                pltpu.VMEM((SEQ, DIM), BF),
                pltpu.VMEM((SEQ, DIM), BF),
                pltpu.VMEM((HEADS * SEQ, HEAD_DIM), BF),
                pltpu.VMEM((KV_HEADS, SEQ, HEAD_DIM), BF),
                pltpu.VMEM((KV_HEADS, SEQ, HEAD_DIM), BF),
                pltpu.VMEM((SEQ, DIM), BF),
                pltpu.VMEM((LAYERS, 8 * SEQ, DIM), BF),
                pltpu.VMEM((8 * SEQ, WINDOW), BF),
                pltpu.VMEM((2, 4 * SEQ, DIM), F32),
                pltpu.VMEM((LAYERS, 4 * SEQ, DIM), F32),
                pltpu.VMEM((LAYERS, 2, SEQ, DIM // 2), F32),
                pltpu.VMEM((LAYERS, 2, SEQ, DIM // 2), F32),
                pltpu.VMEM((LAYERS, SEQ, DIM // 2), F32),
                pltpu.VMEM((LAYERS, SEQ, DIM // 2), F32),
                dma((7,)), dma((7,)),
                dma((LAYERS, 3)), dma((LAYERS, 3)),
                dma((LAYERS, 3)), dma((LAYERS, 3)),
                dma((LAYERS, 7)), dma((LAYERS, 7)),
                dma((LAYERS, 2, 7)), dma((LAYERS, 2, 7)),
                dma((LAYERS, 2, 6)), dma((LAYERS, 2, 6)),
                dma((LAYERS, 7)), dma((LAYERS, 7)),
                dma((LAYERS, 7)), dma((LAYERS, 7)),
                dma((LAYERS,)), dma((LAYERS, 2)), dma(()),
            ],
            compiler_params=pltpu.CompilerParams(collective_id=0, has_side_effects=True, vmem_limit_bytes=67043328),
        )(hidden.reshape(SEQ, DIM), gain, cos, sin, attn, w_gate, w_up, w_down)
        return y.reshape(1, SEQ, DIM)

    batch_spec = P(("dp", "fsdp"), None, None)
    gain_spec = P(None, "fsdp")
    proj_spec = P(None, "fsdp", None, None)
    mat_spec = P(None, "fsdp", None)
    return jax.shard_map(local_forward, mesh=mesh, in_specs=(batch_spec, gain_spec, proj_spec, proj_spec, proj_spec, mat_spec, gain_spec, mat_spec, mat_spec, mat_spec), out_specs=batch_spec, check_vma=False)
```

```python
import functools

import jax
import jax.numpy as jnp
import numpy as np
from jax import lax
from jax.experimental import pallas as pl
from jax.experimental.pallas import tpu as pltpu
from jax.sharding import PartitionSpec as P

MESH = pl.DeviceIdType.MESH
ROPE_THETA = 500000.0
NORM_EPS = 1e-5
LAYERS = 2
SEQ = 64
DIM = 1536
HEADS = 12
KV_HEADS = 2
HEAD_DIM = 128
GROUP = HEADS // KV_HEADS
GROUP_COLS = (GROUP + 2) * HEAD_DIM
OUT_COLS = DIM // 2
FFN = 8960
ROWS = DIM // 8
FFN_ROWS = FFN // 8
WINDOW = 1152
MAIN = 1088
EDGE = 32
HALF = ROWS // 2
DIRECT = 112
RELAY = ROWS - DIRECT
BF = jnp.bfloat16
F32 = jnp.float32
CHIPS = (2, 4, 6)
PARTS = ((0, 768), (768, 384))
GU_RELAYED = (2, 4, 6, 3, 5, 7)
RELAYS = (((2, 0), (4, 0)), ((2, 1), (4, 1)), ((6, 0), (6, 1), (3, 0), (5, 0)), ((3, 1), (5, 1), (7, 0), (7, 1)))
GU_EARLY = ((2, 0), (4, 0))
GU_LATE = ((2, 1), (4, 1), (6, 0), (6, 1), (3, 0), (5, 0), (3, 1), (5, 1), (7, 0), (7, 1), (1, 0), (1, 1))


def aligned(value, size):
    return pl.multiple_of(value, size)


def kernel(x_ref, an_ref, mn_ref, cos_ref, sin_ref, wqkv_ref, wo_ref, wg_ref, wu_ref, wd_ref, y_ref,
           gain_mine, gains, gain_rows, wq, wo, wgu, wd, edge, res, mid, n_buf, q_buf, k_buf, v_buf, o_buf, add_mine, add_got, u_buf, z_buf, part,
           r1, r2a, r2b, r3a, r3b,
           gain_s, gain_r, ad_s, ad_r, ax_s, ax_r, ac_s, ac_r, zx_s, zx_r, gd_s, gd_r, gz_s, gz_r, ed_s, ed_r, ag_s, ag_r, rs_s, rs_r,
           own_a, own_gu, own_wd):
    z = lax.axis_index("dp")
    me = lax.axis_index("fsdp")
    c = me % 2
    x = (me // 2) % 2
    y = me // 4

    def peer(k):
        cc = 1 - c if k % 2 else c
        xx = 1 - x if (k // 2) % 2 else x
        yy = 1 - y if k // 4 else y
        return 4 * yy + 2 * xx + cc

    def block(k):
        cc = 1 - c if k % 2 else c
        xx = 1 - x if (k // 2) % 2 else x
        yy = 1 - y if k // 4 else y
        return 4 * cc + 2 * yy + xx

    def window(j):
        return aligned(128 * (35 * (j // 4) + 9 * (j % 4) - (j % 4) // 2), 128)

    def plane(k):
        return (z, peer(k))

    across = (1 - z, me)
    started = []

    def remote(src, dst, send, recv, device):
        return pltpu.make_async_remote_copy(src_ref=src, dst_ref=dst, send_sem=send, recv_sem=recv, device_id=device, device_id_type=MESH)

    def go(copy):
        copy.start()
        started.append(copy)

    barrier = pltpu.get_barrier_semaphore()
    for k in range(1, 8):
        pl.semaphore_signal(barrier, inc=1, device_id=plane(k), device_id_type=MESH)
    pl.semaphore_signal(barrier, inc=1, device_id=across, device_id_type=MESH)
    pl.semaphore_wait(barrier, 8)

    def gain_copy(k):
        return remote(gain_mine, gains.at[me], gain_s.at[k - 1], gain_r.at[k - 1], plane(k))

    def gain_arrival(k):
        dst = gains.at[peer(k)]
        return remote(dst, dst, gain_s.at[k - 1], gain_r.at[k - 1], plane(k))

    attn_src = (wqkv_ref, wo_ref)
    attn_dst = (wq, wo)
    attn_cols = (GROUP_COLS, OUT_COLS)

    def attn_rows(l, m, k, start=0, count=ROWS):
        return attn_dst[m].at[l, pl.ds(aligned(ROWS * peer(k) + start, 32), count), :]

    def attn_shard(l, m):
        return attn_src[m].at[l, :, pl.ds(aligned(attn_cols[m] * z, 128), attn_cols[m])]

    def attn_own(l, m):
        return pltpu.make_async_copy(attn_shard(l, m), attn_rows(l, m, 0), own_a.at[l, m])

    def attn_direct(l, m, n):
        return remote(attn_shard(l, m), attn_rows(l, m, 0), ad_s.at[l, m, n], ad_r.at[l, m, n], plane(2 + 2 * n))

    def attn_arrival(l, m, n):
        dst = attn_rows(l, m, 2 + 2 * n)
        return remote(dst, dst, ad_s.at[l, m, n], ad_r.at[l, m, n], plane(2 + 2 * n))

    def attn_turn(l, m, n):
        rows = attn_rows(l, m, 2 + 2 * n, HALF * n, HALF)
        return remote(rows, rows, ax_s.at[l, m, n], ax_r.at[l, m, n], plane(4 - 2 * n))

    def attn_turn_arrival(l, m, n):
        dst = attn_rows(l, m, 6, HALF * n, HALF)
        return remote(dst, dst, ax_s.at[l, m, n], ax_r.at[l, m, n], plane(4 - 2 * n))

    def attn_core(l, m, slot, k, *part_rows):
        rows = attn_rows(l, m, k, *part_rows)
        return remote(rows, rows, ac_s.at[l, m, slot], ac_r.at[l, m, slot], plane(1))

    def attn_core_own(l, m):
        return remote(attn_shard(l, m), attn_rows(l, m, 0), ac_s.at[l, m, 0], ac_r.at[l, m, 0], plane(1))

    def send_attn(l):
        for m in range(2):
            for n in range(2):
                go(attn_direct(l, m, n))
        for m in range(2):
            go(attn_core_own(l, m))
            attn_own(l, m).start()

    def relay_attn(l):
        for m in range(2):
            for n in range(2):
                attn_arrival(l, m, n).wait_recv()
                go(attn_turn(l, m, n))
                go(attn_core(l, m, 1 + n, 2 + 2 * n))

    def relay_attn_across(l):
        for m in range(2):
            for n in range(2):
                attn_turn_arrival(l, m, n).wait_recv()
                go(attn_core(l, m, 3 + n, 6, HALF * n, HALF))

    def await_attn(l, m):
        attn_own(l, m).wait()
        attn_core(l, m, 0, 1).wait_recv()
        for n in range(2):
            attn_core(l, m, 1 + n, 3 + 2 * n).wait_recv()
            attn_core(l, m, 3 + n, 7, HALF * n, HALF).wait_recv()

    halves = (wg_ref, wu_ref)

    def gu_rows(l, p, g, k, start, count):
        return wgu.at[l, g, pl.ds(aligned(ROWS * peer(k) + start, 16), count), pl.ds(*PARTS[p])]

    def gu_direct(l, p, g, k):
        start, count = (0, ROWS) if k == 1 else (aligned(RELAY * z, 16), DIRECT)
        src = halves[g].at[l, pl.ds(start, count), pl.ds(aligned(window(peer(k)) + PARTS[p][0], 128), PARTS[p][1])]
        return remote(src, gu_rows(l, p, g, 0, start, count), gd_s.at[l, p, g, k - 1], gd_r.at[l, p, g, k - 1], plane(k))

    def gu_arrival(l, p, g, k):
        start, count = (0, ROWS) if k == 1 else (RELAY * z, DIRECT)
        dst = gu_rows(l, p, g, k, start, count)
        return remote(dst, dst, gd_s.at[l, p, g, k - 1], gd_r.at[l, p, g, k - 1], plane(k))

    def gu_across(l, p, g, k):
        rows = gu_rows(l, p, g, k, DIRECT * z, RELAY)
        return remote(rows, rows, gz_s.at[l, p, g, k - 2], gz_r.at[l, p, g, k - 2], across)

    def gu_across_arrival(l, p, g, k):
        dst = gu_rows(l, p, g, k, DIRECT * (1 - z), RELAY)
        return remote(dst, dst, gz_s.at[l, p, g, k - 2], gz_r.at[l, p, g, k - 2], across)

    def gu_own(l, g):
        dst = wgu.at[l, g, pl.ds(aligned(ROWS * me, 64), ROWS), :]
        return pltpu.make_async_copy(halves[g].at[l, :, pl.ds(window(me), WINDOW)], dst, own_gu.at[l, g])

    def send_gu(l, p, blocks):
        for k, g in blocks:
            go(gu_direct(l, p, g, k))

    def relay_gu(l, p, blocks):
        for k, g in blocks:
            gu_arrival(l, p, g, k).wait_recv()
            go(gu_across(l, p, g, k))

    def await_gu(l, p):
        for g in range(2):
            gu_arrival(l, p, g, 1).wait_recv()
            if p == 0:
                gu_own(l, g).wait()
        for k in GU_RELAYED:
            for g in range(2):
                gu_across_arrival(l, p, g, k).wait_recv()

    def start_own(l):
        for g in range(2):
            gu_own(l, g).start()
        wd_copy(l).start()
        edge_own(l).start()
        go(edge_core(l))

    def wd_copy(l):
        return pltpu.make_async_copy(wd_ref.at[l, pl.ds(aligned(EDGE * c, EDGE), MAIN), :], wd.at[l, pl.ds(aligned(2 * EDGE * x, EDGE), MAIN), :], own_wd.at[l, 0])

    def edge_own(l):
        return pltpu.make_async_copy(wd_ref.at[l, pl.ds(aligned(MAIN * (1 - x), EDGE), EDGE), :], edge.at[l, 0], own_wd.at[l, 1])

    def edge_core(l):
        return remote(wd_ref.at[l, pl.ds(aligned(MAIN * x, EDGE), EDGE), :], edge.at[l, 1], ed_s.at[l], ed_r.at[l], plane(1))

    takes = c == x

    def finish_wd(l):
        wd_copy(l).wait()
        edge_own(l).wait()
        edge_core(l).wait_recv()
        own, got = edge[l, 0], edge[l, 1]
        none = jnp.zeros_like(own)
        place = MAIN * (1 - x)
        wd[l, pl.ds(aligned(place, EDGE), EDGE), :] = jnp.where(takes, jnp.where(x == 0, own, got), none)
        wd[l, pl.ds(aligned(place + EDGE, EDGE), EDGE), :] = jnp.where(takes, jnp.where(x == 0, got, own), none)

    first = jnp.where(takes, 0, 2 * EDGE * x)
    last = jnp.where(takes, WINDOW, 2 * EDGE * x + MAIN)

    def normed(ref, row):
        wide = ref[...].astype(F32)
        inv_rms = lax.rsqrt(jnp.mean(wide * wide, axis=-1, keepdims=True) + NORM_EPS)
        return (wide * inv_rms * gain_rows[row : row + 1, :]).astype(BF)

    mine, other = pl.ds(aligned(SEQ * z, SEQ), SEQ), pl.ds(aligned(SEQ * (1 - z), SEQ), SEQ)
    left, right = pl.ds(aligned(OUT_COLS * z, 128), OUT_COLS), pl.ds(aligned(OUT_COLS * (1 - z), 128), OUT_COLS)

    def swap_in(l):
        rows = n_buf.at[l, mine, :]
        return remote(rows, rows, zx_s.at[l, 0], zx_r.at[l, 0], across)

    def swap_in_arrival(l):
        rows = n_buf.at[l, other, :]
        return remote(rows, rows, zx_s.at[l, 0], zx_r.at[l, 0], across)

    def swap_heads(l):
        cols = o_buf.at[l, :, left]
        return remote(cols, cols, zx_s.at[l, 1], zx_r.at[l, 1], across)

    def swap_heads_arrival(l):
        cols = o_buf.at[l, :, right]
        return remote(cols, cols, zx_s.at[l, 1], zx_r.at[l, 1], across)

    def swap_out(l):
        return remote(add_mine.at[l, other, :], add_got.at[l], zx_s.at[l, 2], zx_r.at[l, 2], across)

    def start_layer(l):
        n_buf[l, mine, :] = normed(res, l)
        go(swap_in(l))

    def project(l):
        cos, sin = cos_ref[...], sin_ref[...]

        def rotate(v):
            return (v * cos + pltpu.roll(v, HEAD_DIM // 2, 1) * sin).astype(BF)

        def two_heads(n):
            return jnp.dot(n_buf[l], wq[l, :, pl.ds(aligned(256 * n, 256), 256)], preferred_element_type=F32)

        def q_heads(n, carry):
            pair = two_heads(n)
            for t in range(2):
                turned = rotate(pair[:, 128 * t : 128 * (t + 1)])
                for seq in range(2):
                    q_buf[seq, pl.ds(aligned((2 * n + t) * SEQ, SEQ), SEQ), :] = turned[SEQ * seq : SEQ * (seq + 1)]
            return carry

        lax.fori_loop(0, GROUP // 2, q_heads, 0)
        pair = two_heads(GROUP // 2)
        k_buf[...] = rotate(pair[:, :128])
        v_buf[...] = pair[:, 128:].astype(BF)

    def attend(l):
        row = lax.broadcasted_iota(jnp.int32, (GROUP * SEQ, SEQ), 0) % SEQ
        col = lax.broadcasted_iota(jnp.int32, (GROUP * SEQ, SEQ), 1)
        for seq in range(2):
            rows = slice(SEQ * seq, SEQ * (seq + 1))
            scores = lax.dot_general(q_buf[seq], k_buf[rows, :], (((1,), (1,)), ((), ())), preferred_element_type=F32) * HEAD_DIM ** -0.5
            scores = jnp.where(row >= col, scores, -jnp.inf)
            e = jnp.exp(scores - jnp.max(scores, axis=-1, keepdims=True))
            probs = (e / jnp.sum(e, axis=-1, keepdims=True)).astype(BF)
            o = jnp.dot(probs, v_buf[rows, :], preferred_element_type=F32).astype(BF)
            for j in range(GROUP):
                o_buf[l, rows, pl.ds(aligned(OUT_COLS * z + HEAD_DIM * j, 128), HEAD_DIM)] = o[j * SEQ : (j + 1) * SEQ]

    def project_out(l):
        def out_cols(n, carry):
            cols = pl.ds(aligned(256 * n, 256), 256)
            add_mine[l, :, cols] = jnp.dot(o_buf[l], wo[l, :, cols], preferred_element_type=F32)
            return carry

        lax.fori_loop(0, OUT_COLS // 256, out_cols, 0)

    def finish_attn(l):
        mid[:, left] = (res[:, left].astype(F32) + add_mine[l, mine, :]).astype(BF)
        mid[:, right] = (res[:, right].astype(F32) + add_got[l]).astype(BF)

    def seq_rows(l, k):
        return u_buf.at[l, pl.ds(aligned(SEQ * block(k), SEQ), SEQ), :]

    def ag_copy(l, k):
        return remote(seq_rows(l, 0), seq_rows(l, 0), ag_s.at[l, k - 1], ag_r.at[l, k - 1], plane(k))

    def ag_relay(l, k):
        return remote(seq_rows(l, k), seq_rows(l, k), ag_s.at[l, k], ag_r.at[l, k], plane(1))

    def ag_arrival(l, k):
        dst = seq_rows(l, k)
        return remote(dst, dst, ag_s.at[l, k - 1], ag_r.at[l, k - 1], plane(k))

    def gate_up(l, p, b):
        rows = pl.ds(aligned(256 * b, 256), 256)
        begin, size = PARTS[p]

        def columns(start, width):
            at = pl.ds(aligned(start, 128), width)
            u = u_buf[l, rows, :]
            gate = jnp.dot(u, wgu[l, 0, :, at], preferred_element_type=F32).astype(BF).astype(F32)
            up = jnp.dot(u, wgu[l, 1, :, at], preferred_element_type=F32).astype(BF).astype(F32)
            gated = (jax.nn.silu(gate) * up).astype(BF)
            place = start + lax.broadcasted_iota(jnp.int32, (256, width), 1)
            valid = (place >= first) & (place < last)
            z_buf[rows, at] = jnp.where(valid, gated, jnp.zeros_like(gated))

        def cols(n, carry):
            columns(begin + 256 * n, 256)
            return carry

        lax.fori_loop(0, size // 256, cols, 0)
        if size % 256:
            columns(begin + size - 128, 128)

    def down(l, b, half):
        rows = pl.ds(aligned(256 * b, 256), 256)

        def cols(n, carry):
            at = pl.ds(aligned(256 * n, 256), 256)
            part[b, :, at] = jnp.dot(z_buf[rows, :], wd[l, :, at], preferred_element_type=F32)
            return carry

        lax.fori_loop(3 * half, 3 * half + 3, cols, 0)

    A, B = slice(0, DIM // 2), slice(DIM // 2, DIM)

    def chip_rows(yy, xx):
        return pl.ds(aligned(SEQ * (2 * yy + xx), SEQ), SEQ)

    def rs_core(l, half):
        cols = (A, B)[half]
        sem = 7 if half else 0
        return remote(part.at[1 - c, :, cols], r1.at[l, :, cols], rs_s.at[l, sem], rs_r.at[l, sem], plane(1))

    def rs_a(l, yy):
        return remote(part.at[c, chip_rows(yy, 1 - x), A], r2a.at[l, yy], rs_s.at[l, 1 + yy], rs_r.at[l, 1 + yy], plane(2))

    def rs_b(l, xx):
        return remote(part.at[c, chip_rows(1 - y, xx), B], r2b.at[l, xx], rs_s.at[l, 3 + xx], rs_r.at[l, 3 + xx], plane(4))

    def rs_a_last(l):
        return remote(part.at[c, chip_rows(1 - y, x), A], r3a.at[l], rs_s.at[l, 5], rs_r.at[l, 5], plane(4))

    def rs_b_last(l):
        return remote(part.at[c, chip_rows(y, 1 - x), B], r3b.at[l], rs_s.at[l, 6], rs_r.at[l, 6], plane(2))

    gain_mine[...] = jnp.zeros_like(gain_mine)
    gain_mine[0:LAYERS, 0:ROWS] = an_ref[...].astype(F32)
    gain_mine[LAYERS : 2 * LAYERS, 0:ROWS] = mn_ref[...].astype(F32)
    gain_mine[...] = jnp.where(c == 1, pltpu.roll(gain_mine[...], ROWS, 1), gain_mine[...])
    for k in range(1, 8):
        go(gain_copy(k))
    send_attn(0)
    send_gu(0, 0, GU_EARLY)
    gains[me] = gain_mine[...]
    res[...] = x_ref[...]
    for k in range(1, 8):
        gain_arrival(k).wait_recv()
    for p in range(4):
        gain_rows[:, 384 * p : 384 * (p + 1)] = gains[2 * p] + gains[2 * p + 1]
    start_layer(0)
    relay_attn(0)
    send_gu(0, 0, GU_LATE)
    for l in range(LAYERS):
        start_own(l)

    sends = []
    for l in range(LAYERS):
        relay_gu(l, 0, RELAYS[0])
        relay_attn_across(l)
        await_attn(l, 0)
        swap_in_arrival(l).wait_recv()
        project(l)
        attend(l)
        go(swap_heads(l))
        relay_gu(l, 0, RELAYS[1])
        await_attn(l, 1)
        swap_heads_arrival(l).wait_recv()
        project_out(l)
        go(swap_out(l))
        relay_gu(l, 0, RELAYS[2])
        swap_out(l).wait_recv()
        finish_attn(l)
        u_buf[l, pl.ds(aligned(SEQ * block(0), SEQ), SEQ), :] = normed(mid, 2 + l)
        for k in (2, 4, 6, 1):
            go(ag_copy(l, k))
        send_gu(l, 1, GU_EARLY + GU_LATE)
        if l + 1 < LAYERS:
            send_attn(l + 1)
        relay_gu(l, 0, RELAYS[3])
        for k in CHIPS:
            ag_arrival(l, k).wait_recv()
            go(ag_relay(l, k))
        await_gu(l, 0)
        gate_up(l, 0, c)
        relay_gu(l, 1, RELAYS[0] + RELAYS[1])
        for k in (1, 3, 5, 7):
            ag_arrival(l, k).wait_recv()
        gate_up(l, 0, 1 - c)
        relay_gu(l, 1, RELAYS[2] + RELAYS[3])
        finish_wd(l)
        await_gu(l, 1)
        gate_up(l, 1, 1 - c)
        for copy in sends:
            copy.wait_send()
        sends = []

        def send(copy):
            copy.start()
            sends.append(copy)

        for half in range(2):
            down(l, 1 - c, half)
            send(rs_core(l, half))
        gate_up(l, 1, c)
        for half in range(2):
            down(l, c, half)
            cols = (A, B)[half]
            rs_core(l, half).wait_recv()
            part[c, :, cols] = part[c, :, cols] + r1[l, :, cols]
            for t in range(2):
                send((rs_a, rs_b)[half](l, t))
        for t in range(2):
            rs_a(l, t).wait_recv()
            part[c, chip_rows(t, x), A] = part[c, chip_rows(t, x), A] + r2a[l, t]
        send(rs_a_last(l))
        for t in range(2):
            rs_b(l, t).wait_recv()
            part[c, chip_rows(y, t), B] = part[c, chip_rows(y, t), B] + r2b[l, t]
        send(rs_b_last(l))
        if l + 1 < LAYERS:
            relay_attn(l + 1)
            send_gu(l + 1, 0, GU_EARLY + GU_LATE)
        out = y_ref if l + 1 == LAYERS else res
        rs_a_last(l).wait_recv()
        out[:, A] = (mid[:, A].astype(F32) + (part[c, chip_rows(y, x), A] + r3a[l])).astype(BF)
        rs_b_last(l).wait_recv()
        out[:, B] = (mid[:, B].astype(F32) + (part[c, chip_rows(y, x), B] + r3b[l])).astype(BF)
        if l + 1 < LAYERS:
            start_layer(l + 1)
    for copy in sends + started:
        copy.wait_send()


def solution(mesh):
    vmem = pl.BlockSpec(memory_space=pltpu.VMEM)
    hbm = pl.BlockSpec(memory_space=pl.ANY)
    dma = pltpu.SemaphoreType.DMA
    inv_freq = ROPE_THETA ** -(np.arange(HEAD_DIM // 2) * 2.0 / HEAD_DIM)
    angles = np.tile(np.arange(SEQ)[:, None] * inv_freq[None, :].astype(np.float32), (2, 1)).astype(np.float32)
    cos_table = np.concatenate([np.cos(angles), np.cos(angles)], axis=1)
    sin_table = np.concatenate([-np.sin(angles), np.sin(angles)], axis=1)

    def local_forward(hidden, attn_norm, w_q, w_k, w_v, w_o, mlp_norm, w_gate, w_up, w_down):
        heads = []
        for g in range(KV_HEADS):
            heads += [w_q[:, :, GROUP * g : GROUP * (g + 1)], w_k[:, :, g : g + 1], w_v[:, :, g : g + 1]]
        wqkv = jnp.concatenate(heads, axis=2).reshape(LAYERS, ROWS, KV_HEADS * GROUP_COLS)
        y = pl.pallas_call(
            kernel,
            out_shape=jax.ShapeDtypeStruct((SEQ, DIM), BF),
            in_specs=[vmem] * 5 + [hbm] * 5,
            out_specs=vmem,
            scratch_shapes=[
                pltpu.VMEM((8, 2 * ROWS), F32),
                pltpu.VMEM((8, 8, 2 * ROWS), F32),
                pltpu.VMEM((8, DIM), F32),
                pltpu.VMEM((LAYERS, DIM, GROUP_COLS), BF),
                pltpu.VMEM((LAYERS, DIM, OUT_COLS), BF),
                pltpu.VMEM((LAYERS, 2, DIM, WINDOW), BF),
                pltpu.VMEM((LAYERS, WINDOW, DIM), BF),
                pltpu.VMEM((LAYERS, 2, EDGE, DIM), BF),
                pltpu.VMEM((SEQ, DIM), BF),
                pltpu.VMEM((SEQ, DIM), BF),
                pltpu.VMEM((LAYERS, 2 * SEQ, DIM), BF),
                pltpu.VMEM((2, GROUP * SEQ, HEAD_DIM), BF),
                pltpu.VMEM((2 * SEQ, HEAD_DIM), BF),
                pltpu.VMEM((2 * SEQ, HEAD_DIM), BF),
                pltpu.VMEM((LAYERS, 2 * SEQ, DIM), BF),
                pltpu.VMEM((LAYERS, 2 * SEQ, OUT_COLS), F32),
                pltpu.VMEM((LAYERS, SEQ, OUT_COLS), F32),
                pltpu.VMEM((LAYERS, 8 * SEQ, DIM), BF),
                pltpu.VMEM((8 * SEQ, WINDOW), BF),
                pltpu.VMEM((2, 4 * SEQ, DIM), F32),
                pltpu.VMEM((LAYERS, 4 * SEQ, DIM), F32),
                pltpu.VMEM((LAYERS, 2, SEQ, DIM // 2), F32),
                pltpu.VMEM((LAYERS, 2, SEQ, DIM // 2), F32),
                pltpu.VMEM((LAYERS, SEQ, DIM // 2), F32),
                pltpu.VMEM((LAYERS, SEQ, DIM // 2), F32),
                dma((7,)), dma((7,)),
                dma((LAYERS, 2, 2)), dma((LAYERS, 2, 2)),
                dma((LAYERS, 2, 2)), dma((LAYERS, 2, 2)),
                dma((LAYERS, 2, 5)), dma((LAYERS, 2, 5)),
                dma((LAYERS, 3)), dma((LAYERS, 3)),
                dma((LAYERS, 2, 2, 7)), dma((LAYERS, 2, 2, 7)),
                dma((LAYERS, 2, 2, 6)), dma((LAYERS, 2, 2, 6)),
                dma((LAYERS,)), dma((LAYERS,)),
                dma((LAYERS, 7)), dma((LAYERS, 7)),
                dma((LAYERS, 8)), dma((LAYERS, 8)),
                dma((LAYERS, 2)), dma((LAYERS, 2)), dma((LAYERS, 2)),
            ],
            compiler_params=pltpu.CompilerParams(collective_id=0, has_side_effects=True, vmem_limit_bytes=67043328),
        )(hidden.reshape(SEQ, DIM), attn_norm, mlp_norm, jnp.asarray(cos_table), jnp.asarray(sin_table), wqkv, w_o, w_gate, w_up, w_down)
        return y.reshape(1, SEQ, DIM)

    batch_spec = P(("dp", "fsdp"), None, None)
    gain_spec = P(None, "fsdp")
    proj_spec = P(None, "fsdp", None, None)
    mat_spec = P(None, "fsdp", None)
    return jax.shard_map(local_forward, mesh=mesh, in_specs=(batch_spec, gain_spec, proj_spec, proj_spec, proj_spec, mat_spec, gain_spec, mat_spec, mat_spec, mat_spec), out_specs=batch_spec, check_vma=False)
```

```python
import functools

import jax
import jax.numpy as jnp
import numpy as np
from jax import lax
from jax.experimental import pallas as pl
from jax.experimental.pallas import tpu as pltpu
from jax.sharding import PartitionSpec as P

MESH = pl.DeviceIdType.MESH
ROPE_THETA = 500000.0
NORM_EPS = 1e-5
LAYERS = 2
SEQ = 64
DIM = 1536
HEADS = 12
KV_HEADS = 2
HEAD_DIM = 128
GROUP = HEADS // KV_HEADS
GROUP_COLS = (GROUP + 2) * HEAD_DIM
OUT_COLS = DIM // 2
FFN = 8960
ROWS = DIM // 8
FFN_ROWS = FFN // 8
WINDOW = 1152
MAIN = 1088
EDGE = 32
HALF = ROWS // 2
DIRECT = ((96, 144), (96, 144))
BF = jnp.bfloat16
F32 = jnp.float32
CHIPS = (2, 4, 6)
PARTS = ((0, 896), (896, 256))
GU_RELAYED = (2, 4, 3, 5, 6, 7)
RELAYS = (((2, 0), (4, 0)), ((2, 1), (4, 1)), ((6, 0), (6, 1), (3, 0), (5, 0)), ((3, 1), (5, 1), (7, 0), (7, 1)))
ONE = ((2, 0), (4, 0))
TWO = ((2, 1), (4, 1))
THREE = ((3, 0), (5, 0))
FOUR = ((3, 1), (5, 1))
FIVE = ((6, 0), (6, 1), (7, 0), (7, 1))
CORE = ((1, 0), (1, 1))


def aligned(value, size):
    return pl.multiple_of(value, size)


def kernel(x_ref, an_ref, mn_ref, cos_ref, sin_ref, wqkv_ref, wo_ref, wg_ref, wu_ref, wd_ref, y_ref,
           gain_mine, gains, gain_rows, wq, wo, wgu, wd, edge, res, mid, n_buf, q_buf, k_buf, v_buf, o_buf, add_mine, add_got, u_buf, z_buf, part,
           r1, r2a, r2b, r3a, r3b,
           gain_s, gain_r, ad_s, ad_r, ax_s, ax_r, ac_s, ac_r, zx_s, zx_r, gd_s, gd_r, gz_s, gz_r, ed_s, ed_r, ag_s, ag_r, rs_s, rs_r,
           own_a, own_gu, own_wd):
    z = lax.axis_index("dp")
    me = lax.axis_index("fsdp")
    c = me % 2
    x = (me // 2) % 2
    y = me // 4

    def peer(k):
        cc = 1 - c if k % 2 else c
        xx = 1 - x if (k // 2) % 2 else x
        yy = 1 - y if k // 4 else y
        return 4 * yy + 2 * xx + cc

    def block(k):
        cc = 1 - c if k % 2 else c
        xx = 1 - x if (k // 2) % 2 else x
        yy = 1 - y if k // 4 else y
        return 4 * cc + 2 * yy + xx

    def window(j):
        return aligned(128 * (35 * (j // 4) + 9 * (j % 4) - (j % 4) // 2), 128)

    def plane(k):
        return (z, peer(k))

    across = (1 - z, me)
    started = []

    def remote(src, dst, send, recv, device):
        return pltpu.make_async_remote_copy(src_ref=src, dst_ref=dst, send_sem=send, recv_sem=recv, device_id=device, device_id_type=MESH)

    def go(copy):
        copy.start()
        started.append(copy)

    barrier = pltpu.get_barrier_semaphore()
    for k in range(1, 8):
        pl.semaphore_signal(barrier, inc=1, device_id=plane(k), device_id_type=MESH)
    pl.semaphore_signal(barrier, inc=1, device_id=across, device_id_type=MESH)
    pl.semaphore_wait(barrier, 8)

    def gain_copy(k):
        return remote(gain_mine, gains.at[me], gain_s.at[k - 1], gain_r.at[k - 1], plane(k))

    def gain_arrival(k):
        dst = gains.at[peer(k)]
        return remote(dst, dst, gain_s.at[k - 1], gain_r.at[k - 1], plane(k))

    attn_src = (wqkv_ref, wo_ref)
    attn_dst = (wq, wo)
    attn_cols = (GROUP_COLS, OUT_COLS)

    def attn_rows(l, m, k, start=0, count=ROWS):
        return attn_dst[m].at[l, pl.ds(aligned(ROWS * peer(k) + start, 32), count), :]

    def attn_shard(l, m):
        return attn_src[m].at[l, :, pl.ds(aligned(attn_cols[m] * z, 128), attn_cols[m])]

    def attn_own(l, m):
        return pltpu.make_async_copy(attn_shard(l, m), attn_rows(l, m, 0), own_a.at[l, m])

    def attn_direct(l, m, n):
        return remote(attn_shard(l, m), attn_rows(l, m, 0), ad_s.at[l, m, n], ad_r.at[l, m, n], plane(2 + 2 * n))

    def attn_arrival(l, m, n):
        dst = attn_rows(l, m, 2 + 2 * n)
        return remote(dst, dst, ad_s.at[l, m, n], ad_r.at[l, m, n], plane(2 + 2 * n))

    def attn_turn(l, m, n):
        rows = attn_rows(l, m, 2 + 2 * n, HALF * n, HALF)
        return remote(rows, rows, ax_s.at[l, m, n], ax_r.at[l, m, n], plane(4 - 2 * n))

    def attn_turn_arrival(l, m, n):
        dst = attn_rows(l, m, 6, HALF * n, HALF)
        return remote(dst, dst, ax_s.at[l, m, n], ax_r.at[l, m, n], plane(4 - 2 * n))

    def attn_core(l, m, slot, k, *part_rows):
        rows = attn_rows(l, m, k, *part_rows)
        return remote(rows, rows, ac_s.at[l, m, slot], ac_r.at[l, m, slot], plane(1))

    def attn_core_own(l, m):
        return remote(attn_shard(l, m), attn_rows(l, m, 0), ac_s.at[l, m, 0], ac_r.at[l, m, 0], plane(1))

    def send_attn(l, m):
        for n in range(2):
            go(attn_direct(l, m, n))
        go(attn_core_own(l, m))
        attn_own(l, m).start()

    def relay_attn(l, m):
        for n in range(2):
            attn_arrival(l, m, n).wait_recv()
            go(attn_turn(l, m, n))
            go(attn_core(l, m, 1 + n, 2 + 2 * n))

    def relay_attn_across(l, m):
        for n in range(2):
            attn_turn_arrival(l, m, n).wait_recv()
            go(attn_core(l, m, 3 + n, 6, HALF * n, HALF))

    def await_attn(l, m):
        attn_own(l, m).wait()
        attn_core(l, m, 0, 1).wait_recv()
        for n in range(2):
            attn_core(l, m, 1 + n, 3 + 2 * n).wait_recv()
            attn_core(l, m, 3 + n, 7, HALF * n, HALF).wait_recv()

    halves = (wg_ref, wu_ref)

    def gu_rows(l, p, g, k, start, count):
        return wgu.at[l, g, pl.ds(aligned(ROWS * peer(k) + start, 16), count), pl.ds(*PARTS[p])]

    def gu_direct(l, p, g, k):
        start, count = (0, ROWS) if k == 1 else (aligned((ROWS - DIRECT[l][p]) * z, 16), DIRECT[l][p])
        src = halves[g].at[l, pl.ds(start, count), pl.ds(aligned(window(peer(k)) + PARTS[p][0], 128), PARTS[p][1])]
        return remote(src, gu_rows(l, p, g, 0, start, count), gd_s.at[l, p, g, k - 1], gd_r.at[l, p, g, k - 1], plane(k))

    def gu_arrival(l, p, g, k):
        start, count = (0, ROWS) if k == 1 else ((ROWS - DIRECT[l][p]) * z, DIRECT[l][p])
        dst = gu_rows(l, p, g, k, start, count)
        return remote(dst, dst, gd_s.at[l, p, g, k - 1], gd_r.at[l, p, g, k - 1], plane(k))

    def gu_across(l, p, g, k):
        rows = gu_rows(l, p, g, k, DIRECT[l][p] * z, ROWS - DIRECT[l][p])
        return remote(rows, rows, gz_s.at[l, p, g, k - 2], gz_r.at[l, p, g, k - 2], across)

    def gu_across_arrival(l, p, g, k):
        dst = gu_rows(l, p, g, k, DIRECT[l][p] * (1 - z), ROWS - DIRECT[l][p])
        return remote(dst, dst, gz_s.at[l, p, g, k - 2], gz_r.at[l, p, g, k - 2], across)

    def gu_own(l, g):
        dst = wgu.at[l, g, pl.ds(aligned(ROWS * me, 64), ROWS), :]
        return pltpu.make_async_copy(halves[g].at[l, :, pl.ds(window(me), WINDOW)], dst, own_gu.at[l, g])

    def send_gu(l, p, blocks):
        for k, g in blocks:
            go(gu_direct(l, p, g, k))

    def relay_gu(l, p, blocks):
        for k, g in blocks:
            gu_arrival(l, p, g, k).wait_recv()
            go(gu_across(l, p, g, k))

    def await_gu(l, p):
        for g in range(2):
            gu_arrival(l, p, g, 1).wait_recv()
            if p == 0:
                gu_own(l, g).wait()
        for k in GU_RELAYED:
            for g in range(2):
                gu_across_arrival(l, p, g, k).wait_recv()

    def start_own(l):
        for g in range(2):
            gu_own(l, g).start()
        wd_copy(l).start()
        edge_own(l).start()
        go(edge_core(l))

    def wd_copy(l):
        return pltpu.make_async_copy(wd_ref.at[l, pl.ds(aligned(EDGE * c, EDGE), MAIN), :], wd.at[l, pl.ds(aligned(2 * EDGE * x, EDGE), MAIN), :], own_wd.at[l, 0])

    def edge_own(l):
        return pltpu.make_async_copy(wd_ref.at[l, pl.ds(aligned(MAIN * (1 - x), EDGE), EDGE), :], edge.at[l, 0], own_wd.at[l, 1])

    def edge_core(l):
        return remote(wd_ref.at[l, pl.ds(aligned(MAIN * x, EDGE), EDGE), :], edge.at[l, 1], ed_s.at[l], ed_r.at[l], plane(1))

    takes = c == x

    def finish_wd(l):
        wd_copy(l).wait()
        edge_own(l).wait()
        edge_core(l).wait_recv()
        own, got = edge[l, 0], edge[l, 1]
        none = jnp.zeros_like(own)
        place = MAIN * (1 - x)
        wd[l, pl.ds(aligned(place, EDGE), EDGE), :] = jnp.where(takes, jnp.where(x == 0, own, got), none)
        wd[l, pl.ds(aligned(place + EDGE, EDGE), EDGE), :] = jnp.where(takes, jnp.where(x == 0, got, own), none)

    first = jnp.where(takes, 0, 2 * EDGE * x)
    last = jnp.where(takes, WINDOW, 2 * EDGE * x + MAIN)

    def normed(ref, row):
        wide = ref[...].astype(F32)
        inv_rms = lax.rsqrt(jnp.mean(wide * wide, axis=-1, keepdims=True) + NORM_EPS)
        return (wide * inv_rms * gain_rows[row : row + 1, :]).astype(BF)

    mine, other = pl.ds(aligned(SEQ * z, SEQ), SEQ), pl.ds(aligned(SEQ * (1 - z), SEQ), SEQ)
    left, right = pl.ds(aligned(OUT_COLS * z, 128), OUT_COLS), pl.ds(aligned(OUT_COLS * (1 - z), 128), OUT_COLS)

    def swap_in(l):
        rows = n_buf.at[l, mine, :]
        return remote(rows, rows, zx_s.at[l, 0], zx_r.at[l, 0], across)

    def swap_in_arrival(l):
        rows = n_buf.at[l, other, :]
        return remote(rows, rows, zx_s.at[l, 0], zx_r.at[l, 0], across)

    def swap_heads(l):
        cols = o_buf.at[l, :, left]
        return remote(cols, cols, zx_s.at[l, 1], zx_r.at[l, 1], across)

    def swap_heads_arrival(l):
        cols = o_buf.at[l, :, right]
        return remote(cols, cols, zx_s.at[l, 1], zx_r.at[l, 1], across)

    def swap_out(l):
        return remote(add_mine.at[l, other, :], add_got.at[l], zx_s.at[l, 2], zx_r.at[l, 2], across)

    def start_layer(l):
        n_buf[l, mine, :] = normed(res, l)
        go(swap_in(l))

    def project(l):
        cos, sin = cos_ref[...], sin_ref[...]

        def rotate(v):
            return (v * cos + pltpu.roll(v, HEAD_DIM // 2, 1) * sin).astype(BF)

        def two_heads(n):
            return jnp.dot(n_buf[l], wq[l, :, pl.ds(aligned(256 * n, 256), 256)], preferred_element_type=F32)

        def q_heads(n, carry):
            pair = two_heads(n)
            for t in range(2):
                turned = rotate(pair[:, 128 * t : 128 * (t + 1)])
                for seq in range(2):
                    q_buf[seq, pl.ds(aligned((2 * n + t) * SEQ, SEQ), SEQ), :] = turned[SEQ * seq : SEQ * (seq + 1)]
            return carry

        lax.fori_loop(0, GROUP // 2, q_heads, 0)
        pair = two_heads(GROUP // 2)
        k_buf[...] = rotate(pair[:, :128])
        v_buf[...] = pair[:, 128:].astype(BF)

    def attend(l):
        row = lax.broadcasted_iota(jnp.int32, (GROUP * SEQ, SEQ), 0) % SEQ
        col = lax.broadcasted_iota(jnp.int32, (GROUP * SEQ, SEQ), 1)
        for seq in range(2):
            rows = slice(SEQ * seq, SEQ * (seq + 1))
            scores = lax.dot_general(q_buf[seq], k_buf[rows, :], (((1,), (1,)), ((), ())), preferred_element_type=F32) * HEAD_DIM ** -0.5
            scores = jnp.where(row >= col, scores, -jnp.inf)
            e = jnp.exp(scores - jnp.max(scores, axis=-1, keepdims=True))
            probs = (e / jnp.sum(e, axis=-1, keepdims=True)).astype(BF)
            o = jnp.dot(probs, v_buf[rows, :], preferred_element_type=F32).astype(BF)
            for j in range(GROUP):
                o_buf[l, rows, pl.ds(aligned(OUT_COLS * z + HEAD_DIM * j, 128), HEAD_DIM)] = o[j * SEQ : (j + 1) * SEQ]

    def project_out(l):
        def out_cols(n, carry):
            cols = pl.ds(aligned(256 * n, 256), 256)
            add_mine[l, :, cols] = jnp.dot(o_buf[l], wo[l, :, cols], preferred_element_type=F32)
            return carry

        lax.fori_loop(0, OUT_COLS // 256, out_cols, 0)

    def finish_attn(l):
        mid[:, left] = (res[:, left].astype(F32) + add_mine[l, mine, :]).astype(BF)
        mid[:, right] = (res[:, right].astype(F32) + add_got[l]).astype(BF)

    def seq_rows(l, k):
        return u_buf.at[l, pl.ds(aligned(SEQ * block(k), SEQ), SEQ), :]

    def ag_copy(l, k):
        return remote(seq_rows(l, 0), seq_rows(l, 0), ag_s.at[l, k - 1], ag_r.at[l, k - 1], plane(k))

    def ag_relay(l, k):
        return remote(seq_rows(l, k), seq_rows(l, k), ag_s.at[l, k], ag_r.at[l, k], plane(1))

    def ag_arrival(l, k):
        dst = seq_rows(l, k)
        return remote(dst, dst, ag_s.at[l, k - 1], ag_r.at[l, k - 1], plane(k))

    def gate_up(l, p, b):
        rows = pl.ds(aligned(256 * b, 256), 256)
        begin, size = PARTS[p]

        def columns(start, width):
            at = pl.ds(aligned(start, 128), width)
            u = u_buf[l, rows, :]
            gate = jnp.dot(u, wgu[l, 0, :, at], preferred_element_type=F32).astype(BF).astype(F32)
            up = jnp.dot(u, wgu[l, 1, :, at], preferred_element_type=F32).astype(BF).astype(F32)
            gated = (jax.nn.silu(gate) * up).astype(BF)
            place = start + lax.broadcasted_iota(jnp.int32, (256, width), 1)
            valid = (place >= first) & (place < last)
            z_buf[rows, at] = jnp.where(valid, gated, jnp.zeros_like(gated))

        def cols(n, carry):
            columns(begin + 256 * n, 256)
            return carry

        lax.fori_loop(0, size // 256, cols, 0)
        if size % 256:
            columns(begin + size - 128, 128)

    def down(l, p, b, half):
        rows = pl.ds(aligned(256 * b, 256), 256)
        inner = pl.ds(*PARTS[p])

        def cols(n, carry):
            at = pl.ds(aligned(256 * n, 256), 256)
            add = jnp.dot(z_buf[rows, inner], wd[l, inner, at], preferred_element_type=F32)
            part[b, :, at] = add if p == 0 else part[b, :, at] + add
            return carry

        lax.fori_loop(3 * half, 3 * half + 3, cols, 0)

    A, B = slice(0, DIM // 2), slice(DIM // 2, DIM)

    def chip_rows(yy, xx):
        return pl.ds(aligned(SEQ * (2 * yy + xx), SEQ), SEQ)

    def rs_core(l, half):
        cols = (A, B)[half]
        sem = 7 if half else 0
        return remote(part.at[1 - c, :, cols], r1.at[l, :, cols], rs_s.at[l, sem], rs_r.at[l, sem], plane(1))

    def rs_a(l, yy):
        return remote(part.at[c, chip_rows(yy, 1 - x), A], r2a.at[l, yy], rs_s.at[l, 1 + yy], rs_r.at[l, 1 + yy], plane(2))

    def rs_b(l, xx):
        return remote(part.at[c, chip_rows(1 - y, xx), B], r2b.at[l, xx], rs_s.at[l, 3 + xx], rs_r.at[l, 3 + xx], plane(4))

    def rs_a_last(l):
        return remote(part.at[c, chip_rows(1 - y, x), A], r3a.at[l], rs_s.at[l, 5], rs_r.at[l, 5], plane(4))

    def rs_b_last(l):
        return remote(part.at[c, chip_rows(y, 1 - x), B], r3b.at[l], rs_s.at[l, 6], rs_r.at[l, 6], plane(2))

    sends = []

    def send(copy):
        copy.start()
        sends.append(copy)

    def attention(l):
        await_attn(l, 0)
        swap_in_arrival(l).wait_recv()
        project(l)
        attend(l)
        go(swap_heads(l))

    def attention_out(l):
        await_attn(l, 1)
        swap_heads_arrival(l).wait_recv()
        project_out(l)
        go(swap_out(l))

    def attention_end(l):
        swap_out(l).wait_recv()
        finish_attn(l)
        u_buf[l, pl.ds(aligned(SEQ * block(0), SEQ), SEQ), :] = normed(mid, 2 + l)
        for k in (2, 4, 6, 1):
            go(ag_copy(l, k))
        send_gu(l, 1, ONE + TWO + THREE + FOUR + FIVE + CORE)

    def mlp(l, relays):
        relay_gu(l, 0, relays)
        for k in CHIPS:
            ag_arrival(l, k).wait_recv()
            go(ag_relay(l, k))
        await_gu(l, 0)
        gate_up(l, 0, c)
        relay_gu(l, 1, ONE + TWO)
        for k in (1, 3, 5, 7):
            ag_arrival(l, k).wait_recv()
        gate_up(l, 0, 1 - c)
        relay_gu(l, 1, THREE + FOUR)
        while sends:
            sends.pop().wait_send()
        finish_wd(l)
        for half in range(2):
            down(l, 0, 1 - c, half)
        relay_gu(l, 1, FIVE)
        for half in range(2):
            down(l, 0, c, half)
        await_gu(l, 1)
        gate_up(l, 1, 1 - c)
        for half in range(2):
            down(l, 1, 1 - c, half)
            send(rs_core(l, half))

    def mlp_own(l):
        gate_up(l, 1, c)
        for half in range(2):
            down(l, 1, c, half)
            cols = (A, B)[half]
            rs_core(l, half).wait_recv()
            part[c, :, cols] = part[c, :, cols] + r1[l, :, cols]
            for t in range(2):
                send((rs_a, rs_b)[half](l, t))

    def rs_middle(l):
        for t in range(2):
            rs_a(l, t).wait_recv()
            part[c, chip_rows(t, x), A] = part[c, chip_rows(t, x), A] + r2a[l, t]
        send(rs_a_last(l))
        for t in range(2):
            rs_b(l, t).wait_recv()
            part[c, chip_rows(y, t), B] = part[c, chip_rows(y, t), B] + r2b[l, t]
        send(rs_b_last(l))

    def rs_end(l, out):
        rs_a_last(l).wait_recv()
        out[:, A] = (mid[:, A].astype(F32) + (part[c, chip_rows(y, x), A] + r3a[l])).astype(BF)
        rs_b_last(l).wait_recv()
        out[:, B] = (mid[:, B].astype(F32) + (part[c, chip_rows(y, x), B] + r3b[l])).astype(BF)

    gain_mine[...] = jnp.zeros_like(gain_mine)
    gain_mine[0:LAYERS, 0:ROWS] = an_ref[...].astype(F32)
    gain_mine[LAYERS : 2 * LAYERS, 0:ROWS] = mn_ref[...].astype(F32)
    gain_mine[...] = jnp.where(c == 1, pltpu.roll(gain_mine[...], ROWS, 1), gain_mine[...])
    for k in range(1, 8):
        go(gain_copy(k))
    send_gu(0, 0, ONE + TWO)
    send_attn(0, 0)
    send_attn(0, 1)
    gains[me] = gain_mine[...]
    res[...] = x_ref[...]
    for k in range(1, 8):
        gain_arrival(k).wait_recv()
    for p in range(4):
        gain_rows[:, 384 * p : 384 * (p + 1)] = gains[2 * p] + gains[2 * p + 1]
    start_layer(0)
    relay_gu(0, 0, ONE + TWO)
    relay_attn(0, 0)
    relay_attn(0, 1)
    send_gu(0, 0, THREE + FOUR + FIVE + CORE)
    for l in range(LAYERS):
        start_own(l)
    relay_attn_across(0, 0)
    attention(0)
    relay_attn_across(0, 1)
    relay_gu(0, 0, THREE)
    attention_out(0)
    relay_gu(0, 0, FOUR)
    attention_end(0)
    send_gu(1, 0, ONE)
    send_attn(1, 0)
    send_gu(1, 0, TWO)
    mlp(0, FIVE)
    relay_gu(1, 0, ONE)
    mlp_own(0)
    relay_gu(1, 0, TWO)
    relay_attn(1, 0)
    rs_middle(0)
    send_gu(1, 0, THREE + FOUR)
    send_attn(1, 1)
    relay_attn_across(1, 0)
    rs_end(0, res)
    start_layer(1)
    relay_gu(1, 0, THREE)
    attention(1)
    relay_gu(1, 0, FOUR)
    relay_attn(1, 1)
    send_gu(1, 0, FIVE + CORE)
    relay_attn_across(1, 1)
    attention_out(1)
    relay_gu(1, 0, FIVE[:2])
    attention_end(1)
    mlp(1, FIVE[2:])
    mlp_own(1)
    rs_middle(1)
    rs_end(1, y_ref)
    for copy in sends + started:
        copy.wait_send()


def solution(mesh):
    vmem = pl.BlockSpec(memory_space=pltpu.VMEM)
    hbm = pl.BlockSpec(memory_space=pl.ANY)
    dma = pltpu.SemaphoreType.DMA
    inv_freq = ROPE_THETA ** -(np.arange(HEAD_DIM // 2) * 2.0 / HEAD_DIM)
    angles = np.tile(np.arange(SEQ)[:, None] * inv_freq[None, :].astype(np.float32), (2, 1)).astype(np.float32)
    cos_table = np.concatenate([np.cos(angles), np.cos(angles)], axis=1)
    sin_table = np.concatenate([-np.sin(angles), np.sin(angles)], axis=1)

    def local_forward(hidden, attn_norm, w_q, w_k, w_v, w_o, mlp_norm, w_gate, w_up, w_down):
        heads = []
        for g in range(KV_HEADS):
            heads += [w_q[:, :, GROUP * g : GROUP * (g + 1)], w_k[:, :, g : g + 1], w_v[:, :, g : g + 1]]
        wqkv = jnp.concatenate(heads, axis=2).reshape(LAYERS, ROWS, KV_HEADS * GROUP_COLS)
        y = pl.pallas_call(
            kernel,
            out_shape=jax.ShapeDtypeStruct((SEQ, DIM), BF),
            in_specs=[vmem] * 5 + [hbm] * 5,
            out_specs=vmem,
            scratch_shapes=[
                pltpu.VMEM((8, 2 * ROWS), F32),
                pltpu.VMEM((8, 8, 2 * ROWS), F32),
                pltpu.VMEM((8, DIM), F32),
                pltpu.VMEM((LAYERS, DIM, GROUP_COLS), BF),
                pltpu.VMEM((LAYERS, DIM, OUT_COLS), BF),
                pltpu.VMEM((LAYERS, 2, DIM, WINDOW), BF),
                pltpu.VMEM((LAYERS, WINDOW, DIM), BF),
                pltpu.VMEM((LAYERS, 2, EDGE, DIM), BF),
                pltpu.VMEM((SEQ, DIM), BF),
                pltpu.VMEM((SEQ, DIM), BF),
                pltpu.VMEM((LAYERS, 2 * SEQ, DIM), BF),
                pltpu.VMEM((2, GROUP * SEQ, HEAD_DIM), BF),
                pltpu.VMEM((2 * SEQ, HEAD_DIM), BF),
                pltpu.VMEM((2 * SEQ, HEAD_DIM), BF),
                pltpu.VMEM((LAYERS, 2 * SEQ, DIM), BF),
                pltpu.VMEM((LAYERS, 2 * SEQ, OUT_COLS), F32),
                pltpu.VMEM((LAYERS, SEQ, OUT_COLS), F32),
                pltpu.VMEM((LAYERS, 8 * SEQ, DIM), BF),
                pltpu.VMEM((8 * SEQ, WINDOW), BF),
                pltpu.VMEM((2, 4 * SEQ, DIM), F32),
                pltpu.VMEM((LAYERS, 4 * SEQ, DIM), F32),
                pltpu.VMEM((LAYERS, 2, SEQ, DIM // 2), F32),
                pltpu.VMEM((LAYERS, 2, SEQ, DIM // 2), F32),
                pltpu.VMEM((LAYERS, SEQ, DIM // 2), F32),
                pltpu.VMEM((LAYERS, SEQ, DIM // 2), F32),
                dma((7,)), dma((7,)),
                dma((LAYERS, 2, 2)), dma((LAYERS, 2, 2)),
                dma((LAYERS, 2, 2)), dma((LAYERS, 2, 2)),
                dma((LAYERS, 2, 5)), dma((LAYERS, 2, 5)),
                dma((LAYERS, 3)), dma((LAYERS, 3)),
                dma((LAYERS, 2, 2, 7)), dma((LAYERS, 2, 2, 7)),
                dma((LAYERS, 2, 2, 6)), dma((LAYERS, 2, 2, 6)),
                dma((LAYERS,)), dma((LAYERS,)),
                dma((LAYERS, 7)), dma((LAYERS, 7)),
                dma((LAYERS, 8)), dma((LAYERS, 8)),
                dma((LAYERS, 2)), dma((LAYERS, 2)), dma((LAYERS, 2)),
            ],
            compiler_params=pltpu.CompilerParams(collective_id=0, has_side_effects=True, vmem_limit_bytes=67043328),
        )(hidden.reshape(SEQ, DIM), attn_norm, mlp_norm, jnp.asarray(cos_table), jnp.asarray(sin_table), wqkv, w_o, w_gate, w_up, w_down)
        return y.reshape(1, SEQ, DIM)

    batch_spec = P(("dp", "fsdp"), None, None)
    gain_spec = P(None, "fsdp")
    proj_spec = P(None, "fsdp", None, None)
    mat_spec = P(None, "fsdp", None)
    return jax.shard_map(local_forward, mesh=mesh, in_specs=(batch_spec, gain_spec, proj_spec, proj_spec, proj_spec, mat_spec, gain_spec, mat_spec, mat_spec, mat_spec), out_specs=batch_spec, check_vma=False)
```

```python
import functools

import jax
import jax.numpy as jnp
import numpy as np
from jax import lax
from jax.experimental import pallas as pl
from jax.experimental.pallas import tpu as pltpu
from jax.sharding import PartitionSpec as P

MESH = pl.DeviceIdType.MESH
ROPE_THETA = 500000.0
NORM_EPS = 1e-5
LAYERS = 2
SEQ = 64
DIM = 1536
HEADS = 12
KV_HEADS = 2
HEAD_DIM = 128
LANES = 128
TILE = 256
GROUP = HEADS // KV_HEADS
OUT_COLS = DIM // 2
FFN = 8960
ROWS = DIM // 8
FFN_ROWS = FFN // 8
WINDOW = 1152
MAIN = 1088
EDGE = 32
HALF = ROWS // 2
DIRECT = ((96, 128), (96, 128))
BF = jnp.bfloat16
F32 = jnp.float32
PARTS = ((0, 768), (768, 384))
GU_RELAYED = (2, 4, 3, 5, 6, 7)
RELAYS = (((2, 0), (4, 0)), ((2, 1), (4, 1)), ((6, 0), (6, 1), (3, 0), (5, 0)), ((3, 1), (5, 1), (7, 0), (7, 1)))
ONE, TWO, THREE, FOUR = [tuple((k, g) for k in pair) for pair in ((2, 4), (3, 5)) for g in (0, 1)]
FIVE = tuple((k, g) for k in (6, 7) for g in (0, 1))
CORE = ((1, 0), (1, 1))
KINDS = ((2, 0), (1,))


def aligned(value, size):
    return pl.multiple_of(value, size)


def kernel(x_ref, an_ref, mn_ref, cos_ref, sin_ref, wq_ref, wo_ref, wkv_ref, wg_ref, wu_ref, wd_ref, y_ref,
           gain_mine, gains, gain_rows, wq, wo, wkv, wgu, wd, edge, res, mid, n_buf, q_buf, k_buf, v_buf, o_buf, add_mine, add_got, u_buf, z_buf, part,
           r1, r2a, r2b, r3a, r3b,
           gain_s, gain_r, ad_s, ad_r, ax_s, ax_r, ac_s, ac_r, zx_s, zx_r, gd_s, gd_r, gz_s, gz_r, ed_s, ed_r, ag_s, ag_r, rs_s, rs_r,
           own_a, own_gu, own_wd):
    z = lax.axis_index("dp")
    me = lax.axis_index("fsdp")
    c = me % 2
    x = (me // 2) % 2
    y = me // 4

    def place(k):
        flips = (k % 2, (k // 2) % 2, k // 4)
        return [1 - own if flip else own for own, flip in zip((c, x, y), flips)]

    def peer(k):
        cc, xx, yy = place(k)
        return 4 * yy + 2 * xx + cc

    def block(k):
        cc, xx, yy = place(k)
        return 4 * cc + 2 * yy + xx

    def window(j):
        return aligned(LANES * (35 * (j // 4) + 9 * (j % 4) - (j % 4) // 2), LANES)

    def plane(k):
        return (z, peer(k))

    across = (1 - z, me)
    started = []

    def remote(src, dst, send, recv, device):
        return pltpu.make_async_remote_copy(src_ref=src, dst_ref=dst, send_sem=send, recv_sem=recv, device_id=device, device_id_type=MESH)

    def go(copy):
        copy.start()
        started.append(copy)

    barrier = pltpu.get_barrier_semaphore()
    for k in range(1, 8):
        pl.semaphore_signal(barrier, inc=1, device_id=plane(k), device_id_type=MESH)
    pl.semaphore_signal(barrier, inc=1, device_id=across, device_id_type=MESH)
    pl.semaphore_wait(barrier, 8)

    def gain_copy(k):
        return remote(gain_mine, gains.at[me], gain_s.at[k - 1], gain_r.at[k - 1], plane(k))

    def gain_arrival(k):
        dst = gains.at[peer(k)]
        return remote(dst, dst, gain_s.at[k - 1], gain_r.at[k - 1], plane(k))

    attn_src = (wq_ref, wo_ref, wkv_ref)
    attn_dst = (wq, wo, wkv)
    share = (GROUP, OUT_COLS, KV_HEADS)

    def attn_rows(l, m, k, start=0, count=ROWS):
        rows = pl.ds(aligned(ROWS * peer(k) + start, 32), count)
        return attn_dst[m].at[l, rows, :] if m == 1 else attn_dst[m].at[l, :, rows, :]

    def attn_shard(l, m):
        if m == 1:
            return attn_src[m].at[l, :, pl.ds(aligned(share[m] * z, LANES), share[m])]
        return attn_src[m].at[l, pl.ds(share[m] * z, share[m]), :, :]

    def attn_own(l, m):
        return pltpu.make_async_copy(attn_shard(l, m), attn_rows(l, m, 0), own_a.at[l, m])

    def attn_direct(l, m, n):
        return remote(attn_shard(l, m), attn_rows(l, m, 0), ad_s.at[l, m, n], ad_r.at[l, m, n], plane(2 + 2 * n))

    def attn_arrival(l, m, n):
        dst = attn_rows(l, m, 2 + 2 * n)
        return remote(dst, dst, ad_s.at[l, m, n], ad_r.at[l, m, n], plane(2 + 2 * n))

    def attn_turn(l, m, n):
        rows = attn_rows(l, m, 2 + 2 * n, HALF * n, HALF)
        return remote(rows, rows, ax_s.at[l, m, n], ax_r.at[l, m, n], plane(4 - 2 * n))

    def attn_turn_arrival(l, m, n):
        dst = attn_rows(l, m, 6, HALF * n, HALF)
        return remote(dst, dst, ax_s.at[l, m, n], ax_r.at[l, m, n], plane(4 - 2 * n))

    def attn_core(l, m, slot, k, *part_rows):
        rows = attn_rows(l, m, k, *part_rows)
        return remote(rows, rows, ac_s.at[l, m, slot], ac_r.at[l, m, slot], plane(1))

    def attn_core_own(l, m):
        return remote(attn_shard(l, m), attn_rows(l, m, 0), ac_s.at[l, m, 0], ac_r.at[l, m, 0], plane(1))

    def send_attn(l, out):
        for m in KINDS[out]:
            for n in range(2):
                go(attn_direct(l, m, n))
            go(attn_core_own(l, m))
            attn_own(l, m).start()

    def relay_attn(l, out):
        for m in KINDS[out]:
            for n in range(2):
                attn_arrival(l, m, n).wait_recv()
                go(attn_turn(l, m, n))
                go(attn_core(l, m, 1 + n, 2 + 2 * n))

    def relay_attn_across(l, out):
        for m in KINDS[out]:
            for n in range(2):
                attn_turn_arrival(l, m, n).wait_recv()
                go(attn_core(l, m, 3 + n, 6, HALF * n, HALF))

    def await_attn(l, out):
        for m in KINDS[out]:
            attn_own(l, m).wait()
            attn_core(l, m, 0, 1).wait_recv()
            for n in range(2):
                attn_core(l, m, 1 + n, 3 + 2 * n).wait_recv()
                attn_core(l, m, 3 + n, 7, HALF * n, HALF).wait_recv()

    halves = (wg_ref, wu_ref)

    def gu_rows(l, p, g, k, start, count):
        return wgu.at[l, g, pl.ds(aligned(ROWS * peer(k) + start, 16), count), pl.ds(*PARTS[p])]

    def gu_direct(l, p, g, k):
        start, count = (0, ROWS) if k == 1 else (aligned((ROWS - DIRECT[l][p]) * z, 16), DIRECT[l][p])
        src = halves[g].at[l, pl.ds(start, count), pl.ds(aligned(window(peer(k)) + PARTS[p][0], LANES), PARTS[p][1])]
        return remote(src, gu_rows(l, p, g, 0, start, count), gd_s.at[l, p, g, k - 1], gd_r.at[l, p, g, k - 1], plane(k))

    def gu_arrival(l, p, g, k):
        start, count = (0, ROWS) if k == 1 else ((ROWS - DIRECT[l][p]) * z, DIRECT[l][p])
        dst = gu_rows(l, p, g, k, start, count)
        return remote(dst, dst, gd_s.at[l, p, g, k - 1], gd_r.at[l, p, g, k - 1], plane(k))

    def gu_across(l, p, g, k):
        rows = gu_rows(l, p, g, k, DIRECT[l][p] * z, ROWS - DIRECT[l][p])
        return remote(rows, rows, gz_s.at[l, p, g, k - 2], gz_r.at[l, p, g, k - 2], across)

    def gu_across_arrival(l, p, g, k):
        dst = gu_rows(l, p, g, k, DIRECT[l][p] * (1 - z), ROWS - DIRECT[l][p])
        return remote(dst, dst, gz_s.at[l, p, g, k - 2], gz_r.at[l, p, g, k - 2], across)

    def gu_own(l, g):
        dst = wgu.at[l, g, pl.ds(aligned(ROWS * me, 64), ROWS), :]
        return pltpu.make_async_copy(halves[g].at[l, :, pl.ds(window(me), WINDOW)], dst, own_gu.at[l, g])

    def send_gu(l, p, blocks):
        for k, g in blocks:
            go(gu_direct(l, p, g, k))

    def relay_gu(l, p, blocks):
        for k, g in blocks:
            gu_arrival(l, p, g, k).wait_recv()
            go(gu_across(l, p, g, k))

    def await_gu(l, p):
        for g in range(2):
            gu_arrival(l, p, g, 1).wait_recv()
            if p == 0:
                gu_own(l, g).wait()
        for k in GU_RELAYED:
            for g in range(2):
                gu_across_arrival(l, p, g, k).wait_recv()

    def start_own(l):
        for g in range(2):
            gu_own(l, g).start()
        wd_copy(l).start()
        edge_own(l).start()
        go(edge_core(l))

    def wd_copy(l):
        return pltpu.make_async_copy(wd_ref.at[l, pl.ds(aligned(EDGE * c, EDGE), MAIN), :], wd.at[l, pl.ds(aligned(2 * EDGE * x, EDGE), MAIN), :], own_wd.at[l, 0])

    def edge_own(l):
        return pltpu.make_async_copy(wd_ref.at[l, pl.ds(aligned(MAIN * (1 - x), EDGE), EDGE), :], edge.at[l, 0], own_wd.at[l, 1])

    def edge_core(l):
        return remote(wd_ref.at[l, pl.ds(aligned(MAIN * x, EDGE), EDGE), :], edge.at[l, 1], ed_s.at[l], ed_r.at[l], plane(1))

    takes = c == x

    def finish_wd(l):
        wd_copy(l).wait()
        edge_own(l).wait()
        edge_core(l).wait_recv()
        own, got = edge[l, 0], edge[l, 1]
        none = jnp.zeros_like(own)
        edge_row = MAIN * (1 - x)
        wd[l, pl.ds(aligned(edge_row, EDGE), EDGE), :] = jnp.where(takes, jnp.where(x == 0, own, got), none)
        wd[l, pl.ds(aligned(edge_row + EDGE, EDGE), EDGE), :] = jnp.where(takes, jnp.where(x == 0, got, own), none)

    first = jnp.where(takes, 0, 2 * EDGE * x)
    last = jnp.where(takes, WINDOW, 2 * EDGE * x + MAIN)

    def normed(ref, row):
        wide = ref[...].astype(F32)
        inv_rms = lax.rsqrt(jnp.mean(wide * wide, axis=-1, keepdims=True) + NORM_EPS)
        return (wide * inv_rms * gain_rows[row : row + 1, :]).astype(BF)

    mine, other = pl.ds(aligned(SEQ * z, SEQ), SEQ), pl.ds(aligned(SEQ * (1 - z), SEQ), SEQ)
    left, right = pl.ds(aligned(OUT_COLS * z, LANES), OUT_COLS), pl.ds(aligned(OUT_COLS * (1 - z), LANES), OUT_COLS)

    def swap_in(l):
        rows = n_buf.at[l, mine, :]
        return remote(rows, rows, zx_s.at[l, 0], zx_r.at[l, 0], across)

    def swap_in_arrival(l):
        rows = n_buf.at[l, other, :]
        return remote(rows, rows, zx_s.at[l, 0], zx_r.at[l, 0], across)

    def swap_heads(l):
        cols = o_buf.at[l, :, left]
        return remote(cols, cols, zx_s.at[l, 1], zx_r.at[l, 1], across)

    def swap_heads_arrival(l):
        cols = o_buf.at[l, :, right]
        return remote(cols, cols, zx_s.at[l, 1], zx_r.at[l, 1], across)

    def swap_out(l):
        return remote(add_mine.at[l, other, :], add_got.at[l], zx_s.at[l, 2], zx_r.at[l, 2], across)

    def start_layer(l):
        n_buf[l, mine, :] = normed(res, l)
        go(swap_in(l))

    def project(l):
        cos, sin = cos_ref[...], sin_ref[...]

        def rotate(v):
            return (v * cos + pltpu.roll(v, HEAD_DIM // 2, 1) * sin).astype(BF)

        def two_heads(n):
            pair = (wkv[l, 0], wkv[l, 1]) if n is None else (wq[l, 2 * n], wq[l, 2 * n + 1])
            return jnp.dot(n_buf[l], jnp.concatenate(pair, axis=1), preferred_element_type=F32)

        def q_heads(n, carry):
            pair = two_heads(n)
            for t in range(2):
                turned = rotate(pair[:, LANES * t : LANES * (t + 1)])
                for seq in range(2):
                    q_buf[seq, pl.ds(aligned((2 * n + t) * SEQ, SEQ), SEQ), :] = turned[SEQ * seq : SEQ * (seq + 1)]
            return carry

        lax.fori_loop(0, GROUP // 2, q_heads, 0)
        pair = two_heads(None)
        k_buf[...] = rotate(pair[:, :LANES])
        v_buf[...] = pair[:, LANES:].astype(BF)

    def attend(l):
        row = lax.broadcasted_iota(jnp.int32, (GROUP * SEQ, SEQ), 0) % SEQ
        col = lax.broadcasted_iota(jnp.int32, (GROUP * SEQ, SEQ), 1)
        for seq in range(2):
            rows = slice(SEQ * seq, SEQ * (seq + 1))
            scores = lax.dot_general(q_buf[seq], k_buf[rows, :], (((1,), (1,)), ((), ())), preferred_element_type=F32) * HEAD_DIM ** -0.5
            scores = jnp.where(row >= col, scores, -jnp.inf)
            e = jnp.exp(scores - jnp.max(scores, axis=-1, keepdims=True))
            probs = (e / jnp.sum(e, axis=-1, keepdims=True)).astype(BF)
            o = jnp.dot(probs, v_buf[rows, :], preferred_element_type=F32).astype(BF)
            for j in range(GROUP):
                o_buf[l, rows, pl.ds(aligned(OUT_COLS * z + HEAD_DIM * j, LANES), HEAD_DIM)] = o[j * SEQ : (j + 1) * SEQ]

    def project_out(l):
        def out_cols(n, carry):
            cols = pl.ds(aligned(TILE * n, TILE), TILE)
            add_mine[l, :, cols] = jnp.dot(o_buf[l], wo[l, :, cols], preferred_element_type=F32)
            return carry

        lax.fori_loop(0, OUT_COLS // TILE, out_cols, 0)

    def finish_attn(l):
        mid[:, left] = (res[:, left].astype(F32) + add_mine[l, mine, :]).astype(BF)
        mid[:, right] = (res[:, right].astype(F32) + add_got[l]).astype(BF)

    def seq_rows(l, k, start=0, count=SEQ):
        return u_buf.at[l, pl.ds(aligned(SEQ * block(k) + start, 32), count), :]

    def ag(l, sem, k, to, *rows):
        part_rows = seq_rows(l, k, *rows)
        return remote(part_rows, part_rows, ag_s.at[l, sem], ag_r.at[l, sem], plane(to))

    def ag_half(n):
        return SEQ // 2 * n, SEQ // 2

    def ag_start(l):
        for n in range(2):
            go(ag(l, n, 0, 2 + 2 * n))
        go(ag(l, 2, 0, 1))

    def ag_turn(l):
        for n in range(2):
            k = 2 + 2 * n
            ag(l, n, k, k).wait_recv()
            go(ag(l, 5 + n, k, 6 - k, *ag_half(n)))
            go(ag(l, 3 + n, k, 1))

    def ag_across(l):
        for n in range(2):
            ag(l, 5 + n, 6, 4 - 2 * n, *ag_half(n)).wait_recv()
            go(ag(l, 7 + n, 6, 1, *ag_half(n)))

    def ag_end(l):
        ag(l, 2, 1, 1).wait_recv()
        for n in range(2):
            ag(l, 3 + n, 3 + 2 * n, 1).wait_recv()
            ag(l, 7 + n, 7, 1, *ag_half(n)).wait_recv()

    def gate_up(l, p, b):
        rows = pl.ds(aligned(TILE * b, TILE), TILE)
        begin, size = PARTS[p]

        def columns(start, width):
            at = pl.ds(aligned(start, LANES), width)
            u = u_buf[l, rows, :]
            gate = jnp.dot(u, wgu[l, 0, :, at], preferred_element_type=F32).astype(BF).astype(F32)
            up = jnp.dot(u, wgu[l, 1, :, at], preferred_element_type=F32).astype(BF).astype(F32)
            gated = (jax.nn.silu(gate) * up).astype(BF)
            spot = start + lax.broadcasted_iota(jnp.int32, (TILE, width), 1)
            valid = (spot >= first) & (spot < last)
            z_buf[rows, at] = jnp.where(valid, gated, jnp.zeros_like(gated))

        def cols(n, carry):
            columns(begin + TILE * n, TILE)
            return carry

        lax.fori_loop(0, size // TILE, cols, 0)
        if size % TILE:
            columns(begin + size - LANES, LANES)

    def down(l, p, b, half):
        rows = pl.ds(aligned(TILE * b, TILE), TILE)
        inner = pl.ds(*PARTS[p])

        def cols(n, carry):
            at = pl.ds(aligned(TILE * n, TILE), TILE)
            add = jnp.dot(z_buf[rows, inner], wd[l, inner, at], preferred_element_type=F32)
            part[b, :, at] = add if p == 0 else part[b, :, at] + add
            return carry

        lax.fori_loop(3 * half, 3 * half + 3, cols, 0)

    A, B = slice(0, DIM // 2), slice(DIM // 2, DIM)

    def chip_rows(yy, xx):
        return pl.ds(aligned(SEQ * (2 * yy + xx), SEQ), SEQ)

    def rs_core(l, half):
        cols = (A, B)[half]
        sem = 7 if half else 0
        return remote(part.at[1 - c, :, cols], r1.at[l, :, cols], rs_s.at[l, sem], rs_r.at[l, sem], plane(1))

    def rs_a(l, t):
        return remote(part.at[c, chip_rows((1 - y, y)[t], 1 - x), A], r2a.at[l, t], rs_s.at[l, 1 + t], rs_r.at[l, 1 + t], plane(2))

    def rs_b(l, t):
        return remote(part.at[c, chip_rows(1 - y, (1 - x, x)[t]), B], r2b.at[l, t], rs_s.at[l, 3 + t], rs_r.at[l, 3 + t], plane(4))

    def rs_a_last(l):
        return remote(part.at[c, chip_rows(1 - y, x), A], r3a.at[l], rs_s.at[l, 5], rs_r.at[l, 5], plane(4))

    def rs_b_last(l):
        return remote(part.at[c, chip_rows(y, 1 - x), B], r3b.at[l], rs_s.at[l, 6], rs_r.at[l, 6], plane(2))

    sends = []

    def send(copy):
        copy.start()
        sends.append(copy)

    def attention(l):
        await_attn(l, 0)
        swap_in_arrival(l).wait_recv()
        project(l)
        attend(l)
        go(swap_heads(l))

    def attention_out(l):
        await_attn(l, 1)
        swap_heads_arrival(l).wait_recv()
        project_out(l)
        go(swap_out(l))

    def attention_end(l):
        swap_out(l).wait_recv()
        finish_attn(l)
        u_buf[l, pl.ds(aligned(SEQ * block(0), SEQ), SEQ), :] = normed(mid, 2 + l)
        ag_start(l)
        send_gu(l, 1, ONE + TWO)

    def mlp(l, relays):
        relay_gu(l, 0, relays)
        ag_turn(l)
        send_gu(l, 1, THREE + FOUR + FIVE + CORE)
        if l + 1 < LAYERS:
            send_gu(l + 1, 0, ONE)
            send_attn(l + 1, 0)
            send_gu(l + 1, 0, TWO)
        relay_gu(l, 1, ONE + TWO)
        ag_across(l)
        await_gu(l, 0)
        gate_up(l, 0, c)
        relay_gu(l, 1, THREE)
        ag_end(l)
        gate_up(l, 0, 1 - c)
        relay_gu(l, 1, FOUR)
        while sends:
            sends.pop().wait_send()
        finish_wd(l)
        for half in range(2):
            down(l, 0, 1 - c, half)
        relay_gu(l, 1, FIVE)
        for half in range(2):
            down(l, 0, c, half)
        await_gu(l, 1)
        gate_up(l, 1, 1 - c)
        for half in range(2):
            down(l, 1, 1 - c, half)
            send(rs_core(l, half))

    def mlp_own(l):
        gate_up(l, 1, c)
        for half in range(2):
            down(l, 1, c, half)
            cols = (A, B)[half]
            rs_core(l, half).wait_recv()
            part[c, :, cols] = part[c, :, cols] + r1[l, :, cols]
            for t in range(2):
                send((rs_a, rs_b)[half](l, t))

    def rs_add(l, t):
        row_a, row_b = chip_rows((1 - y, y)[t], x), chip_rows(y, (1 - x, x)[t])
        rs_a(l, t).wait_recv()
        part[c, row_a, A] = part[c, row_a, A] + r2a[l, t]
        if t == 0:
            send(rs_a_last(l))
        rs_b(l, t).wait_recv()
        part[c, row_b, B] = part[c, row_b, B] + r2b[l, t]
        if t == 0:
            send(rs_b_last(l))

    def rs_middle(l):
        for t in range(2):
            rs_add(l, t)

    def rs_end(l, out):
        rs_a_last(l).wait_recv()
        out[:, A] = (mid[:, A].astype(F32) + (part[c, chip_rows(y, x), A] + r3a[l])).astype(BF)
        rs_b_last(l).wait_recv()
        out[:, B] = (mid[:, B].astype(F32) + (part[c, chip_rows(y, x), B] + r3b[l])).astype(BF)

    gain_mine[...] = jnp.zeros_like(gain_mine)
    gain_mine[0:LAYERS, 0:ROWS] = an_ref[...].astype(F32)
    gain_mine[LAYERS : 2 * LAYERS, 0:ROWS] = mn_ref[...].astype(F32)
    gain_mine[...] = jnp.where(c == 1, pltpu.roll(gain_mine[...], ROWS, 1), gain_mine[...])
    for k in range(1, 8):
        go(gain_copy(k))
    send_gu(0, 0, ONE + TWO + THREE)
    for m in range(2):
        send_attn(0, m)
    gains[me] = gain_mine[...]
    res[...] = x_ref[...]
    for k in range(1, 8):
        gain_arrival(k).wait_recv()
    for p in range(4):
        gain_rows[:, 384 * p : 384 * (p + 1)] = gains[2 * p] + gains[2 * p + 1]
    start_layer(0)
    relay_gu(0, 0, ONE + TWO + THREE)
    for m in range(2):
        relay_attn(0, m)
    send_gu(0, 0, FOUR + FIVE + CORE)
    for l in range(LAYERS):
        start_own(l)
    relay_attn_across(0, 0)
    attention(0)
    relay_attn_across(0, 1)
    attention_out(0)
    relay_gu(0, 0, FOUR + FIVE[:2])
    attention_end(0)
    mlp(0, FIVE[2:])
    relay_gu(1, 0, ONE)
    mlp_own(0)
    relay_gu(1, 0, TWO)
    relay_attn(1, 0)
    rs_middle(0)
    send_attn(1, 1)
    send_gu(1, 0, THREE)
    relay_attn_across(1, 0)
    rs_end(0, res)
    start_layer(1)
    attention(1)
    relay_attn(1, 1)
    send_gu(1, 0, FOUR + FIVE + CORE)
    relay_gu(1, 0, THREE)
    relay_attn_across(1, 1)
    attention_out(1)
    relay_gu(1, 0, FOUR)
    attention_end(1)
    mlp(1, FIVE)
    mlp_own(1)
    rs_middle(1)
    rs_end(1, y_ref)
    for copy in sends + started:
        copy.wait_send()


def solution(mesh):
    vmem = pl.BlockSpec(memory_space=pltpu.VMEM)
    hbm = pl.BlockSpec(memory_space=pl.ANY)
    dma = pltpu.SemaphoreType.DMA
    pairs = [(7,), (LAYERS, 3, 2), (LAYERS, 3, 2), (LAYERS, 3, 5), (LAYERS, 3), (LAYERS, 2, 2, 7), (LAYERS, 2, 2, 6), (LAYERS,), (LAYERS, 9), (LAYERS, 8)]
    inv_freq = ROPE_THETA ** -(np.arange(HEAD_DIM // 2) * 2.0 / HEAD_DIM)
    angles = np.tile(np.arange(SEQ)[:, None] * inv_freq[None, :].astype(np.float32), (2, 1)).astype(np.float32)
    cos_table = np.concatenate([np.cos(angles), np.cos(angles)], axis=1)
    sin_table = np.concatenate([-np.sin(angles), np.sin(angles)], axis=1)

    def local_forward(hidden, attn_norm, w_q, w_k, w_v, w_o, mlp_norm, w_gate, w_up, w_down):
        wq = w_q.transpose(0, 2, 1, 3)
        wkv = jnp.stack([w_k, w_v], axis=3).reshape(LAYERS, ROWS, 2 * KV_HEADS, HEAD_DIM).transpose(0, 2, 1, 3)
        y = pl.pallas_call(
            kernel,
            out_shape=jax.ShapeDtypeStruct((SEQ, DIM), BF),
            in_specs=[vmem] * 5 + [hbm] * 6,
            out_specs=vmem,
            scratch_shapes=[
                pltpu.VMEM((8, 2 * ROWS), F32),
                pltpu.VMEM((8, 8, 2 * ROWS), F32),
                pltpu.VMEM((8, DIM), F32),
                pltpu.VMEM((LAYERS, GROUP, DIM, HEAD_DIM), BF),
                pltpu.VMEM((LAYERS, DIM, OUT_COLS), BF),
                pltpu.VMEM((LAYERS, KV_HEADS, DIM, HEAD_DIM), BF),
                pltpu.VMEM((LAYERS, 2, DIM, WINDOW), BF),
                pltpu.VMEM((LAYERS, WINDOW, DIM), BF),
                pltpu.VMEM((LAYERS, 2, EDGE, DIM), BF),
                pltpu.VMEM((SEQ, DIM), BF),
                pltpu.VMEM((SEQ, DIM), BF),
                pltpu.VMEM((LAYERS, 2 * SEQ, DIM), BF),
                pltpu.VMEM((2, GROUP * SEQ, HEAD_DIM), BF),
                pltpu.VMEM((2 * SEQ, HEAD_DIM), BF),
                pltpu.VMEM((2 * SEQ, HEAD_DIM), BF),
                pltpu.VMEM((LAYERS, 2 * SEQ, DIM), BF),
                pltpu.VMEM((LAYERS, 2 * SEQ, OUT_COLS), F32),
                pltpu.VMEM((LAYERS, SEQ, OUT_COLS), F32),
                pltpu.VMEM((LAYERS, 8 * SEQ, DIM), BF),
                pltpu.VMEM((8 * SEQ, WINDOW), BF),
                pltpu.VMEM((2, 4 * SEQ, DIM), F32),
                pltpu.VMEM((LAYERS, 4 * SEQ, DIM), F32),
                pltpu.VMEM((LAYERS, 2, SEQ, DIM // 2), F32),
                pltpu.VMEM((LAYERS, 2, SEQ, DIM // 2), F32),
                pltpu.VMEM((LAYERS, SEQ, DIM // 2), F32),
                pltpu.VMEM((LAYERS, SEQ, DIM // 2), F32),
            ] + [dma(shape) for shape in pairs for end in range(2)] + [dma((LAYERS, 3))] * 3,
            compiler_params=pltpu.CompilerParams(collective_id=0, has_side_effects=True, vmem_limit_bytes=67043328),
        )(hidden.reshape(SEQ, DIM), attn_norm, mlp_norm, jnp.asarray(cos_table), jnp.asarray(sin_table), wq, w_o, wkv, w_gate, w_up, w_down)
        return y.reshape(1, SEQ, DIM)

    batch_spec = P(("dp", "fsdp"), None, None)
    gain_spec = P(None, "fsdp")
    proj_spec = P(None, "fsdp", None, None)
    mat_spec = P(None, "fsdp", None)
    return jax.shard_map(local_forward, mesh=mesh, in_specs=(batch_spec, gain_spec, proj_spec, proj_spec, proj_spec, mat_spec, gain_spec, mat_spec, mat_spec, mat_spec), out_specs=batch_spec, check_vma=False)
```

```python
import functools

import jax
import jax.numpy as jnp
import numpy as np
from jax import lax
from jax.experimental import pallas as pl
from jax.experimental.pallas import tpu as pltpu
from jax.sharding import PartitionSpec as P

MESH = pl.DeviceIdType.MESH
ROPE_THETA = 500000.0
NORM_EPS = 1e-5
LAYERS = 2
SEQ = 64
DIM = 1536
HEADS = 12
KV_HEADS = 2
HEAD_DIM = 128
LANES = 128
TILE = 256
GROUP = HEADS // KV_HEADS
OUT_COLS = DIM // 2
FFN = 8960
ROWS = DIM // 8
FFN_ROWS = FFN // 8
WINDOW = 1152
MAIN = 1088
EDGE = 32
HALF = ROWS // 2
DIRECT = ((96, 128), (96, 128))
BF = jnp.bfloat16
BOTH = range(2)
F32 = jnp.float32
PARTS = ((0, 768), (768, 384))
GU_RELAYED = (2, 4, 3, 5, 6, 7)
RELAYS = (((2, 0), (4, 0)), ((2, 1), (4, 1)), ((6, 0), (6, 1), (3, 0), (5, 0)), ((3, 1), (5, 1), (7, 0), (7, 1)))
ONE, TWO, THREE, FOUR = [tuple((k, g) for k in pair) for pair in ((2, 4), (3, 5)) for g in (0, 1)]
FIVE = tuple((k, g) for k in (6, 7) for g in (0, 1))
CORE = ((1, 0), (1, 1))
KINDS = ((2, 3, 0), (1,))


def aligned(value, size):
    return pl.multiple_of(value, size)


def kernel(x_ref, an_ref, mn_ref, cos_ref, sin_ref, wq_ref, wo_ref, wk_ref, wv_ref, wg_ref, wu_ref, wd_ref, y_ref,
           gain_mine, gains, gain_rows, wq, wo, wkv, wgu, wd, edge, res, mid, n_buf, q_buf, k_buf, v_buf, o_buf, add_mine, add_got, u_buf, z_buf, part,
           r1, r2a, r2b, r3a, r3b,
           gain_s, gain_r, ad_s, ad_r, ax_s, ax_r, ac_s, ac_r, zx_s, zx_r, gd_s, gd_r, gz_s, gz_r, ed_s, ed_r, ag_s, ag_r, rs_s, rs_r,
           own_a, own_gu, own_wd):
    z = lax.axis_index("dp")
    me = lax.axis_index("fsdp")
    c = me % 2
    x = (me // 2) % 2
    y = me // 4

    def place(k):
        flips = (k % 2, (k // 2) % 2, k // 4)
        return [1 - own if flip else own for own, flip in zip((c, x, y), flips)]

    def peer(k):
        cc, xx, yy = place(k)
        return 4 * yy + 2 * xx + cc

    def block(k):
        cc, xx, yy = place(k)
        return 4 * cc + 2 * yy + xx

    def window(j):
        return aligned(LANES * (35 * (j // 4) + 9 * (j % 4) - (j % 4) // 2), LANES)

    def plane(k):
        return (z, peer(k))

    across = (1 - z, me)
    started = []

    def remote(src, dst, send, recv, device):
        return pltpu.make_async_remote_copy(src_ref=src, dst_ref=dst, send_sem=send, recv_sem=recv, device_id=device, device_id_type=MESH)

    def go(copy):
        copy.start()
        started.append(copy)

    barrier = pltpu.get_barrier_semaphore()
    for k in range(1, 8):
        pl.semaphore_signal(barrier, inc=1, device_id=plane(k), device_id_type=MESH)
    pl.semaphore_signal(barrier, inc=1, device_id=across, device_id_type=MESH)
    pl.semaphore_wait(barrier, 8)

    def gain_copy(k):
        return remote(gain_mine, gains.at[me], gain_s.at[k - 1], gain_r.at[k - 1], plane(k))

    def gain_arrival(k):
        dst = gains.at[peer(k)]
        return remote(dst, dst, gain_s.at[k - 1], gain_r.at[k - 1], plane(k))

    attn_src = (wq_ref, wo_ref, wk_ref, wv_ref)
    share = (GROUP, OUT_COLS, 1, 1)
    attn_dst = (wq, wo, wkv, wkv)
    heads_at = (pl.ds(0, GROUP), None, pl.ds(0, 1), pl.ds(1, 1))

    def attn_rows(l, m, k, start=0, count=ROWS):
        rows = pl.ds(aligned(ROWS * peer(k) + start, 32), count)
        return attn_dst[m].at[l, rows, :] if m == 1 else attn_dst[m].at[l, heads_at[m], rows, :]

    def attn_shard(l, m):
        if m == 1:
            return attn_src[m].at[l, :, pl.ds(aligned(share[m] * z, LANES), share[m])]
        return attn_src[m].at[l, pl.ds(share[m] * z, share[m]), :, :]

    def attn_own(l, m):
        return pltpu.make_async_copy(attn_shard(l, m), attn_rows(l, m, 0), own_a.at[l, m])

    def attn_direct(l, m, n):
        return remote(attn_shard(l, m), attn_rows(l, m, 0), ad_s.at[l, m, n], ad_r.at[l, m, n], plane(2 + 2 * n))

    def attn_arrival(l, m, n):
        dst = attn_rows(l, m, 2 + 2 * n)
        return remote(dst, dst, ad_s.at[l, m, n], ad_r.at[l, m, n], plane(2 + 2 * n))

    def attn_turn(l, m, n):
        rows = attn_rows(l, m, 2 + 2 * n, HALF * n, HALF)
        return remote(rows, rows, ax_s.at[l, m, n], ax_r.at[l, m, n], plane(4 - 2 * n))

    def attn_turn_arrival(l, m, n):
        dst = attn_rows(l, m, 6, HALF * n, HALF)
        return remote(dst, dst, ax_s.at[l, m, n], ax_r.at[l, m, n], plane(4 - 2 * n))

    def attn_core(l, m, slot, k, *part_rows):
        rows = attn_rows(l, m, k, *part_rows)
        return remote(rows, rows, ac_s.at[l, m, slot], ac_r.at[l, m, slot], plane(1))

    def attn_core_own(l, m):
        return remote(attn_shard(l, m), attn_rows(l, m, 0), ac_s.at[l, m, 0], ac_r.at[l, m, 0], plane(1))

    def send_attn(l, out):
        for m in KINDS[out]:
            for n in BOTH:
                go(attn_direct(l, m, n))
            go(attn_core_own(l, m))
            attn_own(l, m).start()

    def relay_attn(l, out):
        for m in KINDS[out]:
            for n in BOTH:
                attn_arrival(l, m, n).wait_recv()
                go(attn_turn(l, m, n))
                go(attn_core(l, m, 1 + n, 2 + 2 * n))

    def relay_attn_across(l, out):
        for m in KINDS[out]:
            for n in BOTH:
                attn_turn_arrival(l, m, n).wait_recv()
                go(attn_core(l, m, 3 + n, 6, HALF * n, HALF))

    def await_attn(l, out):
        for m in KINDS[out]:
            attn_own(l, m).wait()
            attn_core(l, m, 0, 1).wait_recv()
            for n in BOTH:
                attn_core(l, m, 1 + n, 3 + 2 * n).wait_recv()
                attn_core(l, m, 3 + n, 7, HALF * n, HALF).wait_recv()

    halves = (wg_ref, wu_ref)

    def gu_rows(l, p, g, k, start, count):
        return wgu.at[l, g, pl.ds(aligned(ROWS * peer(k) + start, 16), count), pl.ds(*PARTS[p])]

    def gu_direct(l, p, g, k):
        start, count = (0, ROWS) if k == 1 else (aligned((ROWS - DIRECT[l][p]) * z, 16), DIRECT[l][p])
        src = halves[g].at[l, pl.ds(start, count), pl.ds(aligned(window(peer(k)) + PARTS[p][0], LANES), PARTS[p][1])]
        return remote(src, gu_rows(l, p, g, 0, start, count), gd_s.at[l, p, g, k - 1], gd_r.at[l, p, g, k - 1], plane(k))

    def gu_arrival(l, p, g, k):
        start, count = (0, ROWS) if k == 1 else ((ROWS - DIRECT[l][p]) * z, DIRECT[l][p])
        dst = gu_rows(l, p, g, k, start, count)
        return remote(dst, dst, gd_s.at[l, p, g, k - 1], gd_r.at[l, p, g, k - 1], plane(k))

    def gu_across(l, p, g, k):
        rows = gu_rows(l, p, g, k, DIRECT[l][p] * z, ROWS - DIRECT[l][p])
        return remote(rows, rows, gz_s.at[l, p, g, k - 2], gz_r.at[l, p, g, k - 2], across)

    def gu_across_arrival(l, p, g, k):
        dst = gu_rows(l, p, g, k, DIRECT[l][p] * (1 - z), ROWS - DIRECT[l][p])
        return remote(dst, dst, gz_s.at[l, p, g, k - 2], gz_r.at[l, p, g, k - 2], across)

    def gu_own(l, g):
        dst = wgu.at[l, g, pl.ds(aligned(ROWS * me, 64), ROWS), :]
        return pltpu.make_async_copy(halves[g].at[l, :, pl.ds(window(me), WINDOW)], dst, own_gu.at[l, g])

    def send_gu(l, p, blocks):
        for k, g in blocks:
            go(gu_direct(l, p, g, k))

    def relay_gu(l, p, blocks):
        for k, g in blocks:
            gu_arrival(l, p, g, k).wait_recv()
            go(gu_across(l, p, g, k))

    def await_gu(l, p):
        for g in BOTH:
            gu_arrival(l, p, g, 1).wait_recv()
            if p == 0:
                gu_own(l, g).wait()
        for k in GU_RELAYED:
            for g in BOTH:
                gu_across_arrival(l, p, g, k).wait_recv()

    def start_own(l):
        for g in BOTH:
            gu_own(l, g).start()
        wd_copy(l).start()
        edge_own(l).start()
        go(edge_core(l))

    def wd_copy(l):
        return pltpu.make_async_copy(wd_ref.at[l, pl.ds(aligned(EDGE * c, EDGE), MAIN), :], wd.at[l, pl.ds(aligned(2 * EDGE * x, EDGE), MAIN), :], own_wd.at[l, 0])

    def edge_own(l):
        return pltpu.make_async_copy(wd_ref.at[l, pl.ds(aligned(MAIN * (1 - x), EDGE), EDGE), :], edge.at[l, 0], own_wd.at[l, 1])

    def edge_core(l):
        return remote(wd_ref.at[l, pl.ds(aligned(MAIN * x, EDGE), EDGE), :], edge.at[l, 1], ed_s.at[l], ed_r.at[l], plane(1))

    takes = c == x

    def finish_wd(l):
        wd_copy(l).wait()
        edge_own(l).wait()
        edge_core(l).wait_recv()
        own, got = edge[l, 0], edge[l, 1]
        none = jnp.zeros_like(own)
        edge_row = MAIN * (1 - x)
        wd[l, pl.ds(aligned(edge_row, EDGE), EDGE), :] = jnp.where(takes, jnp.where(x == 0, own, got), none)
        wd[l, pl.ds(aligned(edge_row + EDGE, EDGE), EDGE), :] = jnp.where(takes, jnp.where(x == 0, got, own), none)

    first = jnp.where(takes, 0, 2 * EDGE * x)
    last = jnp.where(takes, WINDOW, 2 * EDGE * x + MAIN)

    def normed(ref, row):
        wide = ref[...].astype(F32)
        inv_rms = lax.rsqrt(jnp.mean(wide * wide, axis=-1, keepdims=True) + NORM_EPS)
        return (wide * inv_rms * gain_rows[row : row + 1, :]).astype(BF)

    mine, other = pl.ds(aligned(SEQ * z, SEQ), SEQ), pl.ds(aligned(SEQ * (1 - z), SEQ), SEQ)
    left, right = pl.ds(aligned(OUT_COLS * z, LANES), OUT_COLS), pl.ds(aligned(OUT_COLS * (1 - z), LANES), OUT_COLS)

    def swap_in(l):
        rows = n_buf.at[l, mine, :]
        return remote(rows, rows, zx_s.at[l, 0], zx_r.at[l, 0], across)

    def swap_in_arrival(l):
        rows = n_buf.at[l, other, :]
        return remote(rows, rows, zx_s.at[l, 0], zx_r.at[l, 0], across)

    def swap_heads(l):
        cols = o_buf.at[l, :, left]
        return remote(cols, cols, zx_s.at[l, 1], zx_r.at[l, 1], across)

    def swap_heads_arrival(l):
        cols = o_buf.at[l, :, right]
        return remote(cols, cols, zx_s.at[l, 1], zx_r.at[l, 1], across)

    def swap_out(l):
        return remote(add_mine.at[l, other, :], add_got.at[l], zx_s.at[l, 2], zx_r.at[l, 2], across)

    def start_layer(l):
        n_buf[l, mine, :] = normed(res, l)
        go(swap_in(l))

    def project(l):
        cos, sin = cos_ref[...], sin_ref[...]

        def rotate(v):
            return (v * cos + pltpu.roll(v, HEAD_DIM // 2, 1) * sin).astype(BF)

        def two_heads(n):
            pair = (wkv[l, 0], wkv[l, 1]) if n is None else (wq[l, 2 * n], wq[l, 2 * n + 1])
            return jnp.dot(n_buf[l], jnp.concatenate(pair, axis=1), preferred_element_type=F32)

        def q_heads(n, carry):
            pair = two_heads(n)
            for t in BOTH:
                turned = rotate(pair[:, LANES * t : LANES * (t + 1)])
                for seq in BOTH:
                    q_buf[seq, pl.ds(aligned((2 * n + t) * SEQ, SEQ), SEQ), :] = turned[SEQ * seq : SEQ * (seq + 1)]
            return carry

        lax.fori_loop(0, GROUP // 2, q_heads, 0)
        pair = two_heads(None)
        k_buf[...] = rotate(pair[:, :LANES])
        v_buf[...] = pair[:, LANES:].astype(BF)

    def attend(l):
        row = lax.broadcasted_iota(jnp.int32, (GROUP * SEQ, SEQ), 0) % SEQ
        col = lax.broadcasted_iota(jnp.int32, (GROUP * SEQ, SEQ), 1)
        for seq in BOTH:
            rows = slice(SEQ * seq, SEQ * (seq + 1))
            scores = lax.dot_general(q_buf[seq], k_buf[rows, :], (((1,), (1,)), ((), ())), preferred_element_type=F32) * HEAD_DIM ** -0.5
            scores = jnp.where(row >= col, scores, -jnp.inf)
            e = jnp.exp(scores - jnp.max(scores, axis=-1, keepdims=True))
            probs = (e / jnp.sum(e, axis=-1, keepdims=True)).astype(BF)
            o = jnp.dot(probs, v_buf[rows, :], preferred_element_type=F32).astype(BF)
            for j in range(GROUP):
                o_buf[l, rows, pl.ds(aligned(OUT_COLS * z + HEAD_DIM * j, LANES), HEAD_DIM)] = o[j * SEQ : (j + 1) * SEQ]

    def project_out(l):
        def out_cols(n, carry):
            cols = pl.ds(aligned(TILE * n, TILE), TILE)
            add_mine[l, :, cols] = jnp.dot(o_buf[l], wo[l, :, cols], preferred_element_type=F32)
            return carry

        lax.fori_loop(0, OUT_COLS // TILE, out_cols, 0)

    def finish_attn(l):
        mid[:, left] = (res[:, left].astype(F32) + add_mine[l, mine, :]).astype(BF)
        mid[:, right] = (res[:, right].astype(F32) + add_got[l]).astype(BF)

    def seq_rows(l, k, start=0, count=SEQ):
        return u_buf.at[l, pl.ds(aligned(SEQ * block(k) + start, 32), count), :]

    def ag(l, sem, k, to, *rows):
        part_rows = seq_rows(l, k, *rows)
        return remote(part_rows, part_rows, ag_s.at[l, sem], ag_r.at[l, sem], plane(to))

    def ag_half(n):
        return SEQ // 2 * n, SEQ // 2

    def ag_start(l):
        for n in BOTH:
            go(ag(l, n, 0, 2 + 2 * n))
        go(ag(l, 2, 0, 1))

    def ag_turn(l):
        for n in BOTH:
            k = 2 + 2 * n
            ag(l, n, k, k).wait_recv()
            go(ag(l, 5 + n, k, 6 - k, *ag_half(n)))
            go(ag(l, 3 + n, k, 1))

    def ag_across(l):
        for n in BOTH:
            ag(l, 5 + n, 6, 4 - 2 * n, *ag_half(n)).wait_recv()
            go(ag(l, 7 + n, 6, 1, *ag_half(n)))

    def ag_end(l):
        ag(l, 2, 1, 1).wait_recv()
        for n in BOTH:
            ag(l, 3 + n, 3 + 2 * n, 1).wait_recv()
            ag(l, 7 + n, 7, 1, *ag_half(n)).wait_recv()

    def gate_up(l, p, b):
        rows = pl.ds(aligned(TILE * b, TILE), TILE)
        begin, size = PARTS[p]

        def columns(start, width):
            at = pl.ds(aligned(start, LANES), width)
            u = u_buf[l, rows, :]
            gate = jnp.dot(u, wgu[l, 0, :, at], preferred_element_type=F32).astype(BF).astype(F32)
            up = jnp.dot(u, wgu[l, 1, :, at], preferred_element_type=F32).astype(BF).astype(F32)
            gated = (jax.nn.silu(gate) * up).astype(BF)
            spot = start + lax.broadcasted_iota(jnp.int32, (TILE, width), 1)
            valid = (spot >= first) & (spot < last)
            z_buf[rows, at] = jnp.where(valid, gated, jnp.zeros_like(gated))

        def cols(n, carry):
            columns(begin + TILE * n, TILE)
            return carry

        lax.fori_loop(0, size // TILE, cols, 0)
        if size % TILE:
            columns(begin + size - LANES, LANES)

    def down(l, p, b, half):
        rows = pl.ds(aligned(TILE * b, TILE), TILE)
        inner = pl.ds(*PARTS[p])

        def cols(n, carry):
            at = pl.ds(aligned(TILE * n, TILE), TILE)
            add = jnp.dot(z_buf[rows, inner], wd[l, inner, at], preferred_element_type=F32)
            part[b, :, at] = add if p == 0 else part[b, :, at] + add
            return carry

        lax.fori_loop(3 * half, 3 * half + 3, cols, 0)

    A, B = slice(DIM // 2), slice(DIM // 2, DIM)

    def chip_rows(yy, xx):
        return pl.ds(aligned(SEQ * (2 * yy + xx), SEQ), SEQ)

    def rs_core(l, half):
        cols = (A, B)[half]
        sem = 7 if half else 0
        return remote(part.at[1 - c, :, cols], r1.at[l, :, cols], rs_s.at[l, sem], rs_r.at[l, sem], plane(1))

    def rs_a(l, t):
        return remote(part.at[c, chip_rows((1 - y, y)[t], 1 - x), A], r2a.at[l, t], rs_s.at[l, 1 + t], rs_r.at[l, 1 + t], plane(2))

    def rs_b(l, t):
        return remote(part.at[c, chip_rows(1 - y, (1 - x, x)[t]), B], r2b.at[l, t], rs_s.at[l, 3 + t], rs_r.at[l, 3 + t], plane(4))

    def rs_a_last(l):
        return remote(part.at[c, chip_rows(1 - y, x), A], r3a.at[l], rs_s.at[l, 5], rs_r.at[l, 5], plane(4))

    def rs_b_last(l):
        return remote(part.at[c, chip_rows(y, 1 - x), B], r3b.at[l], rs_s.at[l, 6], rs_r.at[l, 6], plane(2))

    sends = []

    def send(copy):
        copy.start()
        sends.append(copy)

    def attention(l):
        await_attn(l, 0)
        swap_in_arrival(l).wait_recv()
        project(l)
        attend(l)
        go(swap_heads(l))

    def attention_out(l):
        await_attn(l, 1)
        swap_heads_arrival(l).wait_recv()
        project_out(l)
        go(swap_out(l))

    def attention_end(l):
        swap_out(l).wait_recv()
        finish_attn(l)
        u_buf[l, pl.ds(aligned(SEQ * block(0), SEQ), SEQ), :] = normed(mid, 2 + l)
        ag_start(l)
        send_gu(l, 1, ONE + TWO)

    def mlp(l, relays):
        relay_gu(l, 0, relays)
        ag_turn(l)
        send_gu(l, 1, THREE + FOUR + FIVE + CORE)
        if l + 1 < LAYERS:
            send_gu(l + 1, 0, ONE)
            send_attn(l + 1, 0)
            send_gu(l + 1, 0, TWO)
        relay_gu(l, 1, ONE + TWO)
        ag_across(l)
        await_gu(l, 0)
        gate_up(l, 0, c)
        relay_gu(l, 1, THREE)
        ag_end(l)
        gate_up(l, 0, 1 - c)
        relay_gu(l, 1, FOUR[:1] + FIVE[:2])
        while sends:
            sends.pop().wait_send()
        finish_wd(l)
        for half in BOTH:
            down(l, 0, 1 - c, half)
        relay_gu(l, 1, FOUR[1:] + FIVE[2:])
        for half in BOTH:
            down(l, 0, c, half)
        await_gu(l, 1)
        gate_up(l, 1, 1 - c)
        for half in BOTH:
            down(l, 1, 1 - c, half)
            send(rs_core(l, half))

    def mlp_own(l):
        gate_up(l, 1, c)
        for half in BOTH:
            down(l, 1, c, half)
            cols = (A, B)[half]
            rs_core(l, half).wait_recv()
            part[c, :, cols] = part[c, :, cols] + r1[l, :, cols]
            for t in BOTH:
                send((rs_a, rs_b)[half](l, t))

    def rs_add(l, t):
        row_a, row_b = chip_rows((1 - y, y)[t], x), chip_rows(y, (1 - x, x)[t])
        rs_a(l, t).wait_recv()
        part[c, row_a, A] = part[c, row_a, A] + r2a[l, t]
        if t == 0:
            send(rs_a_last(l))
        rs_b(l, t).wait_recv()
        part[c, row_b, B] = part[c, row_b, B] + r2b[l, t]
        if t == 0:
            send(rs_b_last(l))

    def rs_middle(l):
        for t in BOTH:
            rs_add(l, t)

    def rs_end(l, out):
        rs_a_last(l).wait_recv()
        out[:, A] = (mid[:, A].astype(F32) + (part[c, chip_rows(y, x), A] + r3a[l])).astype(BF)
        rs_b_last(l).wait_recv()
        out[:, B] = (mid[:, B].astype(F32) + (part[c, chip_rows(y, x), B] + r3b[l])).astype(BF)

    gain_mine[...] = jnp.zeros_like(gain_mine)
    gain_mine[:LAYERS, :ROWS] = an_ref[...].astype(F32)
    gain_mine[LAYERS : 2 * LAYERS, :ROWS] = mn_ref[...].astype(F32)
    gain_mine[...] = jnp.where(c == 1, pltpu.roll(gain_mine[...], ROWS, 1), gain_mine[...])
    for k in range(1, 8):
        go(gain_copy(k))
    send_gu(0, 0, ONE + TWO + THREE)
    for m in BOTH:
        send_attn(0, m)
    gains[me] = gain_mine[...]
    res[...] = x_ref[...]
    for k in range(1, 8):
        gain_arrival(k).wait_recv()
    for p in range(4):
        gain_rows[:, 384 * p : 384 * (p + 1)] = gains[2 * p] + gains[2 * p + 1]
    start_layer(0)
    relay_gu(0, 0, ONE + TWO + THREE)
    for m in BOTH:
        relay_attn(0, m)
    send_gu(0, 0, FOUR + FIVE + CORE)
    for l in range(LAYERS):
        start_own(l)
    relay_attn_across(0, 0)
    attention(0)
    relay_attn_across(0, 1)
    attention_out(0)
    relay_gu(0, 0, FOUR + FIVE[:2])
    attention_end(0)
    mlp(0, FIVE[2:])
    relay_gu(1, 0, ONE)
    mlp_own(0)
    relay_gu(1, 0, TWO)
    relay_attn(1, 0)
    rs_middle(0)
    send_gu(1, 0, THREE)
    send_attn(1, 1)
    relay_attn_across(1, 0)
    rs_end(0, res)
    start_layer(1)
    attention(1)
    relay_attn(1, 1)
    send_gu(1, 0, FOUR + FIVE + CORE)
    relay_gu(1, 0, THREE)
    relay_attn_across(1, 1)
    attention_out(1)
    relay_gu(1, 0, FOUR[:1])
    attention_end(1)
    mlp(1, FIVE[:1] + FOUR[1:] + FIVE[1:])
    mlp_own(1)
    rs_middle(1)
    rs_end(1, y_ref)
    for copy in sends + started:
        copy.wait_send()


def solution(mesh):
    vmem = pl.BlockSpec(memory_space=pltpu.VMEM)
    hbm = pl.BlockSpec(memory_space=pl.ANY)
    dma = pltpu.SemaphoreType.DMA
    pairs = [(7,), (LAYERS, 4, 2), (LAYERS, 4, 2), (LAYERS, 4, 5), (LAYERS, 3), (LAYERS, 2, 2, 7), (LAYERS, 2, 2, 6), (LAYERS,), (LAYERS, 9), (LAYERS, 8)]
    inv_freq = ROPE_THETA ** -(np.arange(HEAD_DIM // 2) * 2.0 / HEAD_DIM)
    angles = np.tile(np.arange(SEQ)[:, None] * inv_freq[None, :].astype(np.float32), (2, 1)).astype(np.float32)
    cos_table = np.concatenate([np.cos(angles), np.cos(angles)], axis=1)
    sin_table = np.concatenate([-np.sin(angles), np.sin(angles)], axis=1)

    def local_forward(hidden, attn_norm, w_q, w_k, w_v, w_o, mlp_norm, w_gate, w_up, w_down):
        wq = w_q.transpose(0, 2, 1, 3)
        wk, wv = w_k.transpose(0, 2, 1, 3), w_v.transpose(0, 2, 1, 3)
        y = pl.pallas_call(
            kernel,
            out_shape=jax.ShapeDtypeStruct((SEQ, DIM), BF),
            in_specs=[vmem] * 5 + [hbm] * 7,
            out_specs=vmem,
            scratch_shapes=[
                pltpu.VMEM((8, 2 * ROWS), F32),
                pltpu.VMEM((8, 8, 2 * ROWS), F32),
                pltpu.VMEM((8, DIM), F32),
                pltpu.VMEM((LAYERS, GROUP, DIM, HEAD_DIM), BF),
                pltpu.VMEM((LAYERS, DIM, OUT_COLS), BF),
                pltpu.VMEM((LAYERS, KV_HEADS, DIM, HEAD_DIM), BF),
                pltpu.VMEM((LAYERS, 2, DIM, WINDOW), BF),
                pltpu.VMEM((LAYERS, WINDOW, DIM), BF),
                pltpu.VMEM((LAYERS, 2, EDGE, DIM), BF),
                pltpu.VMEM((SEQ, DIM), BF),
                pltpu.VMEM((SEQ, DIM), BF),
                pltpu.VMEM((LAYERS, 2 * SEQ, DIM), BF),
                pltpu.VMEM((2, GROUP * SEQ, HEAD_DIM), BF),
                pltpu.VMEM((2 * SEQ, HEAD_DIM), BF),
                pltpu.VMEM((2 * SEQ, HEAD_DIM), BF),
                pltpu.VMEM((LAYERS, 2 * SEQ, DIM), BF),
                pltpu.VMEM((LAYERS, 2 * SEQ, OUT_COLS), F32),
                pltpu.VMEM((LAYERS, SEQ, OUT_COLS), F32),
                pltpu.VMEM((LAYERS, 8 * SEQ, DIM), BF),
                pltpu.VMEM((8 * SEQ, WINDOW), BF),
                pltpu.VMEM((2, 4 * SEQ, DIM), F32),
                pltpu.VMEM((LAYERS, 4 * SEQ, DIM), F32),
                pltpu.VMEM((LAYERS, 2, SEQ, DIM // 2), F32),
                pltpu.VMEM((LAYERS, 2, SEQ, DIM // 2), F32),
                pltpu.VMEM((LAYERS, SEQ, DIM // 2), F32),
                pltpu.VMEM((LAYERS, SEQ, DIM // 2), F32),
            ] + [dma(shape) for shape in pairs for end in BOTH] + [dma((LAYERS, 4))] * 3,
            compiler_params=pltpu.CompilerParams(collective_id=0, has_side_effects=True, vmem_limit_bytes=67043328),
        )(hidden.reshape(SEQ, DIM), attn_norm, mlp_norm, jnp.asarray(cos_table), jnp.asarray(sin_table), wq, w_o, wk, wv, w_gate, w_up, w_down)
        return y.reshape(1, SEQ, DIM)

    batch_spec = P(("dp", "fsdp"), None, None)
    gain_spec = P(None, "fsdp")
    proj_spec = P(None, "fsdp", None, None)
    mat_spec = P(None, "fsdp", None)
    return jax.shard_map(local_forward, mesh=mesh, in_specs=(batch_spec, gain_spec, proj_spec, proj_spec, proj_spec, mat_spec, gain_spec, mat_spec, mat_spec, mat_spec), out_specs=batch_spec, check_vma=False)
```

```python
import functools

import jax
import jax.numpy as jnp
import numpy as np
from jax import lax
from jax.experimental import pallas as pl
from jax.experimental.pallas import tpu as pltpu
from jax.sharding import PartitionSpec as P

MESH = pl.DeviceIdType.MESH
ROPE_THETA = 500000.0
NORM_EPS = 1e-5
LAYERS = 2
SEQ = 64
DIM = 1536
HEADS = 12
KV_HEADS = 2
HEAD_DIM = 128
LANES = 128
TILE = 256
GROUP = HEADS // KV_HEADS
OUT_COLS = DIM // 2
FFN = 8960
ROWS = DIM // 8
FFN_ROWS = FFN // 8
WINDOW = 1152
MAIN = 1088
EDGE = 32
HALF = ROWS // 2
DIRECT = ((96, 96), (144, 96))
BF = jnp.bfloat16
BOTH = range(2)
F32 = jnp.float32
PARTS = ((0, 768), (768, 384))
GU_RELAYED = (2, 4, 3, 5, 6, 7)
RELAYS = (((2, 0), (4, 0)), ((2, 1), (4, 1)), ((6, 0), (6, 1), (3, 0), (5, 0)), ((3, 1), (5, 1), (7, 0), (7, 1)))
ONE, TWO, THREE, FOUR = [tuple((k, g) for k in pair) for pair in ((2, 4), (3, 5)) for g in (0, 1)]
FIVE = tuple((k, g) for k in (6, 7) for g in (0, 1))
CORE = ((1, 0), (1, 1))
KINDS = ((2, 3, 0), (1,))


def aligned(value, size):
    return pl.multiple_of(value, size)


def kernel(x_ref, an_ref, mn_ref, cos_ref, sin_ref, wq_ref, wo_ref, wk_ref, wv_ref, wg_ref, wu_ref, wd_ref, y_ref,
           gain_mine, gains, gain_rows, wq, wo, wkv, wgu, wd, edge, res, mid, n_buf, q_buf, k_buf, v_buf, o_buf, add_mine, add_got, u_buf, z_buf, part,
           r1, r2a, r2b, r3a, r3b,
           gain_s, gain_r, ad_s, ad_r, ax_s, ax_r, ac_s, ac_r, zx_s, zx_r, gd_s, gd_r, gz_s, gz_r, ed_s, ed_r, ag_s, ag_r, rs_s, rs_r,
           own_a, own_gu, own_wd):
    z = lax.axis_index("dp")
    me = lax.axis_index("fsdp")
    c = me % 2
    x = (me // 2) % 2
    y = me // 4

    def place(k):
        flips = (k % 2, (k // 2) % 2, k // 4)
        return [1 - own if flip else own for own, flip in zip((c, x, y), flips)]

    def peer(k):
        cc, xx, yy = place(k)
        return 4 * yy + 2 * xx + cc

    def block(k):
        cc, xx, yy = place(k)
        return 4 * cc + 2 * yy + xx

    def window(j):
        return aligned(LANES * (35 * (j // 4) + 9 * (j % 4) - (j % 4) // 2), LANES)

    def plane(k):
        return (z, peer(k))

    across = (1 - z, me)
    started = []

    def remote(src, dst, send, recv, device):
        return pltpu.make_async_remote_copy(src_ref=src, dst_ref=dst, send_sem=send, recv_sem=recv, device_id=device, device_id_type=MESH)

    def go(copy):
        copy.start()
        started.append(copy)

    barrier = pltpu.get_barrier_semaphore()
    for k in range(1, 8):
        pl.semaphore_signal(barrier, inc=1, device_id=plane(k), device_id_type=MESH)
    pl.semaphore_signal(barrier, inc=1, device_id=across, device_id_type=MESH)
    pl.semaphore_wait(barrier, 8)

    def gain_copy(k):
        return remote(gain_mine, gains.at[me], gain_s.at[k - 1], gain_r.at[k - 1], plane(k))

    def gain_arrival(k):
        dst = gains.at[peer(k)]
        return remote(dst, dst, gain_s.at[k - 1], gain_r.at[k - 1], plane(k))

    attn_src = (wq_ref, wo_ref, wk_ref, wv_ref)
    share = (GROUP, OUT_COLS, 1, 1)
    attn_dst = (wq, wo, wkv, wkv)
    heads_at = (pl.ds(0, GROUP), None, pl.ds(0, 1), pl.ds(1, 1))

    def attn_rows(l, m, k, start=0, count=ROWS):
        rows = pl.ds(aligned(ROWS * peer(k) + start, 32), count)
        return attn_dst[m].at[l, rows, :] if m == 1 else attn_dst[m].at[l, heads_at[m], rows, :]

    def attn_shard(l, m):
        if m == 1:
            return attn_src[m].at[l, :, pl.ds(aligned(share[m] * z, LANES), share[m])]
        return attn_src[m].at[l, pl.ds(share[m] * z, share[m]), :, :]

    def attn_own(l, m):
        return pltpu.make_async_copy(attn_shard(l, m), attn_rows(l, m, 0), own_a.at[l, m])

    def attn_direct(l, m, n):
        return remote(attn_shard(l, m), attn_rows(l, m, 0), ad_s.at[l, m, n], ad_r.at[l, m, n], plane(2 + 2 * n))

    def attn_arrival(l, m, n):
        dst = attn_rows(l, m, 2 + 2 * n)
        return remote(dst, dst, ad_s.at[l, m, n], ad_r.at[l, m, n], plane(2 + 2 * n))

    def attn_turn(l, m, n):
        rows = attn_rows(l, m, 2 + 2 * n, HALF * n, HALF)
        return remote(rows, rows, ax_s.at[l, m, n], ax_r.at[l, m, n], plane(4 - 2 * n))

    def attn_turn_arrival(l, m, n):
        dst = attn_rows(l, m, 6, HALF * n, HALF)
        return remote(dst, dst, ax_s.at[l, m, n], ax_r.at[l, m, n], plane(4 - 2 * n))

    def attn_core(l, m, slot, k, *part_rows):
        rows = attn_rows(l, m, k, *part_rows)
        return remote(rows, rows, ac_s.at[l, m, slot], ac_r.at[l, m, slot], plane(1))

    def attn_core_own(l, m):
        return remote(attn_shard(l, m), attn_rows(l, m, 0), ac_s.at[l, m, 0], ac_r.at[l, m, 0], plane(1))

    def send_attn(l, out):
        for m in KINDS[out]:
            for n in BOTH:
                go(attn_direct(l, m, n))
            go(attn_core_own(l, m))
            attn_own(l, m).start()

    def relay_attn(l, out):
        for m in KINDS[out]:
            for n in BOTH:
                attn_arrival(l, m, n).wait_recv()
                go(attn_turn(l, m, n))
                go(attn_core(l, m, 1 + n, 2 + 2 * n))

    def relay_attn_across(l, out):
        for m in KINDS[out]:
            for n in BOTH:
                attn_turn_arrival(l, m, n).wait_recv()
                go(attn_core(l, m, 3 + n, 6, HALF * n, HALF))

    def await_attn(l, out):
        for m in KINDS[out]:
            attn_own(l, m).wait()
            attn_core(l, m, 0, 1).wait_recv()
            for n in BOTH:
                attn_core(l, m, 1 + n, 3 + 2 * n).wait_recv()
                attn_core(l, m, 3 + n, 7, HALF * n, HALF).wait_recv()

    halves = (wg_ref, wu_ref)

    def gu_rows(l, p, g, k, start, count):
        return wgu.at[l, g, pl.ds(aligned(ROWS * peer(k) + start, 16), count), pl.ds(*PARTS[p])]

    def gu_direct(l, p, g, k):
        start, count = (0, ROWS) if k == 1 else (aligned((ROWS - DIRECT[p][k // 6]) * z, 16), DIRECT[p][k // 6])
        src = halves[g].at[l, pl.ds(start, count), pl.ds(aligned(window(peer(k)) + PARTS[p][0], LANES), PARTS[p][1])]
        return remote(src, gu_rows(l, p, g, 0, start, count), gd_s.at[l, p, g, k - 1], gd_r.at[l, p, g, k - 1], plane(k))

    def gu_arrival(l, p, g, k):
        start, count = (0, ROWS) if k == 1 else ((ROWS - DIRECT[p][k // 6]) * z, DIRECT[p][k // 6])
        dst = gu_rows(l, p, g, k, start, count)
        return remote(dst, dst, gd_s.at[l, p, g, k - 1], gd_r.at[l, p, g, k - 1], plane(k))

    def gu_across(l, p, g, k):
        rows = gu_rows(l, p, g, k, DIRECT[p][k // 6] * z, ROWS - DIRECT[p][k // 6])
        return remote(rows, rows, gz_s.at[l, p, g, k - 2], gz_r.at[l, p, g, k - 2], across)

    def gu_across_arrival(l, p, g, k):
        dst = gu_rows(l, p, g, k, DIRECT[p][k // 6] * (1 - z), ROWS - DIRECT[p][k // 6])
        return remote(dst, dst, gz_s.at[l, p, g, k - 2], gz_r.at[l, p, g, k - 2], across)

    def gu_own(l, g):
        dst = wgu.at[l, g, pl.ds(aligned(ROWS * me, 64), ROWS), :]
        return pltpu.make_async_copy(halves[g].at[l, :, pl.ds(window(me), WINDOW)], dst, own_gu.at[l, g])

    def send_gu(l, p, blocks):
        for k, g in blocks:
            go(gu_direct(l, p, g, k))

    def relay_gu(l, p, blocks):
        for k, g in blocks:
            gu_arrival(l, p, g, k).wait_recv()
            go(gu_across(l, p, g, k))

    def await_gu(l, p):
        for g in BOTH:
            gu_arrival(l, p, g, 1).wait_recv()
            if p == 0:
                gu_own(l, g).wait()
        for k in GU_RELAYED:
            for g in BOTH:
                gu_across_arrival(l, p, g, k).wait_recv()

    def start_own(l):
        for g in BOTH:
            gu_own(l, g).start()
        wd_copy(l).start()
        edge_own(l).start()
        go(edge_core(l))

    def wd_copy(l):
        return pltpu.make_async_copy(wd_ref.at[l, pl.ds(aligned(EDGE * c, EDGE), MAIN), :], wd.at[l, pl.ds(aligned(2 * EDGE * x, EDGE), MAIN), :], own_wd.at[l, 0])

    def edge_own(l):
        return pltpu.make_async_copy(wd_ref.at[l, pl.ds(aligned(MAIN * (1 - x), EDGE), EDGE), :], edge.at[l, 0], own_wd.at[l, 1])

    def edge_core(l):
        return remote(wd_ref.at[l, pl.ds(aligned(MAIN * x, EDGE), EDGE), :], edge.at[l, 1], ed_s.at[l], ed_r.at[l], plane(1))

    takes = c == x

    def finish_wd(l):
        wd_copy(l).wait()
        edge_own(l).wait()
        edge_core(l).wait_recv()
        own, got = edge[l, 0], edge[l, 1]
        none = jnp.zeros_like(own)
        edge_row = MAIN * (1 - x)
        wd[l, pl.ds(aligned(edge_row, EDGE), EDGE), :] = jnp.where(takes, jnp.where(x == 0, own, got), none)
        wd[l, pl.ds(aligned(edge_row + EDGE, EDGE), EDGE), :] = jnp.where(takes, jnp.where(x == 0, got, own), none)

    first = jnp.where(takes, 0, 2 * EDGE * x)
    last = jnp.where(takes, WINDOW, 2 * EDGE * x + MAIN)

    def normed(ref, row):
        wide = ref[...].astype(F32)
        inv_rms = lax.rsqrt(jnp.mean(wide * wide, axis=-1, keepdims=True) + NORM_EPS)
        return (wide * inv_rms * gain_rows[row : row + 1, :]).astype(BF)

    mine, other = pl.ds(aligned(SEQ * z, SEQ), SEQ), pl.ds(aligned(SEQ * (1 - z), SEQ), SEQ)
    left, right = pl.ds(aligned(OUT_COLS * z, LANES), OUT_COLS), pl.ds(aligned(OUT_COLS * (1 - z), LANES), OUT_COLS)

    def swap_in(l):
        rows = n_buf.at[l, mine, :]
        return remote(rows, rows, zx_s.at[l, 0], zx_r.at[l, 0], across)

    def swap_in_arrival(l):
        rows = n_buf.at[l, other, :]
        return remote(rows, rows, zx_s.at[l, 0], zx_r.at[l, 0], across)

    def swap_heads(l):
        cols = o_buf.at[l, :, left]
        return remote(cols, cols, zx_s.at[l, 1], zx_r.at[l, 1], across)

    def swap_heads_arrival(l):
        cols = o_buf.at[l, :, right]
        return remote(cols, cols, zx_s.at[l, 1], zx_r.at[l, 1], across)

    def swap_out(l):
        return remote(add_mine.at[l, other, :], add_got.at[l], zx_s.at[l, 2], zx_r.at[l, 2], across)

    def start_layer(l):
        n_buf[l, mine, :] = normed(res, l)
        go(swap_in(l))

    def project(l):
        cos, sin = cos_ref[...], sin_ref[...]

        def rotate(v):
            return (v * cos + pltpu.roll(v, HEAD_DIM // 2, 1) * sin).astype(BF)

        def two_heads(n):
            pair = (wkv[l, 0], wkv[l, 1]) if n is None else (wq[l, 2 * n], wq[l, 2 * n + 1])
            return jnp.dot(n_buf[l], jnp.concatenate(pair, axis=1), preferred_element_type=F32)

        def q_heads(n, carry):
            pair = two_heads(n)
            for t in BOTH:
                turned = rotate(pair[:, LANES * t : LANES * (t + 1)])
                for seq in BOTH:
                    q_buf[seq, pl.ds(aligned((2 * n + t) * SEQ, SEQ), SEQ), :] = turned[SEQ * seq : SEQ * (seq + 1)]
            return carry

        lax.fori_loop(0, GROUP // 2, q_heads, 0)
        pair = two_heads(None)
        k_buf[...] = rotate(pair[:, :LANES])
        v_buf[...] = pair[:, LANES:].astype(BF)

    def attend(l):
        row = lax.broadcasted_iota(jnp.int32, (GROUP * SEQ, SEQ), 0) % SEQ
        col = lax.broadcasted_iota(jnp.int32, (GROUP * SEQ, SEQ), 1)
        for seq in BOTH:
            rows = slice(SEQ * seq, SEQ * (seq + 1))
            scores = lax.dot_general(q_buf[seq], k_buf[rows, :], (((1,), (1,)), ((), ())), preferred_element_type=F32) * HEAD_DIM ** -0.5
            scores = jnp.where(row >= col, scores, -jnp.inf)
            e = jnp.exp(scores - jnp.max(scores, axis=-1, keepdims=True))
            probs = (e / jnp.sum(e, axis=-1, keepdims=True)).astype(BF)
            o = jnp.dot(probs, v_buf[rows, :], preferred_element_type=F32).astype(BF)
            for j in range(GROUP):
                o_buf[l, rows, pl.ds(aligned(OUT_COLS * z + HEAD_DIM * j, LANES), HEAD_DIM)] = o[j * SEQ : (j + 1) * SEQ]

    def project_out(l):
        def out_cols(n, carry):
            cols = pl.ds(aligned(TILE * n, TILE), TILE)
            add_mine[l, :, cols] = jnp.dot(o_buf[l], wo[l, :, cols], preferred_element_type=F32)
            return carry

        lax.fori_loop(0, OUT_COLS // TILE, out_cols, 0)

    def finish_attn(l):
        mid[:, left] = (res[:, left].astype(F32) + add_mine[l, mine, :]).astype(BF)
        mid[:, right] = (res[:, right].astype(F32) + add_got[l]).astype(BF)

    def seq_rows(l, k, start=0, count=SEQ):
        return u_buf.at[l, pl.ds(aligned(SEQ * block(k) + start, 32), count), :]

    def ag(l, sem, k, to, *rows):
        part_rows = seq_rows(l, k, *rows)
        return remote(part_rows, part_rows, ag_s.at[l, sem], ag_r.at[l, sem], plane(to))

    def ag_half(n):
        return SEQ // 2 * n, SEQ // 2

    def ag_start(l):
        for n in BOTH:
            go(ag(l, n, 0, 2 + 2 * n))
        go(ag(l, 2, 0, 1))

    def ag_turn(l):
        for n in BOTH:
            k = 2 + 2 * n
            ag(l, n, k, k).wait_recv()
            go(ag(l, 5 + n, k, 6 - k, *ag_half(n)))
            go(ag(l, 3 + n, k, 1))

    def ag_across(l):
        for n in BOTH:
            ag(l, 5 + n, 6, 4 - 2 * n, *ag_half(n)).wait_recv()
            go(ag(l, 7 + n, 6, 1, *ag_half(n)))

    def ag_end(l):
        ag(l, 2, 1, 1).wait_recv()
        for n in BOTH:
            ag(l, 3 + n, 3 + 2 * n, 1).wait_recv()
            ag(l, 7 + n, 7, 1, *ag_half(n)).wait_recv()

    def gate_up(l, p, b):
        rows = pl.ds(aligned(TILE * b, TILE), TILE)
        begin, size = PARTS[p]

        def columns(start, width):
            at = pl.ds(aligned(start, LANES), width)
            u = u_buf[l, rows, :]
            gate = jnp.dot(u, wgu[l, 0, :, at], preferred_element_type=F32).astype(BF).astype(F32)
            up = jnp.dot(u, wgu[l, 1, :, at], preferred_element_type=F32).astype(BF).astype(F32)
            gated = (jax.nn.silu(gate) * up).astype(BF)
            spot = start + lax.broadcasted_iota(jnp.int32, (TILE, width), 1)
            valid = (spot >= first) & (spot < last)
            z_buf[rows, at] = jnp.where(valid, gated, jnp.zeros_like(gated))

        def cols(n, carry):
            columns(begin + TILE * n, TILE)
            return carry

        lax.fori_loop(0, size // TILE, cols, 0)
        if size % TILE:
            columns(begin + size - LANES, LANES)

    def down(l, p, b, half):
        rows = pl.ds(aligned(TILE * b, TILE), TILE)
        inner = pl.ds(*PARTS[p])

        def cols(n, carry):
            at = pl.ds(aligned(TILE * n, TILE), TILE)
            add = jnp.dot(z_buf[rows, inner], wd[l, inner, at], preferred_element_type=F32)
            part[b, :, at] = add if p == 0 else part[b, :, at] + add
            return carry

        lax.fori_loop(3 * half, 3 * half + 3, cols, 0)

    A, B = slice(DIM // 2), slice(DIM // 2, DIM)

    def chip_rows(yy, xx):
        return pl.ds(aligned(SEQ * (2 * yy + xx), SEQ), SEQ)

    def rs_core(l, half):
        cols = (A, B)[half]
        sem = 7 if half else 0
        return remote(part.at[1 - c, :, cols], r1.at[l, :, cols], rs_s.at[l, sem], rs_r.at[l, sem], plane(1))

    def rs_a(l, t):
        return remote(part.at[c, chip_rows((1 - y, y)[t], 1 - x), A], r2a.at[l, t], rs_s.at[l, 1 + t], rs_r.at[l, 1 + t], plane(2))

    def rs_b(l, t):
        return remote(part.at[c, chip_rows(1 - y, (1 - x, x)[t]), B], r2b.at[l, t], rs_s.at[l, 3 + t], rs_r.at[l, 3 + t], plane(4))

    def rs_a_last(l):
        return remote(part.at[c, chip_rows(1 - y, x), A], r3a.at[l], rs_s.at[l, 5], rs_r.at[l, 5], plane(4))

    def rs_b_last(l):
        return remote(part.at[c, chip_rows(y, 1 - x), B], r3b.at[l], rs_s.at[l, 6], rs_r.at[l, 6], plane(2))

    sends = []

    def send(copy):
        copy.start()
        sends.append(copy)

    def attention(l):
        await_attn(l, 0)
        swap_in_arrival(l).wait_recv()
        project(l)
        attend(l)
        go(swap_heads(l))

    def attention_out(l):
        await_attn(l, 1)
        swap_heads_arrival(l).wait_recv()
        project_out(l)
        go(swap_out(l))

    def attention_end(l):
        swap_out(l).wait_recv()
        finish_attn(l)
        u_buf[l, pl.ds(aligned(SEQ * block(0), SEQ), SEQ), :] = normed(mid, 2 + l)
        ag_start(l)
        send_gu(l, 1, ONE + TWO)

    def mlp(l, relays):
        relay_gu(l, 0, relays)
        ag_turn(l)
        send_gu(l, 1, THREE + FOUR + FIVE + CORE)
        if l + 1 < LAYERS:
            send_gu(l + 1, 0, ONE)
            send_attn(l + 1, 0)
            send_gu(l + 1, 0, TWO)
        relay_gu(l, 1, ONE + TWO)
        ag_across(l)
        await_gu(l, 0)
        gate_up(l, 0, c)
        relay_gu(l, 1, THREE)
        ag_end(l)
        gate_up(l, 0, 1 - c)
        relay_gu(l, 1, FOUR[:1] + FIVE[:2])
        while sends:
            sends.pop().wait_send()
        finish_wd(l)
        for half in BOTH:
            down(l, 0, 1 - c, half)
        relay_gu(l, 1, FOUR[1:] + FIVE[2:])
        for half in BOTH:
            down(l, 0, c, half)
        await_gu(l, 1)
        gate_up(l, 1, 1 - c)
        for half in BOTH:
            down(l, 1, 1 - c, half)
            send(rs_core(l, half))

    def mlp_own(l):
        gate_up(l, 1, c)
        for half in BOTH:
            down(l, 1, c, half)
            cols = (A, B)[half]
            rs_core(l, half).wait_recv()
            part[c, :, cols] = part[c, :, cols] + r1[l, :, cols]
            for t in BOTH:
                send((rs_a, rs_b)[half](l, t))

    def rs_add(l, t):
        row_a, row_b = chip_rows((1 - y, y)[t], x), chip_rows(y, (1 - x, x)[t])
        rs_a(l, t).wait_recv()
        part[c, row_a, A] = part[c, row_a, A] + r2a[l, t]
        if t == 0:
            send(rs_a_last(l))
        rs_b(l, t).wait_recv()
        part[c, row_b, B] = part[c, row_b, B] + r2b[l, t]
        if t == 0:
            send(rs_b_last(l))

    def rs_middle(l):
        for t in BOTH:
            rs_add(l, t)

    def rs_end(l, out):
        rs_a_last(l).wait_recv()
        out[:, A] = (mid[:, A].astype(F32) + (part[c, chip_rows(y, x), A] + r3a[l])).astype(BF)
        rs_b_last(l).wait_recv()
        out[:, B] = (mid[:, B].astype(F32) + (part[c, chip_rows(y, x), B] + r3b[l])).astype(BF)

    gain_mine[...] = jnp.zeros_like(gain_mine)
    gain_mine[:LAYERS, :ROWS] = an_ref[...].astype(F32)
    gain_mine[LAYERS : 2 * LAYERS, :ROWS] = mn_ref[...].astype(F32)
    gain_mine[...] = jnp.where(c == 1, pltpu.roll(gain_mine[...], ROWS, 1), gain_mine[...])
    for k in range(1, 8):
        go(gain_copy(k))
    send_gu(0, 0, ONE + TWO + THREE)
    for m in BOTH:
        send_attn(0, m)
    gains[me] = gain_mine[...]
    res[...] = x_ref[...]
    for k in range(1, 8):
        gain_arrival(k).wait_recv()
    for p in range(4):
        gain_rows[:, 384 * p : 384 * (p + 1)] = gains[2 * p] + gains[2 * p + 1]
    start_layer(0)
    relay_gu(0, 0, ONE + TWO + THREE)
    for m in BOTH:
        relay_attn(0, m)
    send_gu(0, 0, FOUR + FIVE + CORE)
    for l in range(LAYERS):
        start_own(l)
    relay_attn_across(0, 0)
    attention(0)
    relay_attn_across(0, 1)
    attention_out(0)
    relay_gu(0, 0, FOUR + FIVE[:2])
    attention_end(0)
    mlp(0, FIVE[2:])
    relay_gu(1, 0, ONE)
    mlp_own(0)
    relay_gu(1, 0, TWO)
    relay_attn(1, 0)
    rs_middle(0)
    send_gu(1, 0, THREE)
    send_attn(1, 1)
    relay_attn_across(1, 0)
    rs_end(0, res)
    start_layer(1)
    attention(1)
    relay_attn(1, 1)
    send_gu(1, 0, FOUR + FIVE + CORE)
    relay_gu(1, 0, THREE)
    relay_attn_across(1, 1)
    attention_out(1)
    relay_gu(1, 0, FOUR[:1])
    attention_end(1)
    mlp(1, FIVE[:1] + FOUR[1:] + FIVE[1:])
    mlp_own(1)
    rs_middle(1)
    rs_end(1, y_ref)
    for copy in sends + started:
        copy.wait_send()


def solution(mesh):
    vmem = pl.BlockSpec(memory_space=pltpu.VMEM)
    hbm = pl.BlockSpec(memory_space=pl.ANY)
    dma = pltpu.SemaphoreType.DMA
    pairs = [(7,), (LAYERS, 4, 2), (LAYERS, 4, 2), (LAYERS, 4, 5), (LAYERS, 3), (LAYERS, 2, 2, 7), (LAYERS, 2, 2, 6), (LAYERS,), (LAYERS, 9), (LAYERS, 8)]
    inv_freq = ROPE_THETA ** -(np.arange(HEAD_DIM // 2) * 2.0 / HEAD_DIM)
    angles = np.tile(np.arange(SEQ)[:, None] * inv_freq[None, :].astype(np.float32), (2, 1)).astype(np.float32)
    cos_table = np.concatenate([np.cos(angles), np.cos(angles)], axis=1)
    sin_table = np.concatenate([-np.sin(angles), np.sin(angles)], axis=1)

    def local_forward(hidden, attn_norm, w_q, w_k, w_v, w_o, mlp_norm, w_gate, w_up, w_down):
        wq = w_q.transpose(0, 2, 1, 3)
        wk, wv = w_k.transpose(0, 2, 1, 3), w_v.transpose(0, 2, 1, 3)
        y = pl.pallas_call(
            kernel,
            out_shape=jax.ShapeDtypeStruct((SEQ, DIM), BF),
            in_specs=[vmem] * 5 + [hbm] * 7,
            out_specs=vmem,
            scratch_shapes=[
                pltpu.VMEM((8, 2 * ROWS), F32),
                pltpu.VMEM((8, 8, 2 * ROWS), F32),
                pltpu.VMEM((8, DIM), F32),
                pltpu.VMEM((LAYERS, GROUP, DIM, HEAD_DIM), BF),
                pltpu.VMEM((LAYERS, DIM, OUT_COLS), BF),
                pltpu.VMEM((LAYERS, KV_HEADS, DIM, HEAD_DIM), BF),
                pltpu.VMEM((LAYERS, 2, DIM, WINDOW), BF),
                pltpu.VMEM((LAYERS, WINDOW, DIM), BF),
                pltpu.VMEM((LAYERS, 2, EDGE, DIM), BF),
                pltpu.VMEM((SEQ, DIM), BF),
                pltpu.VMEM((SEQ, DIM), BF),
                pltpu.VMEM((LAYERS, 2 * SEQ, DIM), BF),
                pltpu.VMEM((2, GROUP * SEQ, HEAD_DIM), BF),
                pltpu.VMEM((2 * SEQ, HEAD_DIM), BF),
                pltpu.VMEM((2 * SEQ, HEAD_DIM), BF),
                pltpu.VMEM((LAYERS, 2 * SEQ, DIM), BF),
                pltpu.VMEM((LAYERS, 2 * SEQ, OUT_COLS), F32),
                pltpu.VMEM((LAYERS, SEQ, OUT_COLS), F32),
                pltpu.VMEM((LAYERS, 8 * SEQ, DIM), BF),
                pltpu.VMEM((8 * SEQ, WINDOW), BF),
                pltpu.VMEM((2, 4 * SEQ, DIM), F32),
                pltpu.VMEM((LAYERS, 4 * SEQ, DIM), F32),
                pltpu.VMEM((LAYERS, 2, SEQ, DIM // 2), F32),
                pltpu.VMEM((LAYERS, 2, SEQ, DIM // 2), F32),
                pltpu.VMEM((LAYERS, SEQ, DIM // 2), F32),
                pltpu.VMEM((LAYERS, SEQ, DIM // 2), F32),
            ] + [dma(shape) for shape in pairs for end in BOTH] + [dma((LAYERS, 4))] * 3,
            compiler_params=pltpu.CompilerParams(collective_id=0, has_side_effects=True, vmem_limit_bytes=67043328),
        )(hidden.reshape(SEQ, DIM), attn_norm, mlp_norm, jnp.asarray(cos_table), jnp.asarray(sin_table), wq, w_o, wk, wv, w_gate, w_up, w_down)
        return y.reshape(1, SEQ, DIM)

    batch_spec = P(("dp", "fsdp"), None, None)
    gain_spec = P(None, "fsdp")
    proj_spec = P(None, "fsdp", None, None)
    mat_spec = P(None, "fsdp", None)
    return jax.shard_map(local_forward, mesh=mesh, in_specs=(batch_spec, gain_spec, proj_spec, proj_spec, proj_spec, mat_spec, gain_spec, mat_spec, mat_spec, mat_spec), out_specs=batch_spec, check_vma=False)
```

```python
import functools

import jax
import jax.numpy as jnp
import numpy as np
from jax import lax
from jax.experimental import pallas as pl
from jax.experimental.pallas import tpu as pltpu
from jax.sharding import PartitionSpec as P

MESH = pl.DeviceIdType.MESH
ROPE_THETA = 500000.0
NORM_EPS = 1e-5
LAYERS = 2
SEQ = 64
DIM = 1536
HEADS = 12
KV_HEADS = 2
HEAD_DIM = 128
LANES = 128
TILE = 256
GROUP = HEADS // KV_HEADS
OUT_COLS = DIM // 2
FFN = 8960
ROWS = DIM // 8
FFN_ROWS = FFN // 8
WINDOW = 1152
MAIN = 1088
EDGE = 32
HALF = ROWS // 2
DIRECT = ((96, 96), (144, 96))
BF = jnp.bfloat16
BOTH = range(2)
F32 = jnp.float32
PARTS = ((0, 768), (768, 384))
GU_RELAYED = (2, 4, 3, 5, 6, 7)
RELAYS = (((2, 0), (4, 0)), ((2, 1), (4, 1)), ((6, 0), (6, 1), (3, 0), (5, 0)), ((3, 1), (5, 1), (7, 0), (7, 1)))
ONE, TWO, THREE, FOUR = [tuple((k, g) for k in pair) for pair in ((2, 4), (3, 5)) for g in (0, 1)]
FIVE = tuple((k, g) for k in (6, 7) for g in (0, 1))
CORE = ((1, 0), (1, 1))
KINDS = ((2, 3, 0), (1,))


def aligned(value, size):
    return pl.multiple_of(value, size)


def kernel(x_ref, an_ref, mn_ref, cos_ref, sin_ref, wq_ref, wo_ref, wk_ref, wv_ref, wg_ref, wu_ref, wd_ref, y_ref,
           gain_mine, gains, gain_rows, wq, wo, wkv, wgu, wd, edge, res, mid, n_buf, q_buf, k_buf, v_buf, o_buf, add_mine, add_got, u_buf, z_buf, part,
           r1, r2a, r2b, r3a, r3b,
           gain_s, gain_r, ad_s, ad_r, ax_s, ax_r, ac_s, ac_r, zx_s, zx_r, gd_s, gd_r, gz_s, gz_r, ed_s, ed_r, ag_s, ag_r, rs_s, rs_r,
           own_a, own_gu, own_wd):
    z = lax.axis_index("dp")
    me = lax.axis_index("fsdp")
    c = me % 2
    x = (me // 2) % 2
    y = me // 4

    def place(k):
        flips = (k % 2, (k // 2) % 2, k // 4)
        return [1 - own if flip else own for own, flip in zip((c, x, y), flips)]

    def peer(k):
        cc, xx, yy = place(k)
        return 4 * yy + 2 * xx + cc

    def block(k):
        cc, xx, yy = place(k)
        return 4 * cc + 2 * yy + xx

    def window(j):
        return aligned(LANES * (35 * (j // 4) + 9 * (j % 4) - (j % 4) // 2), LANES)

    def plane(k):
        return (z, peer(k))

    across = (1 - z, me)
    started = []

    def remote(src, dst, send, recv, device):
        return pltpu.make_async_remote_copy(src_ref=src, dst_ref=dst, send_sem=send, recv_sem=recv, device_id=device, device_id_type=MESH)

    def go(copy):
        copy.start()
        started.append(copy)

    barrier = pltpu.get_barrier_semaphore()
    for k in range(1, 8):
        pl.semaphore_signal(barrier, inc=1, device_id=plane(k), device_id_type=MESH)
    pl.semaphore_signal(barrier, inc=1, device_id=across, device_id_type=MESH)
    pl.semaphore_wait(barrier, 8)

    def gain_copy(k):
        return remote(gain_mine, gains.at[me], gain_s.at[k - 1], gain_r.at[k - 1], plane(k))

    def gain_arrival(k):
        dst = gains.at[peer(k)]
        return remote(dst, dst, gain_s.at[k - 1], gain_r.at[k - 1], plane(k))

    attn_src = (wq_ref, wo_ref, wk_ref, wv_ref)
    share = (GROUP, OUT_COLS, 1, 1)
    attn_dst = (wq, wo, wkv, wkv)
    heads_at = (pl.ds(0, GROUP), None, pl.ds(0, 1), pl.ds(1, 1))

    def attn_rows(l, m, k, start=0, count=ROWS):
        rows = pl.ds(aligned(ROWS * peer(k) + start, 32), count)
        return attn_dst[m].at[l, rows, :] if m == 1 else attn_dst[m].at[l, heads_at[m], rows, :]

    def attn_shard(l, m):
        if m == 1:
            return attn_src[m].at[l, :, pl.ds(aligned(share[m] * z, LANES), share[m])]
        return attn_src[m].at[l, pl.ds(share[m] * z, share[m]), :, :]

    def attn_own(l, m):
        return pltpu.make_async_copy(attn_shard(l, m), attn_rows(l, m, 0), own_a.at[l, m])

    def attn_direct(l, m, n):
        return remote(attn_shard(l, m), attn_rows(l, m, 0), ad_s.at[l, m, n], ad_r.at[l, m, n], plane(2 + 2 * n))

    def attn_arrival(l, m, n):
        dst = attn_rows(l, m, 2 + 2 * n)
        return remote(dst, dst, ad_s.at[l, m, n], ad_r.at[l, m, n], plane(2 + 2 * n))

    def attn_turn(l, m, n):
        rows = attn_rows(l, m, 2 + 2 * n, HALF * n, HALF)
        return remote(rows, rows, ax_s.at[l, m, n], ax_r.at[l, m, n], plane(4 - 2 * n))

    def attn_turn_arrival(l, m, n):
        dst = attn_rows(l, m, 6, HALF * n, HALF)
        return remote(dst, dst, ax_s.at[l, m, n], ax_r.at[l, m, n], plane(4 - 2 * n))

    def attn_core(l, m, slot, k, *part_rows):
        rows = attn_rows(l, m, k, *part_rows)
        return remote(rows, rows, ac_s.at[l, m, slot], ac_r.at[l, m, slot], plane(1))

    def attn_core_own(l, m):
        return remote(attn_shard(l, m), attn_rows(l, m, 0), ac_s.at[l, m, 0], ac_r.at[l, m, 0], plane(1))

    def send_attn(l, out):
        for m in KINDS[out]:
            for n in BOTH:
                go(attn_direct(l, m, n))
            go(attn_core_own(l, m))
            attn_own(l, m).start()

    def relay_attn(l, out):
        for m in KINDS[out]:
            for n in BOTH:
                attn_arrival(l, m, n).wait_recv()
                go(attn_turn(l, m, n))
                go(attn_core(l, m, 1 + n, 2 + 2 * n))

    def relay_attn_across(l, out):
        for m in KINDS[out]:
            for n in BOTH:
                attn_turn_arrival(l, m, n).wait_recv()
                go(attn_core(l, m, 3 + n, 6, HALF * n, HALF))

    def await_attn(l, out):
        for m in KINDS[out]:
            attn_own(l, m).wait()
            attn_core(l, m, 0, 1).wait_recv()
            for n in BOTH:
                attn_core(l, m, 1 + n, 3 + 2 * n).wait_recv()
                attn_core(l, m, 3 + n, 7, HALF * n, HALF).wait_recv()

    halves = (wg_ref, wu_ref)

    def gu_rows(l, p, g, k, start, count):
        return wgu.at[l, g, pl.ds(aligned(ROWS * peer(k) + start, 16), count), pl.ds(*PARTS[p])]

    def gu_direct(l, p, g, k):
        start, count = (0, ROWS) if k == 1 else (aligned((ROWS - DIRECT[p][k // 6]) * z, 16), DIRECT[p][k // 6])
        src = halves[g].at[l, pl.ds(start, count), pl.ds(aligned(window(peer(k)) + PARTS[p][0], LANES), PARTS[p][1])]
        return remote(src, gu_rows(l, p, g, 0, start, count), gd_s.at[l, p, g, k - 1], gd_r.at[l, p, g, k - 1], plane(k))

    def gu_arrival(l, p, g, k):
        start, count = (0, ROWS) if k == 1 else ((ROWS - DIRECT[p][k // 6]) * z, DIRECT[p][k // 6])
        dst = gu_rows(l, p, g, k, start, count)
        return remote(dst, dst, gd_s.at[l, p, g, k - 1], gd_r.at[l, p, g, k - 1], plane(k))

    def gu_across(l, p, g, k):
        rows = gu_rows(l, p, g, k, DIRECT[p][k // 6] * z, ROWS - DIRECT[p][k // 6])
        return remote(rows, rows, gz_s.at[l, p, g, k - 2], gz_r.at[l, p, g, k - 2], across)

    def gu_across_arrival(l, p, g, k):
        dst = gu_rows(l, p, g, k, DIRECT[p][k // 6] * (1 - z), ROWS - DIRECT[p][k // 6])
        return remote(dst, dst, gz_s.at[l, p, g, k - 2], gz_r.at[l, p, g, k - 2], across)

    def gu_own(l, g):
        dst = wgu.at[l, g, pl.ds(aligned(ROWS * me, 64), ROWS), :]
        return pltpu.make_async_copy(halves[g].at[l, :, pl.ds(window(me), WINDOW)], dst, own_gu.at[l, g])

    def send_gu(l, p, blocks):
        for k, g in blocks:
            go(gu_direct(l, p, g, k))

    def relay_gu(l, p, blocks):
        for k, g in blocks:
            gu_arrival(l, p, g, k).wait_recv()
            go(gu_across(l, p, g, k))

    def await_gu(l, p):
        for g in BOTH:
            gu_arrival(l, p, g, 1).wait_recv()
            if p == 0:
                gu_own(l, g).wait()
        for k in GU_RELAYED:
            for g in BOTH:
                gu_across_arrival(l, p, g, k).wait_recv()

    def start_own(l):
        for g in BOTH:
            gu_own(l, g).start()
        wd_copy(l).start()
        edge_own(l).start()
        go(edge_core(l))

    def wd_copy(l):
        return pltpu.make_async_copy(wd_ref.at[l, pl.ds(aligned(EDGE * c, EDGE), MAIN), :], wd.at[l, pl.ds(aligned(2 * EDGE * x, EDGE), MAIN), :], own_wd.at[l, 0])

    def edge_own(l):
        return pltpu.make_async_copy(wd_ref.at[l, pl.ds(aligned(MAIN * (1 - x), EDGE), EDGE), :], edge.at[l, 0], own_wd.at[l, 1])

    def edge_core(l):
        return remote(wd_ref.at[l, pl.ds(aligned(MAIN * x, EDGE), EDGE), :], edge.at[l, 1], ed_s.at[l], ed_r.at[l], plane(1))

    takes = c == x

    def finish_wd(l):
        wd_copy(l).wait()
        edge_own(l).wait()
        edge_core(l).wait_recv()
        own, got = edge[l, 0], edge[l, 1]
        none = jnp.zeros_like(own)
        edge_row = MAIN * (1 - x)
        wd[l, pl.ds(aligned(edge_row, EDGE), EDGE), :] = jnp.where(takes, jnp.where(x == 0, own, got), none)
        wd[l, pl.ds(aligned(edge_row + EDGE, EDGE), EDGE), :] = jnp.where(takes, jnp.where(x == 0, got, own), none)

    first = jnp.where(takes, 0, 2 * EDGE * x)
    last = jnp.where(takes, WINDOW, 2 * EDGE * x + MAIN)

    def normed(ref, row):
        wide = ref[...].astype(F32)
        inv_rms = lax.rsqrt(jnp.mean(wide * wide, axis=-1, keepdims=True) + NORM_EPS)
        return (wide * inv_rms * gain_rows[row : row + 1, :]).astype(BF)

    mine, other = pl.ds(aligned(SEQ * z, SEQ), SEQ), pl.ds(aligned(SEQ * (1 - z), SEQ), SEQ)
    left, right = pl.ds(aligned(OUT_COLS * z, LANES), OUT_COLS), pl.ds(aligned(OUT_COLS * (1 - z), LANES), OUT_COLS)

    def swap_in(l):
        rows = n_buf.at[l, mine, :]
        return remote(rows, rows, zx_s.at[l, 0], zx_r.at[l, 0], across)

    def swap_in_arrival(l):
        rows = n_buf.at[l, other, :]
        return remote(rows, rows, zx_s.at[l, 0], zx_r.at[l, 0], across)

    def swap_heads(l):
        cols = o_buf.at[l, :, left]
        return remote(cols, cols, zx_s.at[l, 1], zx_r.at[l, 1], across)

    def swap_heads_arrival(l):
        cols = o_buf.at[l, :, right]
        return remote(cols, cols, zx_s.at[l, 1], zx_r.at[l, 1], across)

    def swap_out(l):
        return remote(add_mine.at[l, other, :], add_got.at[l], zx_s.at[l, 2], zx_r.at[l, 2], across)

    def start_layer(l):
        n_buf[l, mine, :] = normed(res, l)
        go(swap_in(l))

    def project(l):
        cos, sin = cos_ref[...], sin_ref[...]

        def rotate(v):
            return (v * cos + pltpu.roll(v, HEAD_DIM // 2, 1) * sin).astype(BF)

        def two_heads(n):
            pair = (wkv[l, 0], wkv[l, 1]) if n is None else (wq[l, 2 * n], wq[l, 2 * n + 1])
            return jnp.dot(n_buf[l], jnp.concatenate(pair, axis=1), preferred_element_type=F32)

        def q_heads(n, carry):
            pair = two_heads(n)
            for t in BOTH:
                turned = rotate(pair[:, LANES * t : LANES * (t + 1)])
                for seq in BOTH:
                    q_buf[seq, pl.ds(aligned((2 * n + t) * SEQ, SEQ), SEQ), :] = turned[SEQ * seq : SEQ * (seq + 1)]
            return carry

        lax.fori_loop(0, GROUP // 2, q_heads, 0)
        pair = two_heads(None)
        k_buf[...] = rotate(pair[:, :LANES])
        v_buf[...] = pair[:, LANES:].astype(BF)

    def attend(l):
        row = lax.broadcasted_iota(jnp.int32, (GROUP * SEQ, SEQ), 0) % SEQ
        col = lax.broadcasted_iota(jnp.int32, (GROUP * SEQ, SEQ), 1)
        for seq in BOTH:
            rows = slice(SEQ * seq, SEQ * (seq + 1))
            scores = lax.dot_general(q_buf[seq], k_buf[rows, :], (((1,), (1,)), ((), ())), preferred_element_type=F32) * HEAD_DIM ** -0.5
            scores = jnp.where(row >= col, scores, -jnp.inf)
            e = jnp.exp(scores - jnp.max(scores, axis=-1, keepdims=True))
            probs = (e / jnp.sum(e, axis=-1, keepdims=True)).astype(BF)
            o = jnp.dot(probs, v_buf[rows, :], preferred_element_type=F32).astype(BF)
            for j in range(GROUP):
                o_buf[l, rows, pl.ds(aligned(OUT_COLS * z + HEAD_DIM * j, LANES), HEAD_DIM)] = o[j * SEQ : (j + 1) * SEQ]

    def project_out(l):
        def out_cols(n, carry):
            cols = pl.ds(aligned(TILE * n, TILE), TILE)
            add_mine[l, :, cols] = jnp.dot(o_buf[l], wo[l, :, cols], preferred_element_type=F32)
            return carry

        lax.fori_loop(0, OUT_COLS // TILE, out_cols, 0)

    def finish_attn(l):
        mid[:, left] = (res[:, left].astype(F32) + add_mine[l, mine, :]).astype(BF)
        mid[:, right] = (res[:, right].astype(F32) + add_got[l]).astype(BF)

    def seq_rows(l, k, start=0, count=SEQ):
        return u_buf.at[l, pl.ds(aligned(SEQ * block(k) + start, 32), count), :]

    def ag(l, sem, k, to, *rows):
        part_rows = seq_rows(l, k, *rows)
        return remote(part_rows, part_rows, ag_s.at[l, sem], ag_r.at[l, sem], plane(to))

    def ag_half(n):
        return SEQ // 2 * n, SEQ // 2

    def ag_start(l):
        for n in BOTH:
            go(ag(l, n, 0, 2 + 2 * n))
        go(ag(l, 2, 0, 1))

    def ag_turn(l):
        for n in BOTH:
            k = 2 + 2 * n
            ag(l, n, k, k).wait_recv()
            go(ag(l, 5 + n, k, 6 - k, *ag_half(n)))
            go(ag(l, 3 + n, k, 1))

    def ag_across(l):
        for n in BOTH:
            ag(l, 5 + n, 6, 4 - 2 * n, *ag_half(n)).wait_recv()
            go(ag(l, 7 + n, 6, 1, *ag_half(n)))

    def ag_end(l):
        ag(l, 2, 1, 1).wait_recv()
        for n in BOTH:
            ag(l, 3 + n, 3 + 2 * n, 1).wait_recv()
            ag(l, 7 + n, 7, 1, *ag_half(n)).wait_recv()

    def gate_up(l, p, b):
        rows = pl.ds(aligned(TILE * b, TILE), TILE)
        begin, size = PARTS[p]

        def columns(start, width):
            at = pl.ds(aligned(start, LANES), width)
            u = u_buf[l, rows, :]
            gate = jnp.dot(u, wgu[l, 0, :, at], preferred_element_type=F32).astype(BF).astype(F32)
            up = jnp.dot(u, wgu[l, 1, :, at], preferred_element_type=F32).astype(BF).astype(F32)
            gated = (jax.nn.silu(gate) * up).astype(BF)
            spot = start + lax.broadcasted_iota(jnp.int32, (TILE, width), 1)
            valid = (spot >= first) & (spot < last)
            z_buf[rows, at] = jnp.where(valid, gated, jnp.zeros_like(gated))

        def cols(n, carry):
            columns(begin + TILE * n, TILE)
            return carry

        if p == 1:
            columns(begin, size)
        else:
            lax.fori_loop(0, size // TILE, cols, 0)

    def down(l, p, b, half):
        rows = pl.ds(aligned(TILE * b, TILE), TILE)
        inner = pl.ds(*PARTS[p])

        def cols(n, carry):
            at = pl.ds(aligned(TILE * n, TILE), TILE)
            add = jnp.dot(z_buf[rows, inner], wd[l, inner, at], preferred_element_type=F32)
            part[b, :, at] = add if p == 0 else part[b, :, at] + add
            return carry

        lax.fori_loop(3 * half, 3 * half + 3, cols, 0, unroll=p == 1)

    A, B = slice(DIM // 2), slice(DIM // 2, DIM)

    def chip_rows(yy, xx):
        return pl.ds(aligned(SEQ * (2 * yy + xx), SEQ), SEQ)

    def rs_core(l, half):
        cols = (A, B)[half]
        sem = 7 if half else 0
        return remote(part.at[1 - c, :, cols], r1.at[l, :, cols], rs_s.at[l, sem], rs_r.at[l, sem], plane(1))

    def rs_a(l, t):
        return remote(part.at[c, chip_rows((1 - y, y)[t], 1 - x), A], r2a.at[l, t], rs_s.at[l, 1 + t], rs_r.at[l, 1 + t], plane(2))

    def rs_b(l, t):
        return remote(part.at[c, chip_rows(1 - y, (1 - x, x)[t]), B], r2b.at[l, t], rs_s.at[l, 3 + t], rs_r.at[l, 3 + t], plane(4))

    def rs_a_last(l):
        return remote(part.at[c, chip_rows(1 - y, x), A], r3a.at[l], rs_s.at[l, 5], rs_r.at[l, 5], plane(4))

    def rs_b_last(l):
        return remote(part.at[c, chip_rows(y, 1 - x), B], r3b.at[l], rs_s.at[l, 6], rs_r.at[l, 6], plane(2))

    sends = []

    def send(copy):
        copy.start()
        sends.append(copy)

    def attention(l):
        await_attn(l, 0)
        swap_in_arrival(l).wait_recv()
        project(l)
        attend(l)
        go(swap_heads(l))

    def attention_out(l):
        await_attn(l, 1)
        swap_heads_arrival(l).wait_recv()
        project_out(l)
        go(swap_out(l))

    def attention_end(l):
        swap_out(l).wait_recv()
        finish_attn(l)
        u_buf[l, pl.ds(aligned(SEQ * block(0), SEQ), SEQ), :] = normed(mid, 2 + l)
        ag_start(l)
        send_gu(l, 1, ONE + TWO)

    def mlp(l, relays):
        relay_gu(l, 0, relays)
        ag_turn(l)
        send_gu(l, 1, THREE + FOUR + FIVE + CORE)
        if l + 1 < LAYERS:
            send_gu(l + 1, 0, ONE)
            send_attn(l + 1, 0)
            send_gu(l + 1, 0, TWO)
        relay_gu(l, 1, ONE + TWO)
        ag_across(l)
        await_gu(l, 0)
        gate_up(l, 0, c)
        relay_gu(l, 1, THREE)
        ag_end(l)
        gate_up(l, 0, 1 - c)
        relay_gu(l, 1, FOUR[:1] + FIVE[:2])
        while sends:
            sends.pop().wait_send()
        finish_wd(l)
        for half in BOTH:
            down(l, 0, 1 - c, half)
        relay_gu(l, 1, FOUR[1:] + FIVE[2:])
        for half in BOTH:
            down(l, 0, c, half)
        await_gu(l, 1)
        gate_up(l, 1, 1 - c)
        for half in BOTH:
            down(l, 1, 1 - c, half)
            send(rs_core(l, half))

    def mlp_own(l):
        gate_up(l, 1, c)
        for half in BOTH:
            down(l, 1, c, half)
            cols = (A, B)[half]
            rs_core(l, half).wait_recv()
            part[c, :, cols] = part[c, :, cols] + r1[l, :, cols]
            for t in BOTH:
                send((rs_a, rs_b)[half](l, t))

    def rs_add(l, t):
        row_a, row_b = chip_rows((1 - y, y)[t], x), chip_rows(y, (1 - x, x)[t])
        rs_a(l, t).wait_recv()
        part[c, row_a, A] = part[c, row_a, A] + r2a[l, t]
        if t == 0:
            send(rs_a_last(l))
        rs_b(l, t).wait_recv()
        part[c, row_b, B] = part[c, row_b, B] + r2b[l, t]
        if t == 0:
            send(rs_b_last(l))

    def rs_middle(l):
        for t in BOTH:
            rs_add(l, t)

    def rs_end(l, out):
        rs_a_last(l).wait_recv()
        out[:, A] = (mid[:, A].astype(F32) + (part[c, chip_rows(y, x), A] + r3a[l])).astype(BF)
        rs_b_last(l).wait_recv()
        out[:, B] = (mid[:, B].astype(F32) + (part[c, chip_rows(y, x), B] + r3b[l])).astype(BF)

    gain_mine[...] = jnp.zeros_like(gain_mine)
    gain_mine[:LAYERS, :ROWS] = an_ref[...].astype(F32)
    gain_mine[LAYERS : 2 * LAYERS, :ROWS] = mn_ref[...].astype(F32)
    gain_mine[...] = jnp.where(c == 1, pltpu.roll(gain_mine[...], ROWS, 1), gain_mine[...])
    for k in range(1, 8):
        go(gain_copy(k))
    send_gu(0, 0, ONE + TWO + THREE)
    for m in BOTH:
        send_attn(0, m)
    gains[me] = gain_mine[...]
    res[...] = x_ref[...]
    for k in range(1, 8):
        gain_arrival(k).wait_recv()
    for p in range(4):
        gain_rows[:, 384 * p : 384 * (p + 1)] = gains[2 * p] + gains[2 * p + 1]
    start_layer(0)
    relay_gu(0, 0, ONE + TWO + THREE)
    for m in BOTH:
        relay_attn(0, m)
    send_gu(0, 0, FOUR + FIVE + CORE)
    for l in range(LAYERS):
        start_own(l)
    relay_attn_across(0, 0)
    attention(0)
    relay_attn_across(0, 1)
    attention_out(0)
    relay_gu(0, 0, FOUR + FIVE[:2])
    attention_end(0)
    mlp(0, FIVE[2:])
    relay_gu(1, 0, ONE)
    mlp_own(0)
    relay_gu(1, 0, TWO)
    relay_attn(1, 0)
    rs_middle(0)
    send_gu(1, 0, THREE)
    send_attn(1, 1)
    relay_attn_across(1, 0)
    rs_end(0, res)
    start_layer(1)
    attention(1)
    relay_attn(1, 1)
    send_gu(1, 0, FOUR + FIVE + CORE)
    relay_gu(1, 0, THREE)
    relay_attn_across(1, 1)
    attention_out(1)
    relay_gu(1, 0, FOUR[:1])
    attention_end(1)
    mlp(1, FIVE[:1] + FOUR[1:] + FIVE[1:])
    mlp_own(1)
    rs_middle(1)
    rs_end(1, y_ref)
    for copy in sends + started:
        copy.wait_send()


def solution(mesh):
    vmem = pl.BlockSpec(memory_space=pltpu.VMEM)
    hbm = pl.BlockSpec(memory_space=pl.ANY)
    dma = pltpu.SemaphoreType.DMA
    pairs = [(7,), (LAYERS, 4, 2), (LAYERS, 4, 2), (LAYERS, 4, 5), (LAYERS, 3), (LAYERS, 2, 2, 7), (LAYERS, 2, 2, 6), (LAYERS,), (LAYERS, 9), (LAYERS, 8)]
    inv_freq = ROPE_THETA ** -(np.arange(HEAD_DIM // 2) * 2.0 / HEAD_DIM)
    angles = np.tile(np.arange(SEQ)[:, None] * inv_freq[None, :].astype(np.float32), (2, 1)).astype(np.float32)
    cos_table = np.concatenate([np.cos(angles), np.cos(angles)], axis=1)
    sin_table = np.concatenate([-np.sin(angles), np.sin(angles)], axis=1)

    def local_forward(hidden, attn_norm, w_q, w_k, w_v, w_o, mlp_norm, w_gate, w_up, w_down):
        wq = w_q.transpose(0, 2, 1, 3)
        wk, wv = w_k.transpose(0, 2, 1, 3), w_v.transpose(0, 2, 1, 3)
        y = pl.pallas_call(
            kernel,
            out_shape=jax.ShapeDtypeStruct((SEQ, DIM), BF),
            in_specs=[vmem] * 5 + [hbm] * 7,
            out_specs=vmem,
            scratch_shapes=[
                pltpu.VMEM((8, 2 * ROWS), F32),
                pltpu.VMEM((8, 8, 2 * ROWS), F32),
                pltpu.VMEM((8, DIM), F32),
                pltpu.VMEM((LAYERS, GROUP, DIM, HEAD_DIM), BF),
                pltpu.VMEM((LAYERS, DIM, OUT_COLS), BF),
                pltpu.VMEM((LAYERS, KV_HEADS, DIM, HEAD_DIM), BF),
                pltpu.VMEM((LAYERS, 2, DIM, WINDOW), BF),
                pltpu.VMEM((LAYERS, WINDOW, DIM), BF),
                pltpu.VMEM((LAYERS, 2, EDGE, DIM), BF),
                pltpu.VMEM((SEQ, DIM), BF),
                pltpu.VMEM((SEQ, DIM), BF),
                pltpu.VMEM((LAYERS, 2 * SEQ, DIM), BF),
                pltpu.VMEM((2, GROUP * SEQ, HEAD_DIM), BF),
                pltpu.VMEM((2 * SEQ, HEAD_DIM), BF),
                pltpu.VMEM((2 * SEQ, HEAD_DIM), BF),
                pltpu.VMEM((LAYERS, 2 * SEQ, DIM), BF),
                pltpu.VMEM((LAYERS, 2 * SEQ, OUT_COLS), F32),
                pltpu.VMEM((LAYERS, SEQ, OUT_COLS), F32),
                pltpu.VMEM((LAYERS, 8 * SEQ, DIM), BF),
                pltpu.VMEM((8 * SEQ, WINDOW), BF),
                pltpu.VMEM((2, 4 * SEQ, DIM), F32),
                pltpu.VMEM((LAYERS, 4 * SEQ, DIM), F32),
                pltpu.VMEM((LAYERS, 2, SEQ, DIM // 2), F32),
                pltpu.VMEM((LAYERS, 2, SEQ, DIM // 2), F32),
                pltpu.VMEM((LAYERS, SEQ, DIM // 2), F32),
                pltpu.VMEM((LAYERS, SEQ, DIM // 2), F32),
            ] + [dma(shape) for shape in pairs for end in BOTH] + [dma((LAYERS, 4))] * 3,
            compiler_params=pltpu.CompilerParams(collective_id=0, has_side_effects=True, vmem_limit_bytes=67043328),
        )(hidden.reshape(SEQ, DIM), attn_norm, mlp_norm, jnp.asarray(cos_table), jnp.asarray(sin_table), wq, w_o, wk, wv, w_gate, w_up, w_down)
        return y.reshape(1, SEQ, DIM)

    batch_spec = P(("dp", "fsdp"), None, None)
    gain_spec = P(None, "fsdp")
    proj_spec = P(None, "fsdp", None, None)
    mat_spec = P(None, "fsdp", None)
    return jax.shard_map(local_forward, mesh=mesh, in_specs=(batch_spec, gain_spec, proj_spec, proj_spec, proj_spec, mat_spec, gain_spec, mat_spec, mat_spec, mat_spec), out_specs=batch_spec, check_vma=False)
```
